16 devices in a mesh: cp: 2 (over z), fsdp: 8 (over y, x, core).
Axes of the slice: x: 2, y: 2, z: 2, core: 2. Of those that a mesh axis runs over, the one named last changes fastest.
Arguments:
- tokens: int32 [128, 256], P('fsdp', 'cp')
- lengths: int32 [128], P('fsdp')
- embed_table: bfloat16 [33, 640], replicated
- layer_vecs: float32 [9, 640], P(None, 'fsdp')
- w_qkv: bfloat16 [640, 3, 20, 32], P('fsdp')
- w_out: bfloat16 [640, 640], P('fsdp')
- w_up: bfloat16 [640, 2560], P('fsdp')
- b_up: float32 [2560], P('fsdp')
- w_down: bfloat16 [2560, 640], P('fsdp')
- grad_out: bfloat16 [128, 256, 640], P('fsdp', 'cp')
Outputs:
- output 1: bfloat16 [128, 256, 640], P('fsdp', 'cp')
- output 2: float32 [33, 640], replicated
- output 3: float32 [9, 640], P(None, 'fsdp')
- output 4: float32 [640, 3, 20, 32], P('fsdp')
- output 5: float32 [640, 640], P('fsdp')
- output 6: float32 [640, 2560], P('fsdp')
- output 7: float32 [2560], P('fsdp')
- output 8: float32 [2560, 640], P('fsdp')
All inputs are finite; a program needn't handle non-finite values.
Results may differ from the reference program's by a relative error of at most 0.0099633.
Values are sent between devices in bfloat16 or wider.
A program may use at most 1 GiB of HBM per device.

```python
import jax
import jax.numpy as jnp
from jax import lax

NUM_SEQS = 128
SEQ_LEN = 256
MODEL_DIM = 640
NUM_HEADS = 20
FFN_DIM = 2560
VOCAB_SIZE = 33
BOS_ID = 0
PAD_ID = 1
EOS_ID = 2
MASK_ID = 32
HEAD_DIM = MODEL_DIM // NUM_HEADS
LN_EPS = 1e-5
ROPE_BASE = 10000.0
TRAIN_RATIO = 0.15 * 0.8
NEG_BIG = -1e30


def draw_tokens(rng_key):
    key_list = jax.random.split(rng_key, 4)
    lengths = jax.random.randint(key_list[0], (NUM_SEQS,), SEQ_LEN // 4, SEQ_LEN + 1)
    lengths = lengths.at[0].set(SEQ_LEN).at[1].set(SEQ_LEN // 4)
    positions = jnp.arange(SEQ_LEN)[None, :]
    len_col = lengths[:, None]
    residues = jax.random.randint(key_list[1], (NUM_SEQS, SEQ_LEN), 4, 31)
    win_start = jax.random.randint(key_list[2], (NUM_SEQS, 1), 0, SEQ_LEN)
    in_win = (positions >= win_start) & (positions < win_start + SEQ_LEN // 4)
    hit_draw = jax.random.randint(key_list[3], (NUM_SEQS, SEQ_LEN), 0, 100)
    is_mask = hit_draw < jnp.where(in_win, 45, 5)
    tokens = jnp.where(is_mask, MASK_ID, residues)
    tokens = jnp.where(positions >= len_col, PAD_ID, tokens)
    tokens = jnp.where(positions == len_col - 1, EOS_ID, tokens)
    tokens = jnp.where(positions == 0, BOS_ID, tokens)
    return tokens.astype(jnp.int32), lengths.astype(jnp.int32)


def setup_inputs(seed: int = 0) -> dict:
    key_list = jax.random.split(jax.random.key(seed), 9)
    tokens, lengths = draw_tokens(key_list[0])
    embed_table = jax.random.normal(key_list[1], (VOCAB_SIZE, MODEL_DIM), jnp.float32)
    row_scale = jnp.array([0.2, 0.3, 0.3, 0.3, SEQ_LEN ** -0.5, 0.3, 0.2, 0.3, 0.3], jnp.float32)
    row_shift = jnp.array([1.0, 0.0, 0.0, 0.0, 0.0, 0.0, 1.0, 0.0, 0.0], jnp.float32)
    layer_vecs = row_shift[:, None] + row_scale[:, None] * jax.random.normal(key_list[2], (9, MODEL_DIM), jnp.float32)
    w_qkv = jax.random.normal(key_list[3], (MODEL_DIM, 3, NUM_HEADS, HEAD_DIM), jnp.float32) * MODEL_DIM ** -0.5
    w_out = jax.random.normal(key_list[4], (MODEL_DIM, MODEL_DIM), jnp.float32) * (SEQ_LEN / (2.0 * MODEL_DIM)) ** 0.5
    w_up = jax.random.normal(key_list[5], (MODEL_DIM, FFN_DIM), jnp.float32) * MODEL_DIM ** -0.5
    b_up = 0.5 * jax.random.normal(key_list[6], (FFN_DIM,), jnp.float32)
    w_down = jax.random.normal(key_list[7], (FFN_DIM, MODEL_DIM), jnp.float32) * FFN_DIM ** -0.5
    grad_out = jax.random.normal(key_list[8], (NUM_SEQS, SEQ_LEN, MODEL_DIM), jnp.float32)
    return {
        'tokens': tokens,
        'lengths': lengths,
        'embed_table': embed_table.astype(jnp.bfloat16),
        'layer_vecs': layer_vecs,
        'w_qkv': w_qkv.astype(jnp.bfloat16),
        'w_out': w_out.astype(jnp.bfloat16),
        'w_up': w_up.astype(jnp.bfloat16),
        'b_up': b_up,
        'w_down': w_down.astype(jnp.bfloat16),
        'grad_out': grad_out.astype(jnp.bfloat16),
    }


def rounded(z_in):
    return z_in + lax.stop_gradient(z_in.astype(jnp.bfloat16).astype(jnp.float32) - z_in)


def layer_norm(z_in, ln_gain, ln_bias):
    row_mean = jnp.mean(z_in, axis=-1, keepdims=True)
    centered = z_in - row_mean
    row_var = jnp.mean(centered * centered, axis=-1, keepdims=True)
    return centered * lax.rsqrt(row_var + LN_EPS) * ln_gain + ln_bias


def rotate(z_in, cos_t, sin_t):
    lower_half, upper_half = jnp.split(z_in, 2, axis=-1)
    return jnp.concatenate([lower_half * cos_t - upper_half * sin_t, upper_half * cos_t + lower_half * sin_t], axis=-1)


def one_sequence(params, embed_f32, tok_row, len_row):
    layer_vecs, w_qkv, w_out, w_up, b_up, w_down = params
    positions = jnp.arange(SEQ_LEN)
    is_mask = tok_row == MASK_ID
    key_valid = positions < len_row
    n_mask = jnp.sum(is_mask.astype(jnp.float32))
    drop_scale = (1.0 - TRAIN_RATIO) / (1.0 - n_mask / len_row.astype(jnp.float32))
    keep_scale = jnp.where(is_mask | jnp.logical_not(key_valid), 0.0, drop_scale)
    embedded = embed_f32[tok_row] * keep_scale[:, None]
    norm_in = rounded(layer_norm(embedded, layer_vecs[0], layer_vecs[1]))
    qkv_lin = jnp.dot(norm_in, w_qkv.reshape(MODEL_DIM, 3 * MODEL_DIM)) + layer_vecs[2:5].reshape(3 * MODEL_DIM)
    qkv_lin = qkv_lin.reshape(SEQ_LEN, 3, NUM_HEADS, HEAD_DIM)
    inv_freq = 1.0 / (ROPE_BASE ** (jnp.arange(0, HEAD_DIM, 2, dtype=jnp.float32) / HEAD_DIM))
    angles = positions.astype(jnp.float32)[:, None] * inv_freq[None, :]
    cos_t = jnp.cos(angles)[:, None, :]
    sin_t = jnp.sin(angles)[:, None, :]
    q_heads = rounded(rotate(qkv_lin[:, 0] * HEAD_DIM ** -0.5, cos_t, sin_t))
    k_heads = rounded(rotate(qkv_lin[:, 1], cos_t, sin_t))
    v_heads = rounded(qkv_lin[:, 2])

    def one_head(head_in):
        q_h, k_h, v_h = head_in
        scores = jnp.dot(q_h, k_h.T)
        scores = jnp.where(key_valid[None, :], scores, NEG_BIG)
        return jnp.dot(jax.nn.softmax(scores, axis=-1), v_h)

    per_head = lax.map(jax.checkpoint(one_head), (q_heads.transpose(1, 0, 2), k_heads.transpose(1, 0, 2), v_heads.transpose(1, 0, 2)))
    attn_out = rounded(per_head.transpose(1, 0, 2).reshape(SEQ_LEN, MODEL_DIM))
    resid_mid = embedded + jnp.dot(attn_out, w_out) + layer_vecs[5]
    norm_mid = rounded(layer_norm(resid_mid, layer_vecs[6], layer_vecs[7]))
    gelu_out = rounded(jax.nn.gelu(jnp.dot(norm_mid, w_up) + b_up, approximate=False))
    return resid_mid + jnp.dot(gelu_out, w_down) + layer_vecs[8]


def reference(tokens, lengths, embed_table, layer_vecs, w_qkv, w_out, w_up, b_up, w_down, grad_out):
    params = (layer_vecs, w_qkv.astype(jnp.float32), w_out.astype(jnp.float32), w_up.astype(jnp.float32), b_up, w_down.astype(jnp.float32))
    seq_fn = jax.checkpoint(one_sequence)

    def forward(params_in, embed_f32):
        def per_row(seq_row):
            return seq_fn(params_in, embed_f32, seq_row[0], seq_row[1])
        return lax.map(per_row, (tokens, lengths))

    layer_out, pullback = jax.vjp(forward, params, embed_table.astype(jnp.float32))
    d_params, d_embed = pullback(grad_out.astype(jnp.float32))
    return (layer_out.astype(jnp.bfloat16), d_embed, d_params[0], d_params[1], d_params[2], d_params[3], d_params[4], d_params[5])
```

```python
import functools

import jax
import jax.numpy as jnp
from jax import lax
from jax.experimental import pallas as pl
from jax.experimental.pallas import tpu as pltpu
from jax.sharding import PartitionSpec as P

MASK_ID = 32
PAD_ID = 1
NCLS = 32
LN_EPS = 1e-5
ROPE_BASE = 10000.0
TRAIN_RATIO = 0.15 * 0.8
NEG_BIG = -1e30
BF = jnp.bfloat16
F32 = jnp.float32
VMEM_LIMIT = 60 * 1024 * 1024
NN = (((1,), (0,)), ((), ()))
NT = (((1,), (1,)), ((), ()))
TN = (((0,), (0,)), ((), ()))


def mm(a, b, dims):
    return lax.dot_general(a, b, dims, preferred_element_type=F32)


def split3(x):
    hi = x.astype(BF)
    rest = x - hi.astype(F32)
    mid = rest.astype(BF)
    lo = (rest - mid.astype(F32)).astype(BF)
    return hi, mid, lo


def one_hot_rows(cls):
    return (lax.broadcasted_iota(jnp.int32, (NCLS, cls.shape[-1]), 0) == cls).astype(BF)


def key_rows(pos, length):
    row = lax.broadcasted_iota(jnp.int32, (16, pos.shape[-1]), 0)
    bias = jnp.where(pos < length, 0.0, NEG_BIG)
    return jnp.where(row == 0, bias, jnp.where(row < 4, 1.0, 0.0)).astype(BF)


def rope_fwd(lo, hi, cos, sin):
    return jnp.concatenate([lo * cos - hi * sin, hi * cos + lo * sin], axis=0)


def attn_fwd_kernel(n_heads, hd, lens, cls_ref, pos_ref, cos_ref, sin_ref, hc_ref, w_ref, b_ref,
                    qkv_ref, o_ref, lse_ref, class_scr, lin_scr):
    step = pl.program_id(0)
    dim = n_heads * hd

    @pl.when(step == 0)
    def _():
        full = mm(hc_ref[...], w_ref[...], NN) + b_ref[...]
        class_scr[:, :dim] = full[:, :dim] * hd ** -0.5
        class_scr[:, dim:] = full[:, dim:]

    rows = class_scr[pl.ds(step * NCLS, NCLS), :]
    hot = one_hot_rows(cls_ref[0])
    hot3 = jnp.concatenate([hot, hot, hot], axis=0)
    for part in range(3):
        cols = slice(part * dim, (part + 1) * dim)
        lin_scr[cols, :] = mm(jnp.concatenate(split3(rows[:, cols]), axis=0), hot3, TN)
    length = lens[step]
    kx = key_rows(pos_ref[...], length)
    qrow = lax.broadcasted_iota(jnp.int32, kx.shape, 0)
    qx = jnp.where(qrow == 0, 1.0, 0.0).astype(BF)
    cos, sin = cos_ref[...], sin_ref[...]
    half = hd // 2

    def head(h):
        base = pl.multiple_of(h * hd, hd)
        q = rope_fwd(lin_scr[pl.ds(base, half), :], lin_scr[pl.ds(base + half, half), :], cos, sin).astype(BF)
        k = rope_fwd(lin_scr[pl.ds(dim + base, half), :], lin_scr[pl.ds(dim + base + half, half), :], cos, sin).astype(BF)
        v = lin_scr[pl.ds(2 * dim + base, hd), :].astype(BF)
        qkv_ref[0, pl.ds(base, hd), :] = q
        qkv_ref[0, pl.ds(dim + base, hd), :] = k
        qkv_ref[0, pl.ds(2 * dim + base, hd), :] = v
        s = mm(jnp.concatenate([k, kx], axis=0), jnp.concatenate([q, qx], axis=0), TN)
        top = jnp.max(s, axis=0, keepdims=True)
        p = jnp.exp(s - top)
        tot = jnp.sum(p, axis=0, keepdims=True)
        o = mm(v, p.astype(BF), NN)
        o_ref[0, pl.ds(base, hd), :] = o / tot
        lse_ref[0, pl.ds(h, 1), :] = top + jnp.log(tot)

    def body(i, carry):
        for u in range(4):
            head(i * 4 + u)
        return carry

    lax.fori_loop(0, n_heads // 4, body, 0)


def ffn_kernel(n_heads, hd, nsq, slen, ftile,
               scales, cls_ref, o_ref, gm_ref, gp_ref, et_ref, vecs_ref, bup_ref, wo_ref, wu_ref, wd_ref,
               outm_ref, outp_ref, do_ref, delta_ref, csum_ref, dvec_ref, dbup_ref, dwo_ref, dwu_ref, dwd_ref,
               x_scr, xh_scr, rs_scr, n_scr, g_scr, y_scr, dn_scr):
    step = pl.program_id(0)
    dim = n_heads * hd
    halfs = slen // 2

    @pl.when(step == 0)
    def _():
        dvec_ref[...] = jnp.zeros_like(dvec_ref)
        dbup_ref[...] = jnp.zeros_like(dbup_ref)
        dwo_ref[...] = jnp.zeros_like(dwo_ref)
        dwu_ref[...] = jnp.zeros_like(dwu_ref)
        dwd_ref[...] = jnp.zeros_like(dwd_ref)

    for i in range(nsq):
        r = slice(i * slen, (i + 1) * slen)
        hot = one_hot_rows(cls_ref[i])
        e = mm(hot, et_ref[...], TN) * scales[step * nsq + i]
        x1 = e + mm(o_ref[i].astype(BF), wo_ref[...], TN) + vecs_ref[5:6, :]
        x_scr[r, :] = x1
        mean = jnp.mean(x1, axis=-1, keepdims=True)
        cen = x1 - mean
        rstd = lax.rsqrt(jnp.mean(cen * cen, axis=-1, keepdims=True) + LN_EPS)
        xh = cen * rstd
        xh_scr[r, :] = xh
        rs_scr[r, :] = rstd
        n_scr[r, :] = (xh * vecs_ref[6:7, :] + vecs_ref[7:8, :]).astype(BF)
        g_scr[i * slen:i * slen + halfs, :] = gm_ref[i]
        g_scr[i * slen + halfs:(i + 1) * slen, :] = gp_ref[i]

    y_scr[...] = jnp.zeros_like(y_scr)
    dn_scr[...] = jnp.zeros_like(dn_scr)

    def body(j, carry):
        c = pl.ds(pl.multiple_of(j * ftile, ftile), ftile)
        n = n_scr[...]
        g = g_scr[...]
        wu = wu_ref[:, c]
        wd = wd_ref[c, :]
        u = mm(n, wu, NN) + bup_ref[:, c]
        phi = 0.5 + 0.5 * lax.erf(u * 0.7071067811865476)
        a = (u * phi).astype(BF)
        slope = phi + u * (jnp.exp(-0.5 * u * u) * 0.3989422804014327)
        y_scr[...] += mm(a, wd, NN)
        du = mm(g, wd, NT) * slope
        dub = du.astype(BF)
        dbup_ref[:, c] += jnp.sum(du, axis=0, keepdims=True)
        dwd_ref[c, :] += mm(a, g, TN)
        dwu_ref[:, c] += mm(n, dub, TN)
        dn_scr[...] += mm(dub, wu, NT)
        return carry

    lax.fori_loop(0, wu_ref.shape[1] // ftile, body, 0)

    for i in range(nsq):
        r = slice(i * slen, (i + 1) * slen)
        out = (x_scr[r, :] + y_scr[r, :] + vecs_ref[8:9, :]).astype(BF)
        outm_ref[i] = out[:halfs]
        outp_ref[i] = out[halfs:]
        dn = dn_scr[r, :]
        xh = xh_scr[r, :]
        dy = dn * vecs_ref[6:7, :]
        m1 = jnp.mean(dy, axis=-1, keepdims=True)
        m2 = jnp.mean(dy * xh, axis=-1, keepdims=True)
        g32 = g_scr[r, :].astype(F32)
        dx = g32 + rs_scr[r, :] * (dy - m1 - xh * m2)
        dvec_ref[0:1, :] += jnp.sum(dx, axis=0, keepdims=True)
        dvec_ref[1:2, :] += jnp.sum(dn * xh, axis=0, keepdims=True)
        dvec_ref[2:3, :] += jnp.sum(dn, axis=0, keepdims=True)
        dvec_ref[3:4, :] += jnp.sum(g32, axis=0, keepdims=True)
        dxb = dx.astype(BF)
        o = o_ref[i]
        dwo_ref[...] += mm(o.astype(BF), dxb, NN)
        do = mm(wo_ref[...], dxb, NT)
        do_ref[i] = do.astype(BF)
        delta_ref[i, 0:n_heads, :] = jnp.sum((do * o).reshape(n_heads, hd, slen), axis=1)
        csum_ref[i] = mm(one_hot_rows(cls_ref[i]), dxb, NN)


def attn_bwd_kernel(n_heads, hd, lens, scales, cls_ref, pos_ref, cos_ref, sin_ref, qkv_ref, do_ref, lse_ref, delta_ref,
                    csum_ref, ec_ref, vecs_ref, w_ref,
                    dw_ref, dvec_ref, dtab_ref, dlin_scr, bsum_scr, dcls_scr):
    step = pl.program_id(0)
    n_seq = pl.num_programs(0)
    dim = n_heads * hd
    half = hd // 2

    @pl.when(step == 0)
    def _():
        bsum_scr[...] = jnp.zeros_like(bsum_scr)

    kx = key_rows(pos_ref[...], lens[step])
    row = lax.broadcasted_iota(jnp.int32, kx.shape, 0)
    cos, sin = cos_ref[...], sin_ref[...]
    ones3 = jnp.where(row < 3, 1.0, 0.0).astype(BF)

    def put(base, val):
        dlin_scr[pl.ds(base, val.shape[0]), :] = val.astype(BF)
        width = val.shape[1] // 2
        bsum_scr[pl.ds(base, val.shape[0]), :] += val[:, :width] + val[:, width:]

    def unrope(val):
        lo, hi = val[:half], val[half:]
        return jnp.concatenate([lo * cos + hi * sin, hi * cos - lo * sin], axis=0)

    def head(h):
        base = pl.multiple_of(h * hd, hd)
        q = qkv_ref[0, pl.ds(base, hd), :]
        k = qkv_ref[0, pl.ds(dim + base, hd), :]
        v = qkv_ref[0, pl.ds(2 * dim + base, hd), :]
        do = do_ref[0, pl.ds(base, hd), :]
        l1, l2, l3 = [t.astype(F32) for t in split3(-lse_ref[0, pl.ds(h, 1), :])]
        qx = jnp.where(row == 0, 1.0, jnp.where(row == 1, l1, jnp.where(row == 2, l2, jnp.where(row == 3, l3, 0.0)))).astype(BF)
        d1, d2, d3 = [t.astype(F32) for t in split3(-delta_ref[0, pl.ds(h, 1), :])]
        dx = jnp.where(row == 0, d1, jnp.where(row == 1, d2, jnp.where(row == 2, d3, 0.0))).astype(BF)
        p = jnp.exp(mm(jnp.concatenate([k, kx], axis=0), jnp.concatenate([q, qx], axis=0), TN))
        dp = mm(jnp.concatenate([v, ones3], axis=0), jnp.concatenate([do, dx], axis=0), TN)
        pb = p.astype(BF)
        ds = (p * dp).astype(BF)
        dv = mm(do, pb, NT)
        dk = mm(q, ds, NT)
        dq = mm(k, ds, NN)
        put(base, unrope(dq) * hd ** -0.5)
        put(dim + base, unrope(dk))
        put(2 * dim + base, dv)

    def body(i, carry):
        for u in range(2):
            head(i * 2 + u)
        return carry

    lax.fori_loop(0, n_heads // 2, body, 0)
    hot = one_hot_rows(cls_ref[0])
    dcls_scr[pl.ds(pl.multiple_of(step * NCLS, NCLS), NCLS), :] = mm(hot, dlin_scr[...], NT)

    @pl.when(step == n_seq - 1)
    def _():
        e = ec_ref[...]
        cen = e - jnp.mean(e, axis=-1, keepdims=True)
        rstd = lax.rsqrt(jnp.mean(cen * cen, axis=-1, keepdims=True) + LN_EPS)
        xh = cen * rstd
        hc = (xh * vecs_ref[0:1, :] + vecs_ref[1:2, :]).astype(BF)
        acc = dcls_scr[...]
        hi = acc.astype(BF)
        lo = (acc - hi.astype(F32)).astype(BF)
        dw_ref[...] = mm(jnp.concatenate([hc, hc], axis=0), jnp.concatenate([hi, lo], axis=0), TN)
        dn = mm(hi, w_ref[...], NT) + mm(lo, w_ref[...], NT)
        dy = dn * vecs_ref[0:1, :]
        m1 = jnp.mean(dy, axis=-1, keepdims=True)
        m2 = jnp.mean(dy * xh, axis=-1, keepdims=True)
        de = rstd * (dy - m1 - xh * m2)
        dvec_ref[0:1, :] = jnp.sum(dn * xh, axis=0, keepdims=True)
        dvec_ref[1:2, :] = jnp.sum(dn, axis=0, keepdims=True)
        bias = jnp.sum(bsum_scr[...], axis=-1, keepdims=True)
        bias = jnp.transpose(jnp.broadcast_to(bias, (3 * dim, 128)))
        for part in range(3):
            dvec_ref[2 + part:3 + part, :] = bias[0:1, part * dim:(part + 1) * dim]
        tab = jnp.zeros((NCLS, dim), F32)
        for b in range(dcls_scr.shape[0] // NCLS):
            tab = tab + (de[b * NCLS:(b + 1) * NCLS] + csum_ref[b]) * scales[b]
        keep = lax.broadcasted_iota(jnp.int32, tab.shape, 0) != PAD_ID
        dtab_ref[...] = jnp.where(keep, tab, 0.0)


def whole(shape):
    return pl.BlockSpec(shape, lambda *_: (0,) * len(shape), pipeline_mode=pl.Buffered(1))


def params(sem="arbitrary"):
    return pltpu.CompilerParams(dimension_semantics=(sem,), vmem_limit_bytes=VMEM_LIMIT)


SMEM = pl.BlockSpec(memory_space=pltpu.SMEM)


def attn_fwd(lens, cls, pos, cos, sin, hc, w, bias, n_heads, hd):
    n_seq, _, slen = cls.shape
    dim = n_heads * hd
    return pl.pallas_call(
        functools.partial(attn_fwd_kernel, n_heads, hd),
        grid=(n_seq,),
        in_specs=[SMEM, pl.BlockSpec((1, 1, slen), lambda i: (i, 0, 0)), whole(pos.shape), whole(cos.shape),
                  whole(sin.shape), whole(hc.shape), whole(w.shape), whole(bias.shape)],
        out_specs=[pl.BlockSpec((1, 3 * dim, slen), lambda i: (i, 0, 0)), pl.BlockSpec((1, dim, slen), lambda i: (i, 0, 0)),
                   pl.BlockSpec((1, n_heads, slen), lambda i: (i, 0, 0))],
        out_shape=[jax.ShapeDtypeStruct((n_seq, 3 * dim, slen), BF), jax.ShapeDtypeStruct((n_seq, dim, slen), F32),
                   jax.ShapeDtypeStruct((n_seq, n_heads, slen), F32)],
        scratch_shapes=[pltpu.VMEM((n_seq * NCLS, 3 * dim), F32), pltpu.VMEM((3 * dim, slen), F32)],
        compiler_params=params(), name="attn_fwd",
        cost_estimate=pl.CostEstimate(flops=20 * 10**9, bytes_accessed=18 * 10**6, transcendentals=10**7),
    )(lens, cls, pos, cos, sin, hc, w, bias)


def ffn(scales, cls, o, gm, gp, etab, vecs, bup, wo, wu, wd, n_heads, hd, nsq=2, ftile=512):
    n_seq, _, slen = cls.shape
    dim, ff = wu.shape
    rows = nsq * slen
    blk = lambda *s: pl.BlockSpec((nsq,) + s, lambda i: (i,) + (0,) * len(s))
    sds = jax.ShapeDtypeStruct
    return pl.pallas_call(
        functools.partial(ffn_kernel, n_heads, hd, nsq, slen, ftile),
        grid=(n_seq // nsq,),
        in_specs=[SMEM, blk(1, slen), blk(dim, slen), blk(slen // 2, dim), blk(slen // 2, dim), whole(etab.shape),
                  whole(vecs.shape), whole(bup.shape), whole(wo.shape), whole(wu.shape), whole(wd.shape)],
        out_specs=[blk(slen // 2, dim), blk(slen // 2, dim), blk(dim, slen), blk(n_heads, slen), blk(NCLS, dim),
                   whole((4, dim)), whole((1, ff)), whole((dim, dim)), whole((dim, ff)), whole((ff, dim))],
        out_shape=[sds((n_seq, slen // 2, dim), BF), sds((n_seq, slen // 2, dim), BF), sds((n_seq, dim, slen), BF),
                   sds((n_seq, n_heads, slen), F32), sds((n_seq, NCLS, dim), F32), sds((4, dim), F32), sds((1, ff), F32),
                   sds((dim, dim), F32), sds((dim, ff), F32), sds((ff, dim), F32)],
        scratch_shapes=[pltpu.VMEM((rows, dim), F32), pltpu.VMEM((rows, dim), F32), pltpu.VMEM((rows, 1), F32),
                        pltpu.VMEM((rows, dim), BF), pltpu.VMEM((rows, dim), BF), pltpu.VMEM((rows, dim), F32),
                        pltpu.VMEM((rows, dim), F32)],
        compiler_params=params(), name="ffn",
        cost_estimate=pl.CostEstimate(flops=60 * 10**9, bytes_accessed=40 * 10**6, transcendentals=10**7),
    )(scales, cls, o, gm, gp, etab, vecs, bup, wo, wu, wd)


def attn_bwd(lens, scales, cls, pos, cos, sin, qkv, do, lse, delta, csum, ec, vecs, w, n_heads, hd):
    n_seq, _, slen = cls.shape
    dim = n_heads * hd
    blk = lambda *s: pl.BlockSpec((1,) + s, lambda i: (i,) + (0,) * len(s))
    sds = jax.ShapeDtypeStruct
    return pl.pallas_call(
        functools.partial(attn_bwd_kernel, n_heads, hd),
        grid=(n_seq,),
        in_specs=[SMEM, SMEM, blk(1, slen), whole(pos.shape), whole(cos.shape), whole(sin.shape), blk(3 * dim, slen),
                  blk(dim, slen), blk(n_heads, slen), blk(n_heads, slen), whole(csum.shape), whole(ec.shape),
                  whole(vecs.shape), whole(w.shape)],
        out_specs=[whole((dim, 3 * dim)), whole((5, dim)), whole((NCLS, dim))],
        out_shape=[sds((dim, 3 * dim), F32), sds((5, dim), F32), sds((NCLS, dim), F32)],
        scratch_shapes=[pltpu.VMEM((3 * dim, slen), BF), pltpu.VMEM((3 * dim, slen // 2), F32),
                        pltpu.VMEM((n_seq * NCLS, 3 * dim), F32)],
        compiler_params=params(), name="attn_bwd",
        cost_estimate=pl.CostEstimate(flops=40 * 10**9, bytes_accessed=20 * 10**6, transcendentals=10**7),
    )(lens, scales, cls, pos, cos, sin, qkv, do, lse, delta, csum, ec, vecs, w)


def reduce_grad(full_grad, axis_dim):
    return lax.psum(lax.psum_scatter(full_grad, 'fsdp', scatter_dimension=axis_dim, tiled=True), 'cp')


def solution(mesh):
    swap = [(0, 1), (1, 0)]

    def local_step(tokens, lengths, embed_table, layer_vecs, w_qkv, w_out, w_up, b_up, w_down, grad_out):
        cp_index = lax.axis_index('cp')
        n_all, seq_half = tokens.shape
        n_seq = n_all // 2
        slen = 2 * seq_half
        vocab, dim = embed_table.shape
        n_heads, hd = w_qkv.shape[2], w_qkv.shape[3]

        def mine(z):
            return lax.dynamic_slice_in_dim(z, cp_index * n_seq, n_seq, 0)

        def other(z):
            return lax.dynamic_slice_in_dim(z, (1 - cp_index) * n_seq, n_seq, 0)

        tok_peer = lax.ppermute(other(tokens), 'cp', swap)
        g_peer = lax.ppermute(other(grad_out), 'cp', swap)
        g_mine = mine(grad_out)
        tok = jnp.concatenate([mine(tokens), tok_peer], axis=1)
        lens = mine(lengths)
        w_qkv2 = lax.all_gather(w_qkv.reshape(w_qkv.shape[0], -1), 'fsdp', axis=0, tiled=True)
        vecs = lax.all_gather(layer_vecs, 'fsdp', axis=1, tiled=True)
        out_w = lax.all_gather(w_out, 'fsdp', axis=0, tiled=True)
        up_w = lax.all_gather(w_up, 'fsdp', axis=0, tiled=True)
        up_b = lax.all_gather(b_up, 'fsdp', axis=0, tiled=True)
        down_w = lax.all_gather(w_down, 'fsdp', axis=0, tiled=True)

        seq_pos = jnp.arange(seq_half)
        pos = jnp.concatenate([cp_index * seq_half + seq_pos, (1 - cp_index) * seq_half + seq_pos])
        inv_freq = 1.0 / (ROPE_BASE ** (jnp.arange(0, hd, 2, dtype=F32) / hd))
        angles = inv_freq[:, None] * pos.astype(F32)[None, :]
        cos_t, sin_t = jnp.cos(angles), jnp.sin(angles)
        is_mask = tok == MASK_ID
        count = jnp.sum(is_mask.astype(jnp.int32), axis=1)
        scales = (1.0 - TRAIN_RATIO) / (1.0 - count.astype(F32) / lens.astype(F32))
        cls = jnp.where(is_mask | (pos[None, :] >= lens[:, None]), PAD_ID, tok)[:, None, :]
        etab = jnp.where(jnp.arange(NCLS)[:, None] == PAD_ID, 0, embed_table[:NCLS])
        e_cls = (etab.astype(F32)[None] * scales[:, None, None]).reshape(n_seq * NCLS, dim)
        cen = e_cls - jnp.mean(e_cls, axis=-1, keepdims=True)
        var = jnp.mean(cen * cen, axis=-1, keepdims=True)
        hc = (cen * lax.rsqrt(var + LN_EPS) * vecs[0] + vecs[1]).astype(BF)
        pos2 = pos[None, :].astype(jnp.int32)

        qkv, o, lse = attn_fwd(lens, cls, pos2, cos_t, sin_t, hc, w_qkv2, vecs[2:5].reshape(1, 3 * dim), n_heads, hd)
        (out_m, out_p, do, delta, csum, dvec_b, d_bup, d_wo, d_wu, d_wd) = ffn(
            scales, cls, o, g_mine, g_peer, etab, vecs, up_b[None, :], out_w, up_w, down_w, n_heads, hd)
        out_back = lax.ppermute(out_p, 'cp', swap)
        layer_out = jnp.where(cp_index == 0, jnp.concatenate([out_m, out_back], 0), jnp.concatenate([out_back, out_m], 0))
        d_w, dvec_a, d_tab = attn_bwd(lens, scales, cls, pos2, cos_t, sin_t, qkv, do, lse, delta, csum, e_cls, vecs, w_qkv2,
                                      n_heads, hd)
        d_table = jnp.concatenate([d_tab, jnp.zeros((vocab - NCLS, dim), F32)], 0)
        d_vecs = jnp.concatenate([dvec_a, dvec_b], 0)
        return (layer_out, lax.psum(d_table, ('cp', 'fsdp')), reduce_grad(d_vecs, 1),
                reduce_grad(d_w, 0).reshape(w_qkv.shape), reduce_grad(d_wo, 0), reduce_grad(d_wu, 0),
                reduce_grad(d_bup[0], 0), reduce_grad(d_wd, 0))

    in_specs = (P('fsdp', 'cp'), P('fsdp'), P(), P(None, 'fsdp'), P('fsdp', None, None, None), P('fsdp', None), P('fsdp', None), P('fsdp'), P('fsdp', None), P('fsdp', 'cp', None))
    out_specs = (P('fsdp', 'cp', None), P(), P(None, 'fsdp'), P('fsdp', None, None, None), P('fsdp', None), P('fsdp', None), P('fsdp'), P('fsdp', None))
    return jax.shard_map(local_step, mesh=mesh, in_specs=in_specs, out_specs=out_specs, check_vma=False)
```

```python
import functools

import jax
import jax.numpy as jnp
from jax import lax
from jax.experimental import pallas as pl
from jax.experimental.pallas import tpu as pltpu
from jax.sharding import PartitionSpec as P

MASK_ID = 32
PAD_ID = 1
NCLS = 32
LN_EPS = 1e-5
ROPE_BASE = 10000.0
TRAIN_RATIO = 0.15 * 0.8
NEG_BIG = -1e30
CORE, XDIR, YDIR = 1, 2, 4
ZDIR = 0
AXIS_OF = {YDIR: 0, XDIR: 1, CORE: 2}
XY, YX = (XDIR, YDIR), (YDIR, XDIR)
BF = jnp.bfloat16
F32 = jnp.float32
VMEM_LIMIT = 67043328
NN = (((1,), (0,)), ((), ()))
NT = (((1,), (1,)), ((), ()))
TN = (((0,), (0,)), ((), ()))
FTILE = 512
N_PIECE = 8
FWD_HEADS = 4
MESH_ID = pl.DeviceIdType.MESH
FFN_PLAN = ("4:asbs,5:a0b0,7:a1b1,8:a2b2csds,9:c0d0,10:a3b3,11:c1d1", "12:c2d2esfs,13:e0f0,14:c3d3,15:e1f1,16:e2f2,18:e3f3")
BWD_PLAN = ("2:a0b0,4:c0d0,8:vs,9:a1b1,10:o0v0,15:c1d1,16:ws,18:a2b2w0", "22:v1,24:xs,25:o1,26:x0,28:c2d2,30:a3b3,32:ys,34:y0w1",
            "35:v2x1,36:o2,38:c3d3")
BWD_TAIL = "zs,z0k0,y1w2x2,k1,z1y2v3o3,k2,z2w3x3,y3,k3,z3"


def mm(a, b, dims):
    return lax.dot_general(a, b, dims, preferred_element_type=F32)


def rmean(x):
    return jnp.mean(x, axis=-1, keepdims=True)


def csum(x):
    return jnp.sum(x, axis=0, keepdims=True)


def normalize(x):
    cen = x - rmean(x)
    rstd = lax.rsqrt(rmean(cen * cen) + LN_EPS)
    return cen * rstd, rstd


def norm_pull(dn, gain, xh, rstd):
    dy = dn * gain
    return rstd * (dy - rmean(dy) - xh * rmean(dy * xh))


def cat(parts):
    return jnp.concatenate(parts, axis=0)


def split3(x):
    hi = x.astype(BF)
    rest = x - hi.astype(F32)
    mid = rest.astype(BF)
    lo = (rest - mid.astype(F32)).astype(BF)
    return hi, mid, lo


def row_iota(rows, width):
    return lax.broadcasted_iota(jnp.int32, (rows, width), 0)


def one_hot_rows(cls):
    return (row_iota(NCLS, cls.shape[-1]) == cls).astype(BF)


def stack_rows(parts, width):
    row = row_iota(16, width)
    out = jnp.zeros(row.shape, F32)
    for i, part in enumerate(parts):
        out = jnp.where(row == i, part, out)
    return out.astype(BF)


def key_rows(pos, length):
    return stack_rows([jnp.where(pos < length, 0.0, NEG_BIG)] + [1.0] * 3, pos.shape[-1])


def rope_fwd(lo, hi, cos, sin):
    return cat([lo * cos - hi * sin, hi * cos + lo * sin])


def place():
    z, me = lax.axis_index('cp'), lax.axis_index('fsdp')
    bit = {CORE: lax.rem(me, XDIR), XDIR: lax.rem(me // XDIR, XDIR), YDIR: me // YDIR}
    partner = {way: (z, me + way - 2 * way * bit[way]) for way in bit}
    partner[ZDIR] = (1 - z, me)
    return bit, partner


def greet(partner):
    barrier = pltpu.get_barrier_semaphore()
    for way in partner:
        pl.semaphore_signal(barrier, inc=1, device_id=partner[way], device_id_type=MESH_ID)
    pl.semaphore_wait(barrier, len(partner))


class Stream:
    def __init__(self, num, order, src, bufs, out, sems, loc, own=None):
        self.num, self.order, self.src, self.bufs, self.out = num, order, src, bufs, out
        self.sems, self.loc, self.own = sems, loc, own

    def pick(self, stage, bit):
        way = self.order[stage - 1]
        buf = self.bufs[stage - 1]
        return buf.at[:, bit] if stage == 1 and way == XDIR else buf.at[bit]

    def copy(self, stage):
        bit, partner = self.loc
        way = (CORE, *self.order, ZDIR)[stage]
        if stage == 0:
            src = self.src(1 - bit[CORE])
        elif way == ZDIR:
            src = self.bufs[stage - 1]
        else:
            src = self.pick(stage, 1 - bit[way])
        return pltpu.make_async_remote_copy(
            src_ref=src, dst_ref=self.bufs[stage], send_sem=self.sems[0].at[self.num, stage],
            recv_sem=self.sems[1].at[self.num, stage], device_id=partner[way], device_id_type=MESH_ID)

    def local(self):
        return pltpu.make_async_copy(self.src(self.loc[0][CORE]), *self.own)

    def start(self):
        self.copy(0).start()
        if self.own:
            self.local().start()

    def advance(self, stage):
        bit = self.loc[0]
        buf = self.bufs[stage]
        self.copy(stage).wait()
        if stage == 0:
            if self.own:
                self.local().wait()
            buf[...] += self.own[0][...] if self.own else self.src(bit[CORE])[...]
        elif stage <= len(self.order):
            buf[...] += self.pick(stage, bit[self.order[stage - 1]])[...]
        else:
            self.out[...] = self.bufs[stage - 1][...] + buf[...]
            return
        self.copy(stage + 1).start()


class AllSum:
    def __init__(self, ref, bufs, sems, loc):
        self.ref, self.bufs, self.sems, self.loc = ref, bufs, sems, loc
        self.ways = (CORE, XDIR, YDIR, ZDIR)

    def copy(self, stage):
        return pltpu.make_async_remote_copy(
            src_ref=self.ref, dst_ref=self.bufs.at[stage], send_sem=self.sems[0].at[stage], recv_sem=self.sems[1].at[stage],
            device_id=self.loc[1][self.ways[stage]], device_id_type=MESH_ID)

    def start(self):
        self.copy(0).start()

    def advance(self, stage):
        self.copy(stage).wait()
        self.ref[...] += self.bufs[stage]
        if stage + 1 < len(self.ways):
            self.copy(stage + 1).start()


def act(streams, text):
    for name, what in zip(text[::2], text[1::2]):
        if what == "s":
            streams[name].start()
        else:
            streams[name].advance(int(what))


def follow(plan, tick, streams):
    for item in ",".join(plan).split(","):
        when, text = item.split(":")

        @pl.when(tick == int(when))
        def _(text=text):
            act(streams, text)


def attn_fwd_kernel(n_heads, hd, lens, cls_ref, pos_ref, cos_ref, sin_ref, hc_ref, w_ref, b_ref,
                    qkv_ref, o_ref, lse_ref, class_scr, lin_scr):
    step = pl.program_id(0)
    dim = n_heads * hd

    @pl.when(step == 0)
    def _():
        full = mm(hc_ref[...], w_ref[...], NN) + b_ref[...]
        class_scr[:, :dim] = full[:, :dim] * hd ** -0.5
        class_scr[:, dim:] = full[:, dim:]

    rows = class_scr[pl.ds(step * NCLS, NCLS), :]
    hot = one_hot_rows(cls_ref[0])
    hot3 = cat([hot] * 3)
    for part in range(3):
        cols = slice(part * dim, (part + 1) * dim)
        lin_scr[cols, :] = mm(cat(split3(rows[:, cols])), hot3, TN)
    length = lens[step]
    kx = key_rows(pos_ref[...], length)
    qx = stack_rows([1.0], kx.shape[-1])
    cos, sin = cos_ref[...], sin_ref[...]
    half = hd // 2

    def heads(hs):
        bases = [pl.multiple_of(h * hd, hd) for h in hs]
        qs, ks, vs = [], [], []
        for base in bases:
            piece = lambda off, size: lin_scr[pl.ds(base + off, size), :]
            qs.append(rope_fwd(piece(0, half), piece(half, half), cos, sin).astype(BF))
            ks.append(rope_fwd(piece(dim, half), piece(dim + half, half), cos, sin).astype(BF))
            vs.append(piece(2 * dim, hd).astype(BF))
            for part, val in enumerate((qs[-1], ks[-1], vs[-1])):
                qkv_ref[0, pl.ds(part * dim + base, hd), :] = val
        ss = [mm(cat([k, kx]), cat([q, qx]), TN) for q, k in zip(qs, ks)]
        tops = [jnp.max(s, axis=0, keepdims=True) for s in ss]
        ps = [jnp.exp(s - t) for s, t in zip(ss, tops)]
        tots = [csum(p) for p in ps]
        os = [mm(v, p.astype(BF), NN) for v, p in zip(vs, ps)]
        for h, base, o, tot, top in zip(hs, bases, os, tots, tops):
            o_ref[0, pl.ds(base, hd), :] = o / tot
            lse_ref[0, pl.ds(h, 1), :] = top + jnp.log(tot)

    def body(i, carry):
        heads([i * FWD_HEADS + u for u in range(FWD_HEADS)])
        return carry

    lax.fori_loop(0, n_heads // FWD_HEADS, body, 0)


def ffn_kernel(n_heads, hd, nsq, slen, keep_tiles,
               scales, cls_ref, o_ref, gm_ref, gp_ref, et_ref, vecs_ref, bup_ref, wo_ref, wu_ref, wd_ref,
               outm_ref, outp_ref, do_ref, delta_ref, csum_ref, dvec_ref, dbup_ref, dwo_ref, gu_ref, gd_ref, ru_ref, rd_ref,
               xh_scr, rs_scr, n_scr, g_scr, y_scr, dn_scr, au_scr, ad_scr, u0, u1, u2, u3, d0, d1, d2, d3,
               send_sem, recv_sem, out_sem):
    tile, blk = pl.program_id(0), pl.program_id(1)
    n_tile, n_blk = pl.num_programs(0), pl.num_programs(1)
    tick = tile * n_blk + blk
    first, last = tile == 0, tile == n_tile - 1
    halfs = slen // 2
    n_rows = nsq * slen
    rows = pl.ds(pl.multiple_of(blk * n_rows, n_rows), n_rows)
    loc = place()
    sems = (send_sem, recv_sem)
    streams = {}
    for t in range(keep_tiles):
        for kind, (order, acc, bufs, out) in enumerate(((XY, au_scr, (u0, u1, u2, u3), ru_ref), (YX, ad_scr, (d0, d1, d2, d3), rd_ref))):
            streams["abcdef"[2 * t + kind]] = Stream(
                2 * t + kind, order, (lambda c, acc=acc, t=t: acc.at[t, :, :, c]), tuple(b.at[t] for b in bufs), out.at[t], sems, loc)

    def handed(t):
        return [pltpu.make_async_copy(acc.at[keep_tiles + t], out.at[t], out_sem.at[2 * t + kind])
                for kind, (acc, out) in enumerate(((au_scr, gu_ref), (ad_scr, gd_ref)))]

    @pl.when(tick == 0)
    def _():
        greet(loc[1])
        dvec_ref[...] = jnp.zeros_like(dvec_ref)
        dbup_ref[...] = jnp.zeros_like(dbup_ref)
        dwo_ref[...] = jnp.zeros_like(dwo_ref)

    follow(FFN_PLAN, tick, streams)

    @pl.when(tick == (n_tile - 1) * n_blk)
    def _():
        for copy in handed(0):
            copy.start()

    @pl.when(first)
    def _():
        for i in range(nsq):
            r = pl.ds(pl.multiple_of(blk * n_rows + i * slen, slen), slen)
            e = mm(one_hot_rows(cls_ref[i]), et_ref[...], TN) * scales[blk * nsq + i]
            x1 = e + mm(o_ref[i].astype(BF), wo_ref[...], TN) + vecs_ref[5:6, :]
            xh, rstd = normalize(x1)
            xh_scr[r, :] = xh
            rs_scr[r, :] = rstd
            y_scr[r, :] = x1 + vecs_ref[8:9, :]
            n_scr[r, :] = (xh * vecs_ref[6:7, :] + vecs_ref[7:8, :]).astype(BF)
            for part, ref in enumerate((gm_ref, gp_ref)):
                g_scr[pl.ds(pl.multiple_of(blk * n_rows + i * slen + part * halfs, halfs), halfs), :] = ref[i]
        dn_scr[rows, :] = jnp.zeros_like(dn_scr[rows, :])

    @pl.when(blk == 0)
    def _():
        au_scr[tile] = jnp.zeros(au_scr.shape[1:], F32)
        ad_scr[tile] = jnp.zeros(ad_scr.shape[1:], F32)

    n = n_scr[rows, :]
    g = g_scr[rows, :]
    wu = wu_ref[...]
    wd = wd_ref[...]
    cols = pl.ds(pl.multiple_of(tile * wu.shape[1], wu.shape[1]), wu.shape[1])
    u = mm(n, wu, NN) + bup_ref[:, cols]
    phi = 0.5 + 0.5 * lax.erf(u * 0.7071067811865476)
    a = (u * phi).astype(BF)
    slope = phi + u * (jnp.exp(-0.5 * u * u) * 0.3989422804014327)
    y_scr[rows, :] += mm(a, wd, NN)
    du = mm(g, wd, NT) * slope
    dub = du.astype(BF)
    dbup_ref[:, cols] += csum(du)
    ad_scr[tile] += mm(a, g, TN).reshape(ad_scr.shape[1:])
    au_scr[tile] += mm(n, dub, TN).reshape(au_scr.shape[1:])
    dn_scr[rows, :] += mm(dub, wu, NT)

    @pl.when(last)
    def _():
        for i in range(nsq):
            r = pl.ds(pl.multiple_of(blk * n_rows + i * slen, slen), slen)
            out = y_scr[r, :].astype(BF)
            outm_ref[i] = out[:halfs]
            outp_ref[i] = out[halfs:]
            dn = dn_scr[r, :]
            xh = xh_scr[r, :]
            g32 = g_scr[r, :].astype(F32)
            dx = g32 + norm_pull(dn, vecs_ref[6:7, :], xh, rs_scr[r, :])
            dvec_ref[...] += cat([csum(dx), csum(dn * xh), csum(dn), csum(g32)])
            dxb = dx.astype(BF)
            o = o_ref[i]
            dwo_ref[...] += mm(o.astype(BF), dxb, NN)
            do = mm(wo_ref[...], dxb, NT)
            do_ref[i] = do.astype(BF)
            delta_ref[i] = jnp.sum((do * o).reshape(n_heads, hd, slen), axis=1)
            csum_ref[i] = mm(one_hot_rows(cls_ref[i]), dxb, NN)

    @pl.when(tick == n_tile * n_blk - 1)
    def _():
        for copy in handed(1):
            copy.start()
        for copy in handed(0) + handed(1):
            copy.wait()


def attn_bwd_kernel(hd, nh, lens, scales, cls_ref, pos_ref, cos_ref, sin_ref, qkv_ref, do_ref, lse_ref, delta_ref, hc_ref,
                    wq_ref, wk_ref, wv_ref, csum_ref, ec_ref, vecs_ref, dvb_ref, dbup_ref, gu_ref, gd_ref, go_ref,
                    ru_ref, rd_ref, ro_ref, rw_ref, rs_ref,
                    dlin_scr, bsum_scr, dcls_scr, dn_scr, dw_scr, small_scr, small_in,
                    u_own, d_own, o_own, u0, u1, u2, u3, d0, d1, d2, d3, o0, o1, o2, o3, w0, w1, w2, w3,
                    send_sem, recv_sem, own_sem, ssend, srecv):
    group, seq = pl.program_id(0), pl.program_id(1)
    n_group, n_seq = pl.num_programs(0), pl.num_programs(1)
    tick = group * n_seq + seq
    gdim = nh * hd
    half = hd // 2
    loc = place()
    sems = (send_sem, recv_sem)
    streams = {"k": AllSum(small_scr, small_in, (ssend, srecv), loc)}
    for t in range(gu_ref.shape[0]):
        for kind, (order, src, own, bufs, out) in enumerate(((XY, gu_ref, u_own, (u0, u1, u2, u3), ru_ref),
                                                             (YX, gd_ref, d_own, (d0, d1, d2, d3), rd_ref))):
            num = 2 * t + kind
            streams["abcd"[num]] = Stream(num, order, (lambda c, src=src, t=t: src.at[t, :, :, c]), tuple(b.at[t] for b in bufs),
                                          out.at[t], sems, loc, (own.at[t], own_sem.at[num]))
    num = own_sem.shape[0] - 1
    streams["o"] = Stream(num, YX, lambda c: go_ref.at[:, :, c], (o0, o1, o2, o3), ro_ref, sems, loc, (o_own, own_sem.at[num]))
    for t in range(rw_ref.shape[0]):
        streams["vwxyz"[t]] = Stream(num + 1 + t, (XY, YX)[t % 2], (lambda c, t=t: dw_scr.at[t, :, :, c]),
                                     tuple(b.at[t] for b in (w0, w1, w2, w3)), rw_ref.at[t], sems, loc)

    @pl.when(tick == 0)
    def _():
        greet(loc[1])
        act(streams, "asbscsdsos")
        dn_scr[...] = jnp.zeros_like(dn_scr)
        small_scr[...] = jnp.zeros_like(small_scr)

    follow(BWD_PLAN, tick, streams)

    @pl.when(seq == 0)
    def _():
        bsum_scr[...] = jnp.zeros_like(bsum_scr)

    width = pos_ref.shape[-1]
    kx = key_rows(pos_ref[...], lens[seq])
    vx = stack_rows([1.0] * 3, width)
    cos, sin = cos_ref[...], sin_ref[...]

    def put(base, val):
        dlin_scr[base:base + hd, :] = val.astype(BF)
        bsum_scr[base:base + hd, :] += val[:, :width // 2] + val[:, width // 2:]

    def unrope(val):
        return rope_fwd(val[:half], val[half:], cos, -sin)

    def extra(ref, h):
        return [t.astype(F32) for t in split3(-ref[0, pl.ds(group * nh + h, 1), :])]

    hs = range(nh)
    span = [slice(h * hd, (h + 1) * hd) for h in hs]
    qs, ks, vs = [[qkv_ref[0, part, span[h], :] for h in hs] for part in range(3)]
    dos = [do_ref[0, span[h], :] for h in hs]
    ss = [mm(cat([ks[h], kx]), cat([qs[h], stack_rows([1.0] + extra(lse_ref, h), width)]), TN) for h in hs]
    dps = [mm(cat([vs[h], vx]), cat([dos[h], stack_rows(extra(delta_ref, h), width)]), TN) for h in hs]
    ps = [jnp.exp(s) for s in ss]
    pbs = [p.astype(BF) for p in ps]
    dss = [(p * dp).astype(BF) for p, dp in zip(ps, dps)]
    dvs = [mm(dos[h], pbs[h], NT) for h in hs]
    dks = [mm(qs[h], dss[h], NT) for h in hs]
    dqs = [mm(ks[h], dss[h], NN) for h in hs]
    for h in hs:
        put(h * hd, unrope(dqs[h]) * hd ** -0.5)
        put(gdim + h * hd, unrope(dks[h]))
        put(2 * gdim + h * hd, dvs[h])

    dcls_scr[pl.ds(pl.multiple_of(seq * NCLS, NCLS), NCLS), :] = mm(one_hot_rows(cls_ref[0]), dlin_scr[...], NT)

    @pl.when(seq == n_seq - 1)
    def _():
        hc = hc_ref[...]
        acc = dcls_scr[...]
        hi, lo, _ = split3(acc)
        dw_scr[group] = mm(cat([hc, hc]), cat([hi, lo]), TN).reshape(dw_scr.shape[1:])
        dn = dn_scr[...]
        cols = pl.ds(pl.multiple_of(group * gdim, gdim), gdim)
        bias = csum(jnp.transpose(bsum_scr[...]))
        for part, w_ref in enumerate((wq_ref, wk_ref, wv_ref)):
            sel = slice(part * gdim, (part + 1) * gdim)
            dn = dn + mm(hi[:, sel], w_ref[...], NT) + mm(lo[:, sel], w_ref[...], NT)
            small_scr[2 + part:3 + part, cols] = bias[:, sel]
        dn_scr[...] = dn

    @pl.when(tick == n_group * n_seq - 1)
    def _():
        tail = BWD_TAIL.split(",")
        act(streams, tail[0])
        dn = dn_scr[...]
        xh, rstd = normalize(ec_ref[...])
        de = norm_pull(dn, vecs_ref[0:1, :], xh, rstd)
        small_scr[0:2, :] = cat([csum(dn * xh), csum(dn)])
        small_scr[5:13, :] = cat([dvb_ref[...], dbup_ref[...]])
        tab = jnp.zeros((NCLS, dn.shape[1]), F32)
        for b in range(dcls_scr.shape[0] // NCLS):
            tab = tab + (de[b * NCLS:(b + 1) * NCLS] + csum_ref[b]) * scales[b]
        small_scr[16:, :] = jnp.where(row_iota(*tab.shape) == PAD_ID, 0.0, tab)
        act(streams, "ks")
        for text in tail[1:]:
            act(streams, text)
        rs_ref[...] = small_scr[...]


def whole(shape):
    return pl.BlockSpec(shape, lambda *_: (0,) * len(shape), pipeline_mode=pl.Buffered(1))


def params(**kw):
    return pltpu.CompilerParams(vmem_limit_bytes=VMEM_LIMIT, **kw)


def cost(flops, moved):
    return pl.CostEstimate(flops=flops * 10**9, bytes_accessed=moved * 10**6, transcendentals=0)


def sds(*t):
    return jax.ShapeDtypeStruct(t, F32)


def sdb(*t):
    return jax.ShapeDtypeStruct(t, BF)


def vm(*t):
    return pltpu.VMEM(t, F32)


def dma(*t):
    return pltpu.SemaphoreType.DMA(t)


def stages(lead, *t):
    return [vm(*lead, 2, 2, *t), vm(*lead, 2, *t), vm(*lead, *t), vm(*lead, *t)]


SMEM = pl.BlockSpec(memory_space=pltpu.SMEM)


def attn_fwd(lens, cls, pos, cos, sin, hc, w, bias, n_heads, hd):
    n_seq, _, slen = cls.shape
    dim = n_heads * hd
    row = lambda *t: pl.BlockSpec((1,) + t, lambda i: (i, 0, 0))
    return pl.pallas_call(
        functools.partial(attn_fwd_kernel, n_heads, hd),
        grid=(n_seq,),
        in_specs=[SMEM, row(1, slen), whole(pos.shape), whole(cos.shape),
                  whole(sin.shape), whole(hc.shape), whole(w.shape), whole(bias.shape)],
        out_specs=[row(3 * dim, slen), row(dim, slen),
                   row(n_heads, slen)],
        out_shape=[sdb(n_seq, 3 * dim, slen), sds(n_seq, dim, slen), sds(n_seq, n_heads, slen)],
        scratch_shapes=[vm(n_seq * NCLS, 3 * dim), vm(3 * dim, slen)],
        compiler_params=params(), name="attn_fwd",
        cost_estimate=cost(20, 18),
    )(lens, cls, pos, cos, sin, hc, w, bias)


def ffn(scales, cls, o, gm, gp, etab, vecs, bup, wo, wu, wd, n_heads, hd, nsq=2, keep_tiles=3):
    n_seq, _, slen = cls.shape
    dim, ff = wu.shape
    tiles = ff // FTILE
    rest = tiles - keep_tiles
    halfs = slen // 2
    piece, slab = dim // N_PIECE, FTILE // N_PIECE
    n_blk = n_seq // nsq
    n_rows = n_seq * slen

    def blk(when, *t):
        return pl.BlockSpec((nsq,) + t, lambda j, r: (jnp.where(when(j), r, when(0) * (n_blk - 1)),) + (0,) * len(t))

    early = lambda j: j == 0
    late = lambda j: j == tiles - 1
    both = lambda j: (j == 0) | (j == tiles - 1)
    anyspace = pl.BlockSpec(memory_space=pl.ANY)
    cube = (2,) * 3
    bwd_u, bwd_d = (rest, *cube, piece, FTILE), (rest, *cube, slab, dim)
    red_u, red_d = (keep_tiles, piece, FTILE), (keep_tiles, slab, dim)
    return pl.pallas_call(
        functools.partial(ffn_kernel, n_heads, hd, nsq, slen, keep_tiles),
        grid=(tiles, n_blk),
        in_specs=[SMEM, blk(both, 1, slen), blk(both, dim, slen), blk(early, halfs, dim), blk(early, halfs, dim),
                  whole(etab.shape), whole(vecs.shape), whole(bup.shape), whole(wo.shape),
                  pl.BlockSpec((dim, FTILE), lambda j, r: (0, j)), pl.BlockSpec((FTILE, dim), lambda j, r: (j, 0))],
        out_specs=[blk(late, halfs, dim), blk(late, halfs, dim), blk(late, dim, slen), blk(late, n_heads, slen),
                   blk(late, NCLS, dim), whole((4, dim)), whole((1, ff)), whole((dim, dim)), anyspace, anyspace,
                   whole(red_u), whole(red_d)],
        out_shape=[sdb(n_seq, halfs, dim), sdb(n_seq, halfs, dim), sdb(n_seq, dim, slen), sds(n_seq, n_heads, slen),
                   sds(n_seq, NCLS, dim), sds(4, dim), sds(1, ff), sds(dim, dim), sds(*bwd_u), sds(*bwd_d), sds(*red_u), sds(*red_d)],
        scratch_shapes=[vm(n_rows, dim), vm(n_rows, 1), pltpu.VMEM((n_rows, dim), BF), pltpu.VMEM((n_rows, dim), BF),
                        vm(n_rows, dim), vm(n_rows, dim), vm(tiles, *cube, piece, FTILE), vm(tiles, *cube, slab, dim)]
        + stages((keep_tiles,), piece, FTILE) + stages((keep_tiles,), slab, dim)
        + [dma(2 * keep_tiles, 4), dma(2 * keep_tiles, 4), dma(2 * rest)],
        compiler_params=params(collective_id=1, has_side_effects=True), name="ffn", cost_estimate=cost(60, 40),
    )(scales, cls, o, gm, gp, etab, vecs, bup, wo, wu, wd)


def attn_bwd(lens, scales, cls, pos, cos, sin, qkv, do, lse, delta, hc, w, csums, ec, vecs, dvec_b, d_bup, d_wu, d_wd, d_wo,
             n_heads, hd, groups=5):
    n_seq, _, slen = cls.shape
    dim = n_heads * hd
    nh = n_heads // groups
    gdim = nh * hd
    cube = (2,) * 3
    blk = lambda *t: pl.BlockSpec((1,) + t, lambda g, i: (i,) + (0,) * len(t))
    wcol = lambda part: pl.BlockSpec((dim, gdim), lambda g, i: (0, part * groups + g))
    anyspace = pl.BlockSpec(memory_space=pl.ANY)
    ut, dt, ot = d_wu.shape[-2:], d_wd.shape[-2:], (dim // N_PIECE, dim)
    wt = (dim // N_PIECE, 3 * gdim)
    rest = d_wu.shape[0]
    fixed = (hc, csums, ec, vecs, dvec_b, d_bup.reshape(-1, dim))
    args = [lens, scales, cls, pos, cos, sin, qkv.reshape(n_seq, 3, dim, slen), do, lse, delta, hc, w, w, w, *fixed[1:],
            d_wu, d_wd, d_wo.reshape(*cube, *ot)]
    specs = [SMEM, SMEM, blk(1, slen), whole(pos.shape), whole(cos.shape), whole(sin.shape),
             pl.BlockSpec((1, 3, gdim, slen), lambda g, i: (i, 0, g, 0)), pl.BlockSpec((1, gdim, slen), lambda g, i: (i, g, 0)),
             blk(n_heads, slen), blk(n_heads, slen), whole(hc.shape), *[wcol(part) for part in range(3)],
             *[whole(t.shape) for t in fixed[1:]], *[anyspace] * 3]
    small = (16 + NCLS, dim)
    shapes = [sds(rest, *ut), sds(rest, *dt), sds(*ot), sds(groups, *wt), sds(*small)]
    n_str = 2 * rest + 1
    return pl.pallas_call(
        functools.partial(attn_bwd_kernel, hd, nh),
        grid=(groups, n_seq),
        in_specs=specs,
        out_specs=[whole(t.shape) for t in shapes],
        out_shape=shapes,
        scratch_shapes=[pltpu.VMEM((3 * gdim, slen), BF), vm(3 * gdim, slen // 2), vm(n_seq * NCLS, 3 * gdim),
                        vm(n_seq * NCLS, dim), vm(groups, *cube, *wt), vm(*small), vm(4, *small),
                        vm(rest, 2, 2, *ut), vm(rest, 2, 2, *dt), vm(2, 2, *ot)]
        + stages((rest,), *ut) + stages((rest,), *dt) + stages((), *ot) + stages((groups,), *wt)
        + [dma(n_str + groups, 4), dma(n_str + groups, 4), dma(n_str), dma(4), dma(4)],
        compiler_params=params(collective_id=0, has_side_effects=True), name="attn_bwd", cost_estimate=cost(40, 20),
    )(*args)


def solution(mesh):
    swap = [(0, 1), (1, 0)]
    n_fsdp = mesh.shape['fsdp']

    def hop(z, way):
        return lax.ppermute(z, 'fsdp', [(i, i ^ way) for i in range(n_fsdp)])

    def local_step(tokens, lengths, embed_table, layer_vecs, w_qkv, w_out, w_up, b_up, w_down, grad_out):
        cp_index = lax.axis_index('cp')
        me = lax.axis_index('fsdp')
        bit = {CORE: me % 2, XDIR: (me // 2) % 2, YDIR: me // 4}
        n_all, seq_half = tokens.shape
        n_seq = n_all // 2
        slen = 2 * seq_half
        vocab, dim = embed_table.shape
        n_heads, hd = w_qkv.shape[2], w_qkv.shape[3]

        def mine(z):
            return lax.dynamic_slice_in_dim(z, cp_index * n_seq, n_seq, 0)

        def other(z):
            return lax.dynamic_slice_in_dim(z, (1 - cp_index) * n_seq, n_seq, 0)

        def gather(z, order, at=0):
            z = z.reshape(z.shape[:at] + (1,) * 3 + z.shape[at:])
            for way in order:
                far = hop(z, way)
                ax = AXIS_OF[way] + at
                z = jnp.where(bit[way] == 0, jnp.concatenate([z, far], ax), jnp.concatenate([far, z], ax))
            return z

        xy, yx = (XDIR, YDIR, CORE), (YDIR, XDIR, CORE)
        tok_peer = lax.ppermute(other(tokens), 'cp', swap)
        small = gather(jnp.concatenate([layer_vecs, b_up.reshape(-1, layer_vecs.shape[1])], 0), xy)
        small = small.reshape((n_fsdp,) + small.shape[3:])
        w2 = w_qkv.reshape(w_qkv.shape[0], -1)
        wh = w2.shape[1] // 2
        w_qkv2 = jnp.concatenate([gather(w2[:, :wh], xy).reshape(dim, wh), gather(w2[:, wh:], yx).reshape(dim, wh)], 1)
        vecs = jnp.swapaxes(small[:, :9], 0, 1).reshape(9, dim)
        slabs = w_up.shape[1] // FTILE
        up_b = jnp.swapaxes(small[:, 9:].reshape(n_fsdp, slabs, -1), 0, 1).reshape(1, -1)
        g_peer = lax.ppermute(other(grad_out), 'cp', swap)
        g_mine = mine(grad_out)
        tok = jnp.concatenate([mine(tokens), tok_peer], axis=1)
        lens = mine(lengths)
        out_w = gather(w_out, xy).reshape(dim, dim)
        w_up_p = jnp.swapaxes(w_up.reshape(-1, n_fsdp, slabs, FTILE // n_fsdp), 1, 2).reshape(w_up.shape)
        up_w = gather(w_up_p, xy).reshape(dim, -1)
        down_w = gather(w_down.reshape(slabs, -1, dim), yx, 1).reshape(-1, dim)

        seq_pos = jnp.arange(seq_half)
        pos = jnp.concatenate([cp_index * seq_half + seq_pos, (1 - cp_index) * seq_half + seq_pos])
        inv_freq = 1.0 / (ROPE_BASE ** (jnp.arange(0, hd, 2, dtype=F32) / hd))
        angles = inv_freq[:, None] * pos.astype(F32)[None, :]
        cos_t, sin_t = jnp.cos(angles), jnp.sin(angles)
        is_mask = tok == MASK_ID
        count = jnp.sum(is_mask.astype(jnp.int32), axis=1)
        scales = (1.0 - TRAIN_RATIO) / (1.0 - count.astype(F32) / lens.astype(F32))
        cls = jnp.where(is_mask | (pos[None, :] >= lens[:, None]), PAD_ID, tok)[:, None, :]
        etab = jnp.where(jnp.arange(NCLS)[:, None] == PAD_ID, 0, embed_table[:NCLS])
        e_cls = (etab.astype(F32)[None] * scales[:, None, None]).reshape(n_seq * NCLS, dim)
        hc = (normalize(e_cls)[0] * vecs[0] + vecs[1]).astype(BF)
        pos2 = pos[None, :].astype(jnp.int32)

        qkv, o, lse = attn_fwd(lens, cls, pos2, cos_t, sin_t, hc, w_qkv2, vecs[2:5].reshape(1, 3 * dim), n_heads, hd)
        (out_m, out_p, do, delta, csums, dvec_b, d_bup, d_wo, d_wu, d_wd, red_wu, red_wd) = ffn(
            scales, cls, o, g_mine, g_peer, etab, vecs, up_b, out_w, up_w, down_w, n_heads, hd)
        out_back = lax.ppermute(out_p, 'cp', swap)
        layer_out = jnp.where(cp_index == 0, jnp.concatenate([out_m, out_back], 0), jnp.concatenate([out_back, out_m], 0))
        rest_wu, rest_wd, red_wo, red_w, red_small = attn_bwd(
            lens, scales, cls, pos2, cos_t, sin_t, qkv, do, lse, delta, hc, w_qkv2, csums, e_cls, vecs, dvec_b, d_bup, d_wu, d_wd,
            d_wo, n_heads, hd)
        groups = red_w.shape[0]
        red_w = jnp.transpose(red_w.reshape(groups, -1, 3, n_heads // groups, hd), (1, 2, 0, 3, 4)).reshape(w_qkv.shape)
        d_vecs = lax.dynamic_slice_in_dim(red_small[:9], me * layer_vecs.shape[1], layer_vecs.shape[1], 1)
        d_bup = lax.dynamic_slice_in_dim(red_small[9:13].reshape(slabs, n_fsdp, -1), me, 1, 1).reshape(b_up.shape)
        red_wu = jnp.concatenate([red_wu, rest_wu], 0).reshape(slabs, -1, n_fsdp, FTILE // n_fsdp)
        d_wup = jnp.transpose(red_wu, (1, 2, 0, 3)).reshape(w_up.shape)
        d_wdown = jnp.concatenate([red_wd, rest_wd], 0).reshape(w_down.shape)
        d_table = jnp.concatenate([red_small[16:16 + NCLS], jnp.zeros((vocab - NCLS, dim), F32)], 0)
        return layer_out, d_table, d_vecs, red_w, red_wo, d_wup, d_bup, d_wdown

    in_specs = (P('fsdp', 'cp'), P('fsdp'), P(), P(None, 'fsdp'), P('fsdp', None, None, None), P('fsdp', None), P('fsdp', None), P('fsdp'), P('fsdp', None), P('fsdp', 'cp', None))
    out_specs = (P('fsdp', 'cp', None), P(), P(None, 'fsdp'), P('fsdp', None, None, None), P('fsdp', None), P('fsdp', None), P('fsdp'), P('fsdp', None))
    return jax.shard_map(local_step, mesh=mesh, in_specs=in_specs, out_specs=out_specs, check_vma=False)
```

```python
import functools

import jax
import jax.numpy as jnp
from jax import lax
from jax.experimental import pallas as pl
from jax.experimental.pallas import tpu as pltpu
from jax.sharding import PartitionSpec as P

MASK_ID = 32
PAD_ID = 1
NCLS = 32
LN_EPS = 1e-5
ROPE_BASE = 10000.0
TRAIN_RATIO = 0.15 * 0.8
NEG_BIG = -1e30
CORE, XDIR, YDIR = 1, 2, 4
ZDIR = 0
XY, YX = (XDIR, YDIR), (YDIR, XDIR)
BF = jnp.bfloat16
F32 = jnp.float32
VMEM_LIMIT = 67043328
NN = (((1,), (0,)), ((), ()))
NT = (((1,), (1,)), ((), ()))
TN = (((0,), (0,)), ((), ()))
FTILE = 512
N_PIECE = 8
FWD_HEADS = 10
MESH_ID = pl.DeviceIdType.MESH
FWD_PLAN = ("1:d0", "2:e0f0", "5:d1", "7:e1f1")
FFN_PLAN = ("4:asbs,6:a0b0,8:csds,9:a1b1,10:c0d0,11:a2b2,12:esfs", "13:c1d1,14:a3b3e0f0,15:c2d2,17:e1f1,18:c3d3e2f2,19:e3f3")
BWD_PLAN = ("2:a0b0,4:c0d0,8:vs,9:a1b1,10:o0v0,15:c1d1,16:ws,18:a2b2w0", "22:v1,24:xs,25:o1,26:x0,28:c2d2,30:a3b3,32:ys,34:y0w1",
            "35:v2x1,36:o2,38:c3d3")
BWD_TAIL = "zs,z0k0,y1w2x2,k1,z1y2v3o3,k2,z2w3x3,y3,k3,z3"


def mm(a, b, dims):
    return lax.dot_general(a, b, dims, preferred_element_type=F32)


def rmean(x):
    return jnp.mean(x, axis=-1, keepdims=True)


def csum(x):
    return jnp.sum(x, axis=0, keepdims=True)


def normalize(x):
    cen = x - rmean(x)
    rstd = lax.rsqrt(rmean(cen * cen) + LN_EPS)
    return cen * rstd, rstd


def norm_pull(dn, gain, xh, rstd):
    dy = dn * gain
    return rstd * (dy - rmean(dy) - xh * rmean(dy * xh))


def cat(parts):
    return jnp.concatenate(parts, axis=0)


def split3(x):
    hi = x.astype(BF)
    rest = x - hi.astype(F32)
    mid = rest.astype(BF)
    lo = (rest - mid.astype(F32)).astype(BF)
    return hi, mid, lo


def row_iota(rows, width):
    return lax.broadcasted_iota(jnp.int32, (rows, width), 0)


def one_hot_rows(cls):
    return (row_iota(NCLS, cls.shape[-1]) == cls).astype(BF)


def stack_rows(parts, width):
    row = row_iota(16, width)
    out = jnp.zeros(row.shape, F32)
    for i, part in enumerate(parts):
        out = jnp.where(row == i, part, out)
    return out.astype(BF)


def key_rows(pos, length):
    return stack_rows([jnp.where(pos < length, 0.0, NEG_BIG)] + [1.0] * 3, pos.shape[-1])


def rope_fwd(lo, hi, cos, sin):
    return cat([lo * cos - hi * sin, hi * cos + lo * sin])


def place():
    z, me = lax.axis_index('cp'), lax.axis_index('fsdp')
    bit = {CORE: lax.rem(me, XDIR), XDIR: lax.rem(me // XDIR, XDIR), YDIR: me // YDIR}
    partner = {way: (z, me + way - 2 * way * bit[way]) for way in bit}
    partner[ZDIR] = (1 - z, me)
    return bit, partner


def greet(partner):
    barrier = pltpu.get_barrier_semaphore()
    for way in partner:
        pl.semaphore_signal(barrier, inc=1, device_id=partner[way], device_id_type=MESH_ID)
    pl.semaphore_wait(barrier, len(partner))


def clean_table(ref):
    return jnp.where(row_iota(NCLS, ref.shape[1]) == PAD_ID, 0.0, ref[:NCLS, :].astype(F32))


class Stream:
    def __init__(self, num, order, src, bufs, out, sems, loc, own=None):
        self.num, self.order, self.src, self.bufs, self.out = num, order, src, bufs, out
        self.sems, self.loc, self.own = sems, loc, own

    def pick(self, stage, bit):
        way = self.order[stage - 1]
        buf = self.bufs[stage - 1]
        return buf.at[:, bit] if stage == 1 and way == XDIR else buf.at[bit]

    def copy(self, stage):
        bit, partner = self.loc
        way = (CORE, *self.order, ZDIR)[stage]
        if stage == 0:
            src = self.src(1 - bit[CORE])
        elif way == ZDIR:
            src = self.bufs[stage - 1]
        else:
            src = self.pick(stage, 1 - bit[way])
        return pltpu.make_async_remote_copy(
            src_ref=src, dst_ref=self.bufs[stage], send_sem=self.sems[0].at[self.num, stage],
            recv_sem=self.sems[1].at[self.num, stage], device_id=partner[way], device_id_type=MESH_ID)

    def local(self):
        return pltpu.make_async_copy(self.src(self.loc[0][CORE]), *self.own)

    def start(self):
        self.copy(0).start()
        if self.own:
            self.local().start()

    def advance(self, stage):
        bit = self.loc[0]
        buf = self.bufs[stage]
        self.copy(stage).wait()
        if stage == 0:
            if self.own:
                self.local().wait()
            buf[...] += self.own[0][...] if self.own else self.src(bit[CORE])[...]
        elif stage <= len(self.order):
            buf[...] += self.pick(stage, bit[self.order[stage - 1]])[...]
        else:
            self.out[...] = self.bufs[stage - 1][...] + buf[...]
            return
        self.copy(stage + 1).start()


class AllSum:
    def __init__(self, ref, bufs, sems, loc):
        self.ref, self.bufs, self.sems, self.loc = ref, bufs, sems, loc
        self.ways = (CORE, XDIR, YDIR, ZDIR)

    def copy(self, stage):
        return pltpu.make_async_remote_copy(
            src_ref=self.ref, dst_ref=self.bufs.at[stage], send_sem=self.sems[0].at[stage], recv_sem=self.sems[1].at[stage],
            device_id=self.loc[1][self.ways[stage]], device_id_type=MESH_ID)

    def start(self):
        self.copy(0).start()

    def advance(self, stage):
        self.copy(stage).wait()
        self.ref[...] += self.bufs[stage]
        if stage + 1 < len(self.ways):
            self.copy(stage + 1).start()


class Gather:
    def __init__(self, num, order, own, full, sems, loc, me):
        self.order, self.own, self.full, self.loc, self.me = order, own, full, loc, me
        self.send, self.recv, self.here = [sem.at[num] for sem in sems]

    def copies(self, stage):
        bit, partner = self.loc
        held, first = [self.me], 0
        for way in self.order[:stage]:
            first += len(held)
            held += [piece + way - 2 * way * bit[way] for piece in held]
        way = (*self.order, CORE)[stage]
        return [pltpu.make_async_remote_copy(
            src_ref=self.full(piece) if i else self.own, dst_ref=self.full(piece), send_sem=self.send.at[first + i],
            recv_sem=self.recv.at[first + i], device_id=partner[way], device_id_type=MESH_ID) for i, piece in enumerate(held)]

    def local(self):
        return pltpu.make_async_copy(self.own, self.full(self.me), self.here)

    def start(self, stage=0):
        if stage == 0:
            self.local().start()
        for copy in self.copies(stage):
            copy.start()

    def finish(self, stage):
        for copy in self.copies(stage):
            copy.wait()
        if stage == len(self.order):
            self.local().wait()

    def advance(self, stage):
        self.finish(stage)
        if stage < len(self.order):
            self.start(stage + 1)


def act(streams, text):
    for name, what in zip(text[::2], text[1::2]):
        if what == "s":
            streams[name].start()
        else:
            streams[name].advance(int(what))


def follow(plan, tick, streams):
    for item in ",".join(plan).split(","):
        when, text = item.split(":")

        @pl.when(tick == int(when))
        def _(text=text):
            act(streams, text)


def attn_fwd_kernel(n_heads, hd, lens, tok_ref, emb_ref, cos_ref, sin_ref, small_ref, wq_own, wo_own, wu_own, wd_own, grad_ref,
                    qkv_ref, o_ref, lse_ref, cls_ref, scale_ref, ec_ref, hc_ref, small_out, vecs_ref,
                    wq_out, wo_ref, wu_ref, wd_ref, gp_ref, class_scr, lin_scr, wu_scr, tok_scr, small_all, wq_ref,
                    send_sem, recv_sem, here_sem, swap_send, swap_recv, put_sem):
    step = pl.program_id(0)
    dim = n_heads * hd
    loc = place()
    z, me = lax.axis_index('cp'), lax.axis_index('fsdp')
    n_seq = tok_scr.shape[0]
    seq_half = tok_scr.shape[1]
    slen = 2 * seq_half
    mine, other = [pl.ds(pl.multiple_of(zz * n_seq, n_seq), n_seq) for zz in (z, 1 - z)]
    sems = (send_sem, recv_sem, here_sem)
    cut = 48
    streams = {}
    for name, order, own, full in (
            ("a", XY, small_ref, lambda f: small_all.at[f]),
            ("b", XY, wq_own.at[:cut], lambda f: wq_ref.at[f, :cut]),
            ("c", YX, wq_own.at[cut:], lambda f: wq_ref.at[f, cut:]),
            ("d", XY, wo_own, lambda f: wo_ref.at[f]),
            ("e", XY, wu_scr, lambda f: wu_ref.at[f]),
            ("f", YX, wd_own, lambda f: wd_ref.at[:, f])):
        streams[name] = Gather(len(streams), order, own, full, sems, loc, me)

    def swap(num, src, dst):
        return pltpu.make_async_remote_copy(src_ref=src, dst_ref=dst, send_sem=swap_send.at[num], recv_sem=swap_recv.at[num],
                                            device_id=loc[1][ZDIR], device_id_type=MESH_ID)

    swaps = [swap(0, tok_ref.at[other], tok_scr), swap(1, grad_ref.at[other], gp_ref)]
    keep = pltpu.make_async_copy(wq_ref, wq_out, put_sem)
    lane = lax.broadcasted_iota(jnp.int32, (1, slen), 1)
    pos = jnp.where(lane < seq_half, z * seq_half + lane, lane - z * seq_half)

    @pl.when(step == 0)
    def _():
        greet(loc[1])
        for copy in swaps:
            copy.start()
        act(streams, "asbscs")
        x = wu_own[...]
        n_slab = FTILE // N_PIECE
        slabs = x.shape[1] // FTILE
        wu_scr[...] = jnp.concatenate(
            [x[:, (f * slabs + j) * n_slab:(f * slabs + j + 1) * n_slab] for j in range(slabs) for f in range(N_PIECE)], axis=1)
        act(streams, "a0b0c0dsesfsa1")
        swaps[0].wait()
        tok = jnp.concatenate([tok_ref[mine, :], tok_scr[...]], axis=1)
        row = row_iota(n_seq, 1)
        length = jnp.zeros(row.shape, jnp.int32)
        for i in range(n_seq):
            length = jnp.where(row == i, lens[z * n_seq + i], length)
        masked = tok == MASK_ID
        count = jnp.sum(jnp.where(masked, 1.0, 0.0), axis=-1, keepdims=True)
        scale = (1.0 - TRAIN_RATIO) / (1.0 - count / length.astype(F32))
        scale_ref[...] = scale
        cls = jnp.where(masked | (pos >= length), PAD_ID, tok)
        emb = clean_table(emb_ref)
        for i in range(n_seq):
            cls_ref[i] = cls[i:i + 1]
            ec_ref[i * NCLS:(i + 1) * NCLS, :] = emb * scale[i:i + 1]
        act(streams, "a2")
        vecs_ref[...] = jnp.concatenate([small_all[f] for f in range(N_PIECE)], axis=1)
        hc_ref[...] = (normalize(ec_ref[...])[0] * vecs_ref[0:1, :] + vecs_ref[1:2, :]).astype(BF)
        small_out[...] = small_all[...]
        act(streams, "b1c1b2c2")
        keep.start()
        full = mm(hc_ref[...], wq_ref[...].reshape(dim, 3 * dim), NN)
        for part in range(3):
            cols = slice(part * dim, (part + 1) * dim)
            val = full[:, cols] + vecs_ref[2 + part:3 + part, :]
            class_scr[:, cols] = val if part else val * hd ** -0.5

    follow(FWD_PLAN, step, streams)
    rows = class_scr[pl.ds(step * NCLS, NCLS), :]
    hot = one_hot_rows(cls_ref[step])
    hot3 = cat([hot] * 3)
    for part in range(3):
        cols = slice(part * dim, (part + 1) * dim)
        lin_scr[cols, :] = mm(cat(split3(rows[:, cols])), hot3, TN)
    kx = key_rows(pos, lens[z * n_seq + step])
    qx = stack_rows([1.0], kx.shape[-1])
    cos, sin = cos_ref[...], sin_ref[...]
    half = hd // 2

    def heads(hs):
        bases = [pl.multiple_of(h * hd, hd) for h in hs]
        qs, ks, vs = [], [], []
        for base in bases:
            piece = lambda off, size: lin_scr[pl.ds(base + off, size), :]
            qs.append(rope_fwd(piece(0, half), piece(half, half), cos, sin).astype(BF))
            ks.append(rope_fwd(piece(dim, half), piece(dim + half, half), cos, sin).astype(BF))
            vs.append(piece(2 * dim, hd).astype(BF))
            for part, val in enumerate((qs[-1], ks[-1], vs[-1])):
                qkv_ref[0, pl.ds(part * dim + base, hd), :] = val
        ss = [mm(cat([k, kx]), cat([q, qx]), TN) for q, k in zip(qs, ks)]
        tops = [jnp.max(s, axis=0, keepdims=True) for s in ss]
        ps = [jnp.exp(s - t) for s, t in zip(ss, tops)]
        tots = [csum(p) for p in ps]
        os = [mm(v, p.astype(BF), NN) for v, p in zip(vs, ps)]
        for h, base, o, tot, top in zip(hs, bases, os, tots, tops):
            o_ref[0, pl.ds(base, hd), :] = o / tot
            lse_ref[0, pl.ds(h, 1), :] = top + jnp.log(tot)

    def body(i, carry):
        heads([i * FWD_HEADS + u for u in range(FWD_HEADS)])
        return carry

    lax.fori_loop(0, n_heads // FWD_HEADS, body, 0)

    @pl.when(step == n_seq - 1)
    def _():
        act(streams, "d2e2f2")
        swaps[1].wait()
        keep.wait()


def ffn_kernel(n_heads, hd, nsq, slen, keep_tiles,
               scale_ref, cls_ref, o_ref, grad_ref, gp_ref, et_ref, vecs_ref, bup_ref, wo_ref, wu_ref, wd_ref,
               outm_ref, outp_ref, do_ref, delta_ref, csum_ref, dvec_ref, dbup_ref, dwo_ref, gu_ref, gd_ref, ru_ref, rd_ref,
               xh_scr, rs_scr, n_scr, g_scr, y_scr, dn_scr, au_scr, ad_scr, u0, u1, u2, u3, d0, d1, d2, d3,
               send_sem, recv_sem, out_sem, grad_sem):
    tile, blk = pl.program_id(0), pl.program_id(1)
    n_tile, n_blk = pl.num_programs(0), pl.num_programs(1)
    tick = tile * n_blk + blk
    first, last = tile == 0, tile == n_tile - 1
    halfs = slen // 2
    n_rows = nsq * slen
    rows = pl.ds(pl.multiple_of(blk * n_rows, n_rows), n_rows)
    loc = place()
    sems = (send_sem, recv_sem)
    streams = {}
    for t in range(keep_tiles):
        for kind, (order, acc, bufs, out) in enumerate(((XY, au_scr, (u0, u1, u2, u3), ru_ref), (YX, ad_scr, (d0, d1, d2, d3), rd_ref))):
            streams["abcdef"[2 * t + kind]] = Stream(
                2 * t + kind, order, (lambda c, acc=acc, t=t: acc.at[t, :, :, c]), tuple(b.at[t] for b in bufs), out.at[t], sems, loc)

    def handed(t):
        return [pltpu.make_async_copy(acc.at[keep_tiles + t], out.at[t], out_sem.at[2 * t + kind])
                for kind, (acc, out) in enumerate(((au_scr, gu_ref), (ad_scr, gd_ref)))]

    n_seq = g_scr.shape[0]
    z = lax.axis_index('cp')
    loads = [pltpu.make_async_copy(src, g_scr.at[:, part], grad_sem.at[part])
             for part, src in enumerate((grad_ref.at[pl.ds(pl.multiple_of(z * n_seq, n_seq), n_seq)], gp_ref))]

    @pl.when(tick == 0)
    def _():
        for load in loads:
            load.start()
        greet(loc[1])
        dvec_ref[...] = jnp.zeros_like(dvec_ref)
        dbup_ref[...] = jnp.zeros_like(dbup_ref)
        dwo_ref[...] = jnp.zeros_like(dwo_ref)

    follow(FFN_PLAN, tick, streams)

    @pl.when(tick == (n_tile - 1) * n_blk)
    def _():
        for copy in handed(0):
            copy.start()

    @pl.when(first)
    def _():
        for i in range(nsq):
            r = pl.ds(pl.multiple_of(blk * n_rows + i * slen, slen), slen)
            e = mm(one_hot_rows(cls_ref[i]), clean_table(et_ref).astype(BF), TN) * scale_ref[pl.ds(blk * nsq + i, 1), :]
            x1 = e + mm(o_ref[i].astype(BF), wo_ref[...], TN) + vecs_ref[5:6, :]
            xh, rstd = normalize(x1)
            xh_scr[r, :] = xh
            rs_scr[r, :] = rstd
            y_scr[r, :] = x1 + vecs_ref[8:9, :]
            n_scr[r, :] = (xh * vecs_ref[6:7, :] + vecs_ref[7:8, :]).astype(BF)
        dn_scr[rows, :] = jnp.zeros_like(dn_scr[rows, :])

    @pl.when(tick == 0)
    def _():
        for load in loads:
            load.wait()

    @pl.when(blk == 0)
    def _():
        au_scr[tile] = jnp.zeros(au_scr.shape[1:], F32)
        ad_scr[tile] = jnp.zeros(ad_scr.shape[1:], F32)

    n = n_scr[rows, :]
    g = g_scr[pl.ds(blk * nsq, nsq)].reshape(n_rows, -1)
    wu = wu_ref[...]
    wd = wd_ref[...]
    cols = pl.ds(pl.multiple_of(tile * wu.shape[1], wu.shape[1]), wu.shape[1])
    u = mm(n, wu, NN) + bup_ref[:, cols]
    phi = 0.5 + 0.5 * lax.erf(u * 0.7071067811865476)
    a = (u * phi).astype(BF)
    slope = phi + u * (jnp.exp(-0.5 * u * u) * 0.3989422804014327)
    y_scr[rows, :] += mm(a, wd, NN)
    du = mm(g, wd, NT) * slope
    dub = du.astype(BF)
    dbup_ref[:, cols] += csum(du)
    ad_scr[tile] += mm(a, g, TN).reshape(ad_scr.shape[1:])
    au_scr[tile] += mm(n, dub, TN).reshape(au_scr.shape[1:])
    dn_scr[rows, :] += mm(dub, wu, NT)

    @pl.when(last)
    def _():
        for i in range(nsq):
            r = pl.ds(pl.multiple_of(blk * n_rows + i * slen, slen), slen)
            out = y_scr[r, :].astype(BF)
            outm_ref[i] = out[:halfs]
            outp_ref[i] = out[halfs:]
            dn = dn_scr[r, :]
            xh = xh_scr[r, :]
            g32 = g_scr[blk * nsq + i].reshape(slen, -1).astype(F32)
            dx = g32 + norm_pull(dn, vecs_ref[6:7, :], xh, rs_scr[r, :])
            dvec_ref[...] += cat([csum(dx), csum(dn * xh), csum(dn), csum(g32)])
            dxb = dx.astype(BF)
            o = o_ref[i]
            dwo_ref[...] += mm(o.astype(BF), dxb, NN)
            do = mm(wo_ref[...], dxb, NT)
            do_ref[i] = do.astype(BF)
            delta_ref[i] = jnp.sum((do * o).reshape(n_heads, hd, slen), axis=1)
            csum_ref[i] = mm(one_hot_rows(cls_ref[i]), dxb, NN)

    @pl.when(tick == n_tile * n_blk - 1)
    def _():
        for copy in handed(1):
            copy.start()
        for copy in handed(0) + handed(1):
            copy.wait()


def attn_bwd_kernel(hd, nh, lens, scale_ref, cls_ref, cos_ref, sin_ref, qkv_ref, do_ref, lse_ref, delta_ref, hc_ref,
                    wq_ref, wk_ref, wv_ref, csum_ref, ec_ref, vecs_ref, dvb_ref, dbup_ref, gu_ref, gd_ref, go_ref,
                    ru_ref, rd_ref, ro_ref, rw_ref, rs_ref,
                    dlin_scr, bsum_scr, dcls_scr, dn_scr, dw_scr, small_scr, small_in,
                    u_own, d_own, o_own, u0, u1, u2, u3, d0, d1, d2, d3, o0, o1, o2, o3, w0, w1, w2, w3,
                    send_sem, recv_sem, own_sem, ssend, srecv):
    group, seq = pl.program_id(0), pl.program_id(1)
    n_group, n_seq = pl.num_programs(0), pl.num_programs(1)
    tick = group * n_seq + seq
    gdim = nh * hd
    half = hd // 2
    loc = place()
    sems = (send_sem, recv_sem)
    streams = {"k": AllSum(small_scr, small_in, (ssend, srecv), loc)}
    for t in range(gu_ref.shape[0]):
        for kind, (order, src, own, bufs, out) in enumerate(((XY, gu_ref, u_own, (u0, u1, u2, u3), ru_ref),
                                                             (YX, gd_ref, d_own, (d0, d1, d2, d3), rd_ref))):
            num = 2 * t + kind
            streams["abcd"[num]] = Stream(num, order, (lambda c, src=src, t=t: src.at[t, :, :, c]), tuple(b.at[t] for b in bufs),
                                          out.at[t], sems, loc, (own.at[t], own_sem.at[num]))
    num = own_sem.shape[0] - 1
    streams["o"] = Stream(num, YX, lambda c: go_ref.at[:, :, c], (o0, o1, o2, o3), ro_ref, sems, loc, (o_own, own_sem.at[num]))
    for t in range(rw_ref.shape[0]):
        streams["vwxyz"[t]] = Stream(num + 1 + t, (XY, YX)[t % 2], (lambda c, t=t: dw_scr.at[t, :, :, c]),
                                     tuple(b.at[t] for b in (w0, w1, w2, w3)), rw_ref.at[t], sems, loc)

    @pl.when(tick == 0)
    def _():
        greet(loc[1])
        act(streams, "asbscsdsos")
        dn_scr[...] = jnp.zeros_like(dn_scr)
        small_scr[...] = jnp.zeros_like(small_scr)

    follow(BWD_PLAN, tick, streams)

    @pl.when(seq == 0)
    def _():
        bsum_scr[...] = jnp.zeros_like(bsum_scr)

    width = cos_ref.shape[-1]
    z = lax.axis_index('cp')
    lane = lax.broadcasted_iota(jnp.int32, (1, width), 1)
    pos = jnp.where(lane < width // 2, z * (width // 2) + lane, lane - z * (width // 2))
    kx = key_rows(pos, lens[z * n_seq + seq])
    vx = stack_rows([1.0] * 3, width)
    cos, sin = cos_ref[...], sin_ref[...]

    def put(base, val):
        dlin_scr[base:base + hd, :] = val.astype(BF)
        bsum_scr[base:base + hd, :] += val[:, :width // 2] + val[:, width // 2:]

    def unrope(val):
        return rope_fwd(val[:half], val[half:], cos, -sin)

    def extra(ref, h):
        return [t.astype(F32) for t in split3(-ref[0, pl.ds(group * nh + h, 1), :])]

    hs = range(nh)
    span = [slice(h * hd, (h + 1) * hd) for h in hs]
    qs, ks, vs = [[qkv_ref[0, part, span[h], :] for h in hs] for part in range(3)]
    dos = [do_ref[0, span[h], :] for h in hs]
    ss = [mm(cat([ks[h], kx]), cat([qs[h], stack_rows([1.0] + extra(lse_ref, h), width)]), TN) for h in hs]
    dps = [mm(cat([vs[h], vx]), cat([dos[h], stack_rows(extra(delta_ref, h), width)]), TN) for h in hs]
    ps = [jnp.exp(s) for s in ss]
    pbs = [p.astype(BF) for p in ps]
    dss = [(p * dp).astype(BF) for p, dp in zip(ps, dps)]
    dvs = [mm(dos[h], pbs[h], NT) for h in hs]
    dks = [mm(qs[h], dss[h], NT) for h in hs]
    dqs = [mm(ks[h], dss[h], NN) for h in hs]
    for h in hs:
        put(h * hd, unrope(dqs[h]) * hd ** -0.5)
        put(gdim + h * hd, unrope(dks[h]))
        put(2 * gdim + h * hd, dvs[h])

    dcls_scr[pl.ds(pl.multiple_of(seq * NCLS, NCLS), NCLS), :] = mm(one_hot_rows(cls_ref[0]), dlin_scr[...], NT)

    @pl.when(seq == n_seq - 1)
    def _():
        hc = hc_ref[...]
        acc = dcls_scr[...]
        hi, lo, _ = split3(acc)
        dw_scr[group] = mm(cat([hc, hc]), cat([hi, lo]), TN).reshape(dw_scr.shape[1:])
        dn = dn_scr[...]
        cols = pl.ds(pl.multiple_of(group * gdim, gdim), gdim)
        bias = csum(jnp.transpose(bsum_scr[...]))
        for part, w_ref in enumerate((wq_ref, wk_ref, wv_ref)):
            sel = slice(part * gdim, (part + 1) * gdim)
            dn = dn + mm(hi[:, sel], w_ref[...], NT) + mm(lo[:, sel], w_ref[...], NT)
            small_scr[2 + part:3 + part, cols] = bias[:, sel]
        dn_scr[...] = dn

    @pl.when(tick == n_group * n_seq - 1)
    def _():
        tail = BWD_TAIL.split(",")
        act(streams, tail[0])
        dn = dn_scr[...]
        xh, rstd = normalize(ec_ref[...])
        de = norm_pull(dn, vecs_ref[0:1, :], xh, rstd)
        small_scr[0:2, :] = cat([csum(dn * xh), csum(dn)])
        small_scr[5:13, :] = cat([dvb_ref[...], dbup_ref[...]])
        tab = jnp.zeros((NCLS, dn.shape[1]), F32)
        for b in range(dcls_scr.shape[0] // NCLS):
            tab = tab + (de[b * NCLS:(b + 1) * NCLS] + csum_ref[b]) * scale_ref[b:b + 1, :]
        small_scr[16:, :] = jnp.where(row_iota(*tab.shape) == PAD_ID, 0.0, tab)
        act(streams, "ks")
        for text in tail[1:]:
            act(streams, text)
        rs_ref[...] = small_scr[...]


def whole(shape):
    return pl.BlockSpec(shape, lambda *_: (0,) * len(shape), pipeline_mode=pl.Buffered(1))


def params(**kw):
    return pltpu.CompilerParams(vmem_limit_bytes=VMEM_LIMIT, **kw)


def cost(flops, moved):
    return pl.CostEstimate(flops=flops * 10**9, bytes_accessed=moved * 10**6, transcendentals=0)


def sds(*t):
    return jax.ShapeDtypeStruct(t, F32)


def sdb(*t):
    return jax.ShapeDtypeStruct(t, BF)


def vm(*t):
    return pltpu.VMEM(t, F32)


def dma(*t):
    return pltpu.SemaphoreType.DMA(t)


def stages(lead, *t):
    return [vm(*lead, 2, 2, *t), vm(*lead, 2, *t), vm(*lead, *t), vm(*lead, *t)]


SMEM = pl.BlockSpec(memory_space=pltpu.SMEM)


def attn_fwd(lens, tokens, embed, cos, sin, small, wq, wo, wu, wd, grad):
    n_seq, seq_half = tokens.shape[0] // 2, tokens.shape[1]
    slen = 2 * seq_half
    dim = wo.shape[1]
    hd = 2 * cos.shape[0]
    n_heads = dim // hd
    row = lambda *t: pl.BlockSpec((1,) + t, lambda i: (i, 0, 0))
    anyspace = pl.BlockSpec(memory_space=pl.ANY)
    held = [(jnp.int32, (n_seq, 1, slen)), (F32, (n_seq, 1)), (F32, (n_seq * NCLS, dim)), (BF, (n_seq * NCLS, dim)),
            (F32, (N_PIECE, *small.shape)), (F32, (small.shape[0], dim))]
    far = [(N_PIECE, *wq.shape), (N_PIECE, *wo.shape), (N_PIECE, *wu.shape), (wd.shape[0], N_PIECE, *wd.shape[1:]), (n_seq, *grad.shape[1:])]
    args = (tokens, embed, cos, sin, small, wq, wo, wu, wd)
    return pl.pallas_call(
        functools.partial(attn_fwd_kernel, n_heads, hd),
        grid=(n_seq,),
        in_specs=[SMEM, *[whole(t.shape) for t in args], anyspace],
        out_specs=[row(3 * dim, slen), row(dim, slen), row(n_heads, slen), *[whole(t) for _, t in held], *[anyspace] * len(far)],
        out_shape=[sdb(n_seq, 3 * dim, slen), sds(n_seq, dim, slen), sds(n_seq, n_heads, slen),
                   *[jax.ShapeDtypeStruct(t, kind) for kind, t in held], *[sdb(*t) for t in far]],
        scratch_shapes=[vm(n_seq * NCLS, 3 * dim), vm(3 * dim, slen), pltpu.VMEM(wu.shape, BF),
                        pltpu.VMEM((n_seq, seq_half), jnp.int32), vm(N_PIECE, *small.shape),
                        pltpu.VMEM((N_PIECE, *wq.shape), BF), dma(6, 7), dma(6, 7), dma(6), dma(2), dma(2), pltpu.SemaphoreType.DMA],
        compiler_params=params(collective_id=2, has_side_effects=True), name="attn_fwd", cost_estimate=cost(20, 18),
    )(lens, *args, grad)


def ffn(scales, cls, o, grad, gp, etab, vecs, bup, wo, wu, wd, n_heads, hd, nsq=2, keep_tiles=3):
    n_seq, _, slen = cls.shape
    dim, ff = wu.shape
    tiles = ff // FTILE
    rest = tiles - keep_tiles
    halfs = slen // 2
    piece, slab = dim // N_PIECE, FTILE // N_PIECE
    n_blk = n_seq // nsq
    n_rows = n_seq * slen

    def blk(when, *t):
        return pl.BlockSpec((nsq,) + t, lambda j, r: (jnp.where(when(j), r, when(0) * (n_blk - 1)),) + (0,) * len(t))

    late = lambda j: j == tiles - 1
    both = lambda j: (j == 0) | (j == tiles - 1)
    anyspace = pl.BlockSpec(memory_space=pl.ANY)
    cube = (2,) * 3
    bwd_u, bwd_d = (rest, *cube, piece, FTILE), (rest, *cube, slab, dim)
    red_u, red_d = (keep_tiles, piece, FTILE), (keep_tiles, slab, dim)
    return pl.pallas_call(
        functools.partial(ffn_kernel, n_heads, hd, nsq, slen, keep_tiles),
        grid=(tiles, n_blk),
        in_specs=[whole(scales.shape), blk(both, 1, slen), blk(both, dim, slen), anyspace, anyspace,
                  whole(etab.shape), whole(vecs.shape), whole(bup.shape), whole(wo.shape),
                  pl.BlockSpec((dim, FTILE), lambda j, r: (0, j)), pl.BlockSpec((FTILE, dim), lambda j, r: (j, 0))],
        out_specs=[blk(late, halfs, dim), blk(late, halfs, dim), blk(late, dim, slen), blk(late, n_heads, slen),
                   blk(late, NCLS, dim), whole((4, dim)), whole((1, ff)), whole((dim, dim)), anyspace, anyspace,
                   whole(red_u), whole(red_d)],
        out_shape=[sdb(n_seq, halfs, dim), sdb(n_seq, halfs, dim), sdb(n_seq, dim, slen), sds(n_seq, n_heads, slen),
                   sds(n_seq, NCLS, dim), sds(4, dim), sds(1, ff), sds(dim, dim), sds(*bwd_u), sds(*bwd_d), sds(*red_u), sds(*red_d)],
        scratch_shapes=[vm(n_rows, dim), vm(n_rows, 1), pltpu.VMEM((n_rows, dim), BF), pltpu.VMEM((n_seq, 2, halfs, dim), BF),
                        vm(n_rows, dim), vm(n_rows, dim), vm(tiles, *cube, piece, FTILE), vm(tiles, *cube, slab, dim)]
        + stages((keep_tiles,), piece, FTILE) + stages((keep_tiles,), slab, dim)
        + [dma(2 * keep_tiles, 4), dma(2 * keep_tiles, 4), dma(2 * rest), dma(2)],
        compiler_params=params(collective_id=1, has_side_effects=True), name="ffn", cost_estimate=cost(60, 40),
    )(scales, cls, o, grad, gp, etab, vecs, bup, wo, wu, wd)


def attn_bwd(lens, scales, cls, cos, sin, qkv, do, lse, delta, hc, w, csums, ec, vecs, dvec_b, d_bup, d_wu, d_wd, d_wo,
             n_heads, hd, groups=5):
    n_seq, _, slen = cls.shape
    dim = n_heads * hd
    nh = n_heads // groups
    gdim = nh * hd
    cube = (2,) * 3
    blk = lambda *t: pl.BlockSpec((1,) + t, lambda g, i: (i,) + (0,) * len(t))
    wcol = lambda part: pl.BlockSpec((dim, gdim), lambda g, i: (0, part * groups + g))
    anyspace = pl.BlockSpec(memory_space=pl.ANY)
    ut, dt, ot = d_wu.shape[-2:], d_wd.shape[-2:], (dim // N_PIECE, dim)
    wt = (dim // N_PIECE, 3 * gdim)
    rest = d_wu.shape[0]
    fixed = (hc, csums, ec, vecs, dvec_b, d_bup.reshape(-1, dim))
    args = [lens, scales, cls, cos, sin, qkv.reshape(n_seq, 3, dim, slen), do, lse, delta, hc, w, w, w, *fixed[1:],
            d_wu, d_wd, d_wo.reshape(*cube, *ot)]
    specs = [SMEM, whole(scales.shape), blk(1, slen), whole(cos.shape), whole(sin.shape),
             pl.BlockSpec((1, 3, gdim, slen), lambda g, i: (i, 0, g, 0)), pl.BlockSpec((1, gdim, slen), lambda g, i: (i, g, 0)),
             blk(n_heads, slen), blk(n_heads, slen), whole(hc.shape), *[wcol(part) for part in range(3)],
             *[whole(t.shape) for t in fixed[1:]], *[anyspace] * 3]
    small = (16 + NCLS, dim)
    shapes = [sds(rest, *ut), sds(rest, *dt), sds(*ot), sds(groups, *wt), sds(*small)]
    n_str = 2 * rest + 1
    return pl.pallas_call(
        functools.partial(attn_bwd_kernel, hd, nh),
        grid=(groups, n_seq),
        in_specs=specs,
        out_specs=[whole(t.shape) for t in shapes],
        out_shape=shapes,
        scratch_shapes=[pltpu.VMEM((3 * gdim, slen), BF), vm(3 * gdim, slen // 2), vm(n_seq * NCLS, 3 * gdim),
                        vm(n_seq * NCLS, dim), vm(groups, *cube, *wt), vm(*small), vm(4, *small),
                        vm(rest, 2, 2, *ut), vm(rest, 2, 2, *dt), vm(2, 2, *ot)]
        + stages((rest,), *ut) + stages((rest,), *dt) + stages((), *ot) + stages((groups,), *wt)
        + [dma(n_str + groups, 4), dma(n_str + groups, 4), dma(n_str), dma(4), dma(4)],
        compiler_params=params(collective_id=0, has_side_effects=True), name="attn_bwd", cost_estimate=cost(40, 20),
    )(*args)


def rope_tables(slen, hd):
    inv_freq = 1.0 / (ROPE_BASE ** (jnp.arange(0, hd, 2, dtype=F32) / hd))
    half = slen // 2
    turn = jnp.arange(slen).reshape(2, half)
    cp_index = lax.axis_index('cp')
    pos = jnp.where(cp_index == 0, turn, turn[::-1]).reshape(slen)
    angles = inv_freq[:, None] * pos.astype(F32)[None, :]
    return jnp.cos(angles), jnp.sin(angles)


def solution(mesh):
    swap = [(0, 1), (1, 0)]
    n_fsdp = mesh.shape['fsdp']

    def local_step(tokens, lengths, embed_table, layer_vecs, w_qkv, w_out, w_up, b_up, w_down, grad_out):
        cp_index = lax.axis_index('cp')
        me = lax.axis_index('fsdp')
        vocab, dim = embed_table.shape
        n_heads, hd = w_qkv.shape[2], w_qkv.shape[3]
        slabs = w_up.shape[1] // FTILE
        cos_t, sin_t = rope_tables(2 * tokens.shape[1], hd)
        small = jnp.concatenate([layer_vecs, b_up.reshape(-1, layer_vecs.shape[1])], 0)
        small = jnp.pad(small, ((0, 16 - small.shape[0]), (0, 0)))
        (qkv, o, lse, cls, scales, e_cls, hc, small_all, vecs, w_all, out_w, up_w, down_w, g_peer) = attn_fwd(
            lengths, tokens, embed_table, cos_t, sin_t, small, w_qkv.reshape(w_qkv.shape[0], -1), w_out, w_up,
            w_down.reshape(slabs, -1, dim), grad_out)
        up_b = jnp.swapaxes(small_all[:, 9:13].reshape(n_fsdp, slabs, -1), 0, 1).reshape(1, -1)
        (out_m, out_p, do, delta, csums, dvec_b, d_bup, d_wo, d_wu, d_wd, red_wu, red_wd) = ffn(
            scales, cls, o, grad_out, g_peer, embed_table, vecs, up_b, out_w.reshape(dim, dim), up_w.reshape(dim, -1),
            down_w.reshape(-1, dim), n_heads, hd)
        out_back = lax.ppermute(out_p, 'cp', swap)
        layer_out = jnp.where(cp_index == 0, jnp.concatenate([out_m, out_back], 0), jnp.concatenate([out_back, out_m], 0))
        rest_wu, rest_wd, red_wo, red_w, red_small = attn_bwd(
            lengths, scales, cls, cos_t, sin_t, qkv, do, lse, delta, hc, w_all.reshape(dim, -1), csums, e_cls, vecs, dvec_b, d_bup, d_wu, d_wd,
            d_wo, n_heads, hd)
        groups = red_w.shape[0]
        red_w = jnp.transpose(red_w.reshape(groups, -1, 3, n_heads // groups, hd), (1, 2, 0, 3, 4)).reshape(w_qkv.shape)
        d_vecs = lax.dynamic_slice_in_dim(red_small[:9], me * layer_vecs.shape[1], layer_vecs.shape[1], 1)
        d_bup = lax.dynamic_slice_in_dim(red_small[9:13].reshape(slabs, n_fsdp, -1), me, 1, 1).reshape(b_up.shape)
        red_wu = jnp.concatenate([red_wu, rest_wu], 0).reshape(slabs, -1, n_fsdp, FTILE // n_fsdp)
        d_wup = jnp.transpose(red_wu, (1, 2, 0, 3)).reshape(w_up.shape)
        d_wdown = jnp.concatenate([red_wd, rest_wd], 0).reshape(w_down.shape)
        d_table = jnp.concatenate([red_small[16:16 + NCLS], jnp.zeros((vocab - NCLS, dim), F32)], 0)
        return layer_out, d_table, d_vecs, red_w, red_wo, d_wup, d_bup, d_wdown

    in_specs = (P('fsdp', 'cp'), P('fsdp'), P(), P(None, 'fsdp'), P('fsdp', None, None, None), P('fsdp', None), P('fsdp', None), P('fsdp'), P('fsdp', None), P('fsdp', 'cp', None))
    out_specs = (P('fsdp', 'cp', None), P(), P(None, 'fsdp'), P('fsdp', None, None, None), P('fsdp', None), P('fsdp', None), P('fsdp'), P('fsdp', None))
    return jax.shard_map(local_step, mesh=mesh, in_specs=in_specs, out_specs=out_specs, check_vma=False)
```

```python
import functools

import jax
import jax.numpy as jnp
from jax import lax
from jax.experimental import pallas as pl
from jax.experimental.pallas import tpu as pltpu
from jax.sharding import PartitionSpec as P

MASK_ID = 32
PAD_ID = 1
NCLS = 32
LN_EPS = 1e-5
ROPE_BASE = 10000.0
TRAIN_RATIO = 0.15 * 0.8
NEG_BIG = -1e30
CORE, XDIR, YDIR = 1, 2, 4
ZDIR = 0
XY, YX = (XDIR, YDIR), (YDIR, XDIR)
BF = jnp.bfloat16
F32 = jnp.float32
VMEM_LIMIT = 67043328
NN = (((1,), (0,)), ((), ()))
NT = (((1,), (1,)), ((), ()))
TN = (((0,), (0,)), ((), ()))
FTILE = 512
N_PIECE = 8
FWD_HEADS = 10
MESH_ID = pl.DeviceIdType.MESH
FWD_PLAN = ("1:d0e0f0", "4:d1", "7:e1f1")
FFN_PLAN = ("4:asbs,5:a0b0,8:a1b1csds,9:c0d0,10:a2b2,12:c1d1esfs", "13:a3b3e0f0,14:c2d2,16:e1f1,17:c3d3,18:e2f2")
BWD_PLAN = ("1:a0b0,2:c0d0,4:vsa1b1,5:o0v0,7:c1d1,8:ws,9:a2b2w0,11:v1", "12:xso1,13:x0,14:c2d2,15:a3b3,16:ys,17:y0w1v2x1,18:o2",
            "19:c3d3v3w2")
BWD_TAIL = "zsqs,z0q0,y1x2,k0,z1q1,y2,k1,w3x3o3,z2q2,k2,y3,z3q3,k3"


def mm(a, b, dims):
    return lax.dot_general(a, b, dims, preferred_element_type=F32)


def rmean(x):
    return jnp.mean(x, axis=-1, keepdims=True)


def csum(x):
    return jnp.sum(x, axis=0, keepdims=True)


def normalize(x):
    cen = x - rmean(x)
    rstd = lax.rsqrt(rmean(cen * cen) + LN_EPS)
    return cen * rstd, rstd


def norm_pull(dn, gain, xh, rstd):
    dy = dn * gain
    return rstd * (dy - rmean(dy) - xh * rmean(dy * xh))


def cat(parts):
    return jnp.concatenate(parts, axis=0)


def split3(x):
    hi = x.astype(BF)
    rest = x - hi.astype(F32)
    mid = rest.astype(BF)
    lo = (rest - mid.astype(F32)).astype(BF)
    return hi, mid, lo


def row_iota(rows, width):
    return lax.broadcasted_iota(jnp.int32, (rows, width), 0)


def one_hot_rows(cls):
    return (row_iota(NCLS, cls.shape[-1]) == cls).astype(BF)


def stack_rows(parts, width):
    row = row_iota(16, width)
    out = jnp.zeros(row.shape, F32)
    for i, part in enumerate(parts):
        out = jnp.where(row == i, part, out)
    return out.astype(BF)


def key_rows(pos, length):
    return stack_rows([jnp.where(pos < length, 0.0, NEG_BIG)] + [1.0] * 3, pos.shape[-1])


def rope_fwd(lo, hi, cos, sin):
    return cat([lo * cos - hi * sin, hi * cos + lo * sin])


def place():
    z, me = lax.axis_index('cp'), lax.axis_index('fsdp')
    bit = {CORE: lax.rem(me, XDIR), XDIR: lax.rem(me // XDIR, XDIR), YDIR: me // YDIR}
    partner = {way: (z, me + way - 2 * way * bit[way]) for way in bit}
    partner[ZDIR] = (1 - z, me)
    return bit, partner


def greet(partner):
    barrier = pltpu.get_barrier_semaphore()
    for way in partner:
        pl.semaphore_signal(barrier, inc=1, device_id=partner[way], device_id_type=MESH_ID)
    pl.semaphore_wait(barrier, len(partner))


def clean_table(ref):
    return jnp.where(row_iota(NCLS, ref.shape[1]) == PAD_ID, 0.0, ref[:NCLS, :].astype(F32))


class Stream:
    def __init__(self, num, order, src, bufs, out, sems, loc, own=None):
        self.num, self.order, self.src, self.bufs, self.out = num, order, src, bufs, out
        self.sems, self.loc, self.own = sems, loc, own

    def pick(self, stage, bit):
        way = self.order[stage - 1]
        buf = self.bufs[stage - 1]
        return buf.at[:, bit] if stage == 1 and way == XDIR else buf.at[bit]

    def copy(self, stage):
        bit, partner = self.loc
        way = (CORE, *self.order, ZDIR)[stage]
        if stage == 0:
            src = self.src(1 - bit[CORE])
        elif way == ZDIR:
            src = self.bufs[stage - 1]
        else:
            src = self.pick(stage, 1 - bit[way])
        return pltpu.make_async_remote_copy(
            src_ref=src, dst_ref=self.bufs[stage], send_sem=self.sems[0].at[self.num, stage],
            recv_sem=self.sems[1].at[self.num, stage], device_id=partner[way], device_id_type=MESH_ID)

    def local(self):
        return pltpu.make_async_copy(self.src(self.loc[0][CORE]), *self.own)

    def start(self):
        self.copy(0).start()
        if self.own:
            self.local().start()

    def advance(self, stage):
        bit = self.loc[0]
        buf = self.bufs[stage]
        self.copy(stage).wait()
        if stage == 0:
            if self.own:
                self.local().wait()
            buf[...] += self.own[0][...] if self.own else self.src(bit[CORE])[...]
        elif stage <= len(self.order):
            buf[...] += self.pick(stage, bit[self.order[stage - 1]])[...]
        else:
            self.out[...] = self.bufs[stage - 1][...] + buf[...]
            return
        self.copy(stage + 1).start()


class AllSum:
    def __init__(self, ref, bufs, sems, loc):
        self.ref, self.bufs, self.sems, self.loc = ref, bufs, sems, loc
        self.ways = (CORE, XDIR, YDIR, ZDIR)

    def copy(self, stage):
        return pltpu.make_async_remote_copy(
            src_ref=self.ref, dst_ref=self.bufs.at[stage], send_sem=self.sems[0].at[stage], recv_sem=self.sems[1].at[stage],
            device_id=self.loc[1][self.ways[stage]], device_id_type=MESH_ID)

    def start(self):
        self.copy(0).start()

    def advance(self, stage):
        self.copy(stage).wait()
        self.ref[...] += self.bufs[stage]
        if stage + 1 < len(self.ways):
            self.copy(stage + 1).start()


class Gather:
    def __init__(self, num, order, own, full, sems, loc, me):
        self.order, self.own, self.full, self.loc, self.me = order, own, full, loc, me
        self.send, self.recv, self.here = [sem.at[num] for sem in sems]

    def copies(self, stage, low=0, high=None):
        bit, partner = self.loc
        held, first = [self.me], 0
        for way in self.order[:stage]:
            first += len(held)
            held += [piece + way - 2 * way * bit[way] for piece in held]
        way = (*self.order, CORE)[stage]
        return [pltpu.make_async_remote_copy(
            src_ref=self.full(piece) if i else self.own, dst_ref=self.full(piece), send_sem=self.send.at[first + i],
            recv_sem=self.recv.at[first + i], device_id=partner[way], device_id_type=MESH_ID)
            for i, piece in enumerate(held) if i in range(len(held))[low:high]]

    def local(self):
        return pltpu.make_async_copy(self.own, self.full(self.me), self.here)

    def start(self, stage=0):
        todo = []
        if stage == 0:
            todo.append(self.local())
        if stage < len(self.order):
            todo += self.copies(stage)
        done = 1 << stage
        for copy in todo + self.copies(len(self.order), done >> 1, done):
            copy.start()

    def finish(self, stage):
        for copy in self.copies(stage):
            copy.wait()
        if stage == len(self.order):
            self.local().wait()

    def advance(self, stage):
        self.finish(stage)
        if stage < len(self.order):
            self.start(stage + 1)


def act(streams, text):
    for name, what in zip(text[::2], text[1::2]):
        if what == "s":
            streams[name].start()
        else:
            streams[name].advance(int(what))


def follow(plan, tick, streams):
    for item in ",".join(plan).split(","):
        when, text = item.split(":")

        @pl.when(tick == int(when))
        def _(text=text):
            act(streams, text)


def attn_fwd_kernel(n_heads, hd, lens, tok_ref, emb_ref, cos_ref, sin_ref, small_ref, wq_own, wo_own, wu_own, wd_own, grad_ref,
                    qkv_ref, o_ref, lse_ref, cls_ref, scale_ref, ec_ref, hc_ref, small_out, vecs_ref,
                    wq_out, wo_ref, wu_ref, wd_ref, gp_ref, class_scr, lin_scr, wu_scr, tok_scr, small_all, wq_ref,
                    send_sem, recv_sem, here_sem, swap_send, swap_recv, put_sem):
    step = pl.program_id(0)
    dim = n_heads * hd
    loc = place()
    z, me = lax.axis_index('cp'), lax.axis_index('fsdp')
    n_seq = tok_scr.shape[0]
    seq_half = tok_scr.shape[1]
    slen = 2 * seq_half
    mine, other = [pl.ds(pl.multiple_of(zz * n_seq, n_seq), n_seq) for zz in (z, 1 - z)]
    sems = (send_sem, recv_sem, here_sem)
    cut = 48
    streams = {}
    for name, order, own, full in (
            ("a", XY, small_ref, lambda f: small_all.at[f]),
            ("b", XY, wq_own.at[:cut], lambda f: wq_ref.at[f, :cut]),
            ("c", YX, wq_own.at[cut:], lambda f: wq_ref.at[f, cut:]),
            ("d", XY, wo_own, lambda f: wo_ref.at[f]),
            ("e", XY, wu_scr, lambda f: wu_ref.at[f]),
            ("f", YX, wd_own, lambda f: wd_ref.at[:, f])):
        streams[name] = Gather(len(streams), order, own, full, sems, loc, me)

    def swap(num, src, dst):
        return pltpu.make_async_remote_copy(src_ref=src, dst_ref=dst, send_sem=swap_send.at[num], recv_sem=swap_recv.at[num],
                                            device_id=loc[1][ZDIR], device_id_type=MESH_ID)

    swaps = [swap(0, tok_ref.at[other], tok_scr), swap(1, grad_ref.at[other], gp_ref)]
    keep = pltpu.make_async_copy(wq_ref, wq_out, put_sem)
    lane = lax.broadcasted_iota(jnp.int32, (1, slen), 1)
    pos = jnp.where(lane < seq_half, z * seq_half + lane, lane - z * seq_half)

    @pl.when(step == 0)
    def _():
        greet(loc[1])
        for copy in swaps:
            copy.start()
        act(streams, "asbscs")
        x = wu_own[...]
        n_slab = FTILE // N_PIECE
        slabs = x.shape[1] // FTILE
        wu_scr[...] = jnp.concatenate(
            [x[:, (f * slabs + j) * n_slab:(f * slabs + j + 1) * n_slab] for j in range(slabs) for f in range(N_PIECE)], axis=1)
        act(streams, "a0b0c0dsesfsa1")
        swaps[0].wait()
        tok = jnp.concatenate([tok_ref[mine, :], tok_scr[...]], axis=1)
        row = row_iota(n_seq, 1)
        length = jnp.zeros(row.shape, jnp.int32)
        for i in range(n_seq):
            length = jnp.where(row == i, lens[z * n_seq + i], length)
        masked = tok == MASK_ID
        count = jnp.sum(jnp.where(masked, 1.0, 0.0), axis=-1, keepdims=True)
        scale = (1.0 - TRAIN_RATIO) / (1.0 - count / length.astype(F32))
        scale_ref[...] = scale
        cls = jnp.where(masked | (pos >= length), PAD_ID, tok)
        emb = clean_table(emb_ref)
        for i in range(n_seq):
            cls_ref[i] = cls[i:i + 1]
            ec_ref[i * NCLS:(i + 1) * NCLS, :] = emb * scale[i:i + 1]
        act(streams, "a2")
        vecs_ref[...] = jnp.concatenate([small_all[f] for f in range(N_PIECE)], axis=1)
        hc_ref[...] = (normalize(ec_ref[...])[0] * vecs_ref[0:1, :] + vecs_ref[1:2, :]).astype(BF)
        small_out[...] = small_all[...]
        act(streams, "b1c1b2c2")
        keep.start()
        full = mm(hc_ref[...], wq_ref[...].reshape(dim, 3 * dim), NN)
        for part in range(3):
            cols = slice(part * dim, (part + 1) * dim)
            val = full[:, cols] + vecs_ref[2 + part:3 + part, :]
            class_scr[:, cols] = val if part else val * hd ** -0.5

    follow(FWD_PLAN, step, streams)
    rows = class_scr[pl.ds(step * NCLS, NCLS), :]
    hot = one_hot_rows(cls_ref[step])
    hot3 = cat([hot] * 3)
    for part in range(3):
        cols = slice(part * dim, (part + 1) * dim)
        lin_scr[cols, :] = mm(cat(split3(rows[:, cols])), hot3, TN)
    kx = key_rows(pos, lens[z * n_seq + step])
    qx = stack_rows([1.0], kx.shape[-1])
    cos, sin = cos_ref[...], sin_ref[...]
    half = hd // 2

    def heads(hs):
        bases = [pl.multiple_of(h * hd, hd) for h in hs]
        qs, ks, vs = [], [], []
        for base in bases:
            piece = lambda off, size: lin_scr[pl.ds(base + off, size), :]
            qs.append(rope_fwd(piece(0, half), piece(half, half), cos, sin).astype(BF))
            ks.append(rope_fwd(piece(dim, half), piece(dim + half, half), cos, sin).astype(BF))
            vs.append(piece(2 * dim, hd).astype(BF))
            for part, val in enumerate((qs[-1], ks[-1], vs[-1])):
                qkv_ref[0, pl.ds(part * dim + base, hd), :] = val
        ss = [mm(cat([k, kx]), cat([q, qx]), TN) for q, k in zip(qs, ks)]
        tops = [jnp.max(s, axis=0, keepdims=True) for s in ss]
        ps = [jnp.exp(s - t) for s, t in zip(ss, tops)]
        tots = [csum(p) for p in ps]
        os = [mm(v, p.astype(BF), NN) for v, p in zip(vs, ps)]
        for h, base, o, tot, top in zip(hs, bases, os, tots, tops):
            o_ref[0, pl.ds(base, hd), :] = o / tot
            lse_ref[0, pl.ds(h, 1), :] = top + jnp.log(tot)

    def body(i, carry):
        heads([i * FWD_HEADS + u for u in range(FWD_HEADS)])
        return carry

    lax.fori_loop(0, n_heads // FWD_HEADS, body, 0)

    @pl.when(step == n_seq - 1)
    def _():
        act(streams, "d2e2f2")
        swaps[1].wait()
        keep.wait()


def ffn_kernel(n_heads, hd, nsq, slen, keep_tiles,
               scale_ref, cls_ref, o_ref, grad_ref, gp_ref, et_ref, vecs_ref, bup_ref, wo_ref, wu_ref, wd_ref,
               outm_ref, outp_ref, do_ref, delta_ref, csum_ref, dvec_ref, dbup_ref, dwo_ref, gu_ref, gd_ref, ru_ref, rd_ref,
               xh_scr, rs_scr, n_scr, g_scr, y_scr, dn_scr, au_scr, ad_scr, u0, u1, u2, u3, d0, d1, d2, d3,
               send_sem, recv_sem, out_sem, grad_sem):
    tile, blk = pl.program_id(0), pl.program_id(1)
    n_tile, n_blk = pl.num_programs(0), pl.num_programs(1)
    tick = tile * n_blk + blk
    first, last = tile == 0, tile == n_tile - 1
    halfs = slen // 2
    n_rows = nsq * slen
    rows = pl.ds(pl.multiple_of(blk * n_rows, n_rows), n_rows)
    loc = place()
    sems = (send_sem, recv_sem)
    streams = {}
    for t in range(keep_tiles):
        for kind, (order, acc, bufs, out) in enumerate(((XY, au_scr, (u0, u1, u2, u3), ru_ref), (YX, ad_scr, (d0, d1, d2, d3), rd_ref))):
            streams["abcdef"[2 * t + kind]] = Stream(
                2 * t + kind, order, (lambda c, acc=acc, t=t: acc.at[t, :, :, c]), tuple(b.at[t] for b in bufs), out.at[t], sems, loc)

    def handed(t):
        return [pltpu.make_async_copy(acc.at[keep_tiles + t], out.at[t], out_sem.at[2 * t + kind])
                for kind, (acc, out) in enumerate(((au_scr, gu_ref), (ad_scr, gd_ref)))]

    n_seq = g_scr.shape[0]
    z = lax.axis_index('cp')
    loads = [pltpu.make_async_copy(src, g_scr.at[:, part], grad_sem.at[part])
             for part, src in enumerate((grad_ref.at[pl.ds(pl.multiple_of(z * n_seq, n_seq), n_seq)], gp_ref))]

    @pl.when(tick == 0)
    def _():
        for load in loads:
            load.start()
        greet(loc[1])
        dvec_ref[...] = jnp.zeros_like(dvec_ref)
        dbup_ref[...] = jnp.zeros_like(dbup_ref)
        dwo_ref[...] = jnp.zeros_like(dwo_ref)

    follow(FFN_PLAN, tick, streams)

    @pl.when(tick == (n_tile - 1) * n_blk)
    def _():
        for copy in handed(0):
            copy.start()

    @pl.when(first)
    def _():
        for i in range(nsq):
            r = pl.ds(pl.multiple_of(blk * n_rows + i * slen, slen), slen)
            e = mm(one_hot_rows(cls_ref[i]), clean_table(et_ref).astype(BF), TN) * scale_ref[pl.ds(blk * nsq + i, 1), :]
            x1 = e + mm(o_ref[i].astype(BF), wo_ref[...], TN) + vecs_ref[5:6, :]
            xh, rstd = normalize(x1)
            xh_scr[r, :] = xh
            rs_scr[r, :] = rstd
            y_scr[r, :] = x1 + vecs_ref[8:9, :]
            n_scr[r, :] = (xh * vecs_ref[6:7, :] + vecs_ref[7:8, :]).astype(BF)
        dn_scr[rows, :] = jnp.zeros_like(dn_scr[rows, :])

    @pl.when(tick == 0)
    def _():
        for load in loads:
            load.wait()

    @pl.when(blk == 0)
    def _():
        au_scr[tile] = jnp.zeros(au_scr.shape[1:], F32)
        ad_scr[tile] = jnp.zeros(ad_scr.shape[1:], F32)

    n = n_scr[rows, :]
    g = g_scr[pl.ds(blk * nsq, nsq)].reshape(n_rows, -1)
    wu = wu_ref[...]
    wd = wd_ref[...]
    cols = pl.ds(pl.multiple_of(tile * wu.shape[1], wu.shape[1]), wu.shape[1])
    u = mm(n, wu, NN) + bup_ref[:, cols]
    phi = 0.5 + 0.5 * lax.erf(u * 0.7071067811865476)
    a = (u * phi).astype(BF)
    slope = phi + u * (jnp.exp(-0.5 * u * u) * 0.3989422804014327)
    y_scr[rows, :] += mm(a, wd, NN)
    du = mm(g, wd, NT) * slope
    dub = du.astype(BF)
    dbup_ref[:, cols] += csum(du)
    ad_scr[tile] += mm(a, g, TN).reshape(ad_scr.shape[1:])
    au_scr[tile] += mm(n, dub, TN).reshape(au_scr.shape[1:])
    dn_scr[rows, :] += mm(dub, wu, NT)

    @pl.when(last)
    def _():
        for i in range(nsq):
            r = pl.ds(pl.multiple_of(blk * n_rows + i * slen, slen), slen)
            out = y_scr[r, :].astype(BF)
            outm_ref[i] = out[:halfs]
            outp_ref[i] = out[halfs:]
            dn = dn_scr[r, :]
            xh = xh_scr[r, :]
            g32 = g_scr[blk * nsq + i].reshape(slen, -1).astype(F32)
            dx = g32 + norm_pull(dn, vecs_ref[6:7, :], xh, rs_scr[r, :])
            dvec_ref[...] += cat([csum(dx), csum(dn * xh), csum(dn), csum(g32)])
            dxb = dx.astype(BF)
            o = o_ref[i]
            dwo_ref[...] += mm(o.astype(BF), dxb, NN)
            do = mm(wo_ref[...], dxb, NT)
            do_ref[i] = do.astype(BF)
            delta_ref[i] = jnp.sum((do * o).reshape(n_heads, hd, slen), axis=1)
            csum_ref[i] = mm(one_hot_rows(cls_ref[i]), dxb, NN)

    @pl.when(tick == n_tile * n_blk - 1)
    def _():
        for copy in handed(1):
            copy.start()
        for copy in handed(0) + handed(1):
            copy.wait()
        act(streams, "e3f3")


def attn_bwd_kernel(hd, nh, lens, scale_ref, cls_ref, cos_ref, sin_ref, qkv_ref, do_ref, lse_ref, delta_ref, hc_ref,
                    wq_ref, wk_ref, wv_ref, csum_ref, ec_ref, vecs_ref, dvb_ref, dbup_ref, gu_ref, gd_ref, go_ref,
                    ru_ref, rd_ref, ro_ref, rw_ref, rs_ref,
                    dlin_scr, bsum_scr, dcls_scr, dn_scr, dw_scr, small_scr, small_in,
                    u_own, d_own, o_own, u0, u1, u2, u3, d0, d1, d2, d3, o0, o1, o2, o3, w0, w1, w2, w3,
                    send_sem, recv_sem, own_sem, ssend, srecv):
    group, step = pl.program_id(0), pl.program_id(1)
    n_group, n_step = pl.num_programs(0), pl.num_programs(1)
    tick = group * n_step + step
    nsq = cls_ref.shape[0]
    n_seq = nsq * n_step
    gdim = nh * hd
    half = hd // 2
    loc = place()
    sems = (send_sem, recv_sem)
    streams = {"k": AllSum(small_scr, small_in, (ssend, srecv), loc)}
    for t in range(gu_ref.shape[0]):
        for kind, (order, src, own, bufs, out) in enumerate(((XY, gu_ref, u_own, (u0, u1, u2, u3), ru_ref),
                                                             (YX, gd_ref, d_own, (d0, d1, d2, d3), rd_ref))):
            num = 2 * t + kind
            streams["abcd"[num]] = Stream(num, order, (lambda c, src=src, t=t: src.at[t, :, :, c]), tuple(b.at[t] for b in bufs),
                                          out.at[t], sems, loc, (own.at[t], own_sem.at[num]))
    num = own_sem.shape[0] - 1
    streams["o"] = Stream(num, YX, lambda c: go_ref.at[:, :, c], (o0, o1, o2, o3), ro_ref, sems, loc, (o_own, own_sem.at[num]))
    n_piece = rw_ref.shape[1]
    for i, name in enumerate("vwxyzq"):
        t = min(i, rw_ref.shape[0] - 1)
        lo, hi = {"z": (0, n_piece // 2), "q": (n_piece // 2, n_piece)}.get(name, (0, n_piece))
        part = slice(lo, hi)
        streams[name] = Stream(num + 1 + i, (XY, YX)[i % 2], (lambda c, t=t, part=part: dw_scr.at[t, :, :, c, part]),
                               (w0.at[t, :, :, part], w1.at[t, :, part], w2.at[t, part], w3.at[t, part]), rw_ref.at[t, part],
                               sems, loc)

    @pl.when(tick == 0)
    def _():
        greet(loc[1])
        act(streams, "asbscsdsos")
        dn_scr[...] = jnp.zeros_like(dn_scr)
        small_scr[...] = jnp.zeros_like(small_scr)

    follow(BWD_PLAN, tick, streams)

    @pl.when(step == 0)
    def _():
        bsum_scr[...] = jnp.zeros_like(bsum_scr)

    width = cos_ref.shape[-1]
    z = lax.axis_index('cp')
    lane = lax.broadcasted_iota(jnp.int32, (1, width), 1)
    pos = jnp.where(lane < width // 2, z * (width // 2) + lane, lane - z * (width // 2))
    kxs = [key_rows(pos, lens[z * n_seq + step * nsq + b]) for b in range(nsq)]
    vx = stack_rows([1.0] * 3, width)
    cos, sin = cos_ref[...], sin_ref[...]

    def put(b, base, val):
        dlin_scr[b, base:base + hd, :] = val.astype(BF)
        bsum_scr[base:base + hd, :] += val[:, :width // 2] + val[:, width // 2:]

    def unrope(val):
        return rope_fwd(val[:half], val[half:], cos, -sin)

    def extra(ref, b, h):
        return [t.astype(F32) for t in split3(-ref[b, pl.ds(group * nh + h, 1), :])]

    items = [(b, h, slice(h * hd, (h + 1) * hd)) for b in range(nsq) for h in range(nh)]
    qs, ks, vs = [[qkv_ref[b, part, span, :] for b, _, span in items] for part in range(3)]
    dos = [do_ref[b, span, :] for b, _, span in items]
    ss = [mm(cat([k, kxs[b]]), cat([q, stack_rows([1.0] + extra(lse_ref, b, h), width)]), TN)
          for k, q, (b, h, _) in zip(ks, qs, items)]
    dps = [mm(cat([v, vx]), cat([do, stack_rows(extra(delta_ref, b, h), width)]), TN) for v, do, (b, h, _) in zip(vs, dos, items)]
    ps = [jnp.exp(t) for t in ss]
    pbs = [p.astype(BF) for p in ps]
    dss = [(p * dp).astype(BF) for p, dp in zip(ps, dps)]
    dvs = [mm(do, p, NT) for do, p in zip(dos, pbs)]
    dks = [mm(q, ds, NT) for q, ds in zip(qs, dss)]
    dqs = [mm(k, ds, NN) for k, ds in zip(ks, dss)]
    for dq, dk, dv, (b, h, _) in zip(dqs, dks, dvs, items):
        put(b, h * hd, unrope(dq) * hd ** -0.5)
        put(b, gdim + h * hd, unrope(dk))
        put(b, 2 * gdim + h * hd, dv)

    for b in range(nsq):
        at = pl.multiple_of((step * nsq + b) * NCLS, NCLS)
        dcls_scr[pl.ds(at, NCLS), :] = mm(one_hot_rows(cls_ref[b]), dlin_scr[b], NT)

    @pl.when(step == n_step - 1)
    def _():
        hc = hc_ref[...]
        acc = dcls_scr[...]
        hi, lo, _ = split3(acc)
        dw_scr[group] = mm(cat([hc, hc]), cat([hi, lo]), TN).reshape(dw_scr.shape[1:])
        dn = dn_scr[...]
        cols = pl.ds(pl.multiple_of(group * gdim, gdim), gdim)
        bias = csum(jnp.transpose(bsum_scr[...]))
        for part, w_ref in enumerate((wq_ref, wk_ref, wv_ref)):
            sel = slice(part * gdim, (part + 1) * gdim)
            dn = dn + mm(hi[:, sel], w_ref[...], NT) + mm(lo[:, sel], w_ref[...], NT)
            small_scr[2 + part:3 + part, cols] = bias[:, sel]
        dn_scr[...] = dn

    @pl.when(tick == n_group * n_step - 1)
    def _():
        tail = BWD_TAIL.split(",")
        act(streams, tail[0])
        dn = dn_scr[...]
        xh, rstd = normalize(ec_ref[...])
        de = norm_pull(dn, vecs_ref[0:1, :], xh, rstd)
        small_scr[0:2, :] = cat([csum(dn * xh), csum(dn)])
        small_scr[5:13, :] = cat([dvb_ref[...], dbup_ref[...]])
        tab = jnp.zeros((NCLS, dn.shape[1]), F32)
        for b in range(dcls_scr.shape[0] // NCLS):
            tab = tab + (de[b * NCLS:(b + 1) * NCLS] + csum_ref[b]) * scale_ref[b:b + 1, :]
        small_scr[16:, :] = jnp.where(row_iota(*tab.shape) == PAD_ID, 0.0, tab)
        act(streams, "ks")
        for text in tail[1:]:
            act(streams, text)
        rs_ref[...] = small_scr[...]


def whole(shape):
    return pl.BlockSpec(shape, lambda *_: (0,) * len(shape), pipeline_mode=pl.Buffered(1))


def params(**kw):
    return pltpu.CompilerParams(vmem_limit_bytes=VMEM_LIMIT, **kw)


def cost(flops, moved):
    return pl.CostEstimate(flops=flops * 10**9, bytes_accessed=moved * 10**6, transcendentals=0)


def sds(*t):
    return jax.ShapeDtypeStruct(t, F32)


def sdb(*t):
    return jax.ShapeDtypeStruct(t, BF)


def vm(*t):
    return pltpu.VMEM(t, F32)


def dma(*t):
    return pltpu.SemaphoreType.DMA(t)


def stages(lead, *t):
    return [vm(*lead, 2, 2, *t), vm(*lead, 2, *t), vm(*lead, *t), vm(*lead, *t)]


SMEM = pl.BlockSpec(memory_space=pltpu.SMEM)


def attn_fwd(lens, tokens, embed, cos, sin, small, wq, wo, wu, wd, grad):
    n_seq, seq_half = tokens.shape[0] // 2, tokens.shape[1]
    slen = 2 * seq_half
    dim = wo.shape[1]
    hd = 2 * cos.shape[0]
    n_heads = dim // hd
    row = lambda *t: pl.BlockSpec((1,) + t, lambda i: (i, 0, 0))
    anyspace = pl.BlockSpec(memory_space=pl.ANY)
    held = [(jnp.int32, (n_seq, 1, slen)), (F32, (n_seq, 1)), (F32, (n_seq * NCLS, dim)), (BF, (n_seq * NCLS, dim)),
            (F32, (N_PIECE, *small.shape)), (F32, (small.shape[0], dim))]
    far = [(N_PIECE, *wq.shape), (N_PIECE, *wo.shape), (N_PIECE, *wu.shape), (wd.shape[0], N_PIECE, *wd.shape[1:]), (n_seq, *grad.shape[1:])]
    args = (tokens, embed, cos, sin, small, wq, wo, wu, wd)
    return pl.pallas_call(
        functools.partial(attn_fwd_kernel, n_heads, hd),
        grid=(n_seq,),
        in_specs=[SMEM, *[whole(t.shape) for t in args], anyspace],
        out_specs=[row(3 * dim, slen), row(dim, slen), row(n_heads, slen), *[whole(t) for _, t in held], *[anyspace] * len(far)],
        out_shape=[sdb(n_seq, 3 * dim, slen), sds(n_seq, dim, slen), sds(n_seq, n_heads, slen),
                   *[jax.ShapeDtypeStruct(t, kind) for kind, t in held], *[sdb(*t) for t in far]],
        scratch_shapes=[vm(n_seq * NCLS, 3 * dim), vm(3 * dim, slen), pltpu.VMEM(wu.shape, BF),
                        pltpu.VMEM((n_seq, seq_half), jnp.int32), vm(N_PIECE, *small.shape),
                        pltpu.VMEM((N_PIECE, *wq.shape), BF), dma(6, 7), dma(6, 7), dma(6), dma(2), dma(2), pltpu.SemaphoreType.DMA],
        compiler_params=params(collective_id=2, has_side_effects=True), name="attn_fwd", cost_estimate=cost(20, 18),
    )(lens, *args, grad)


def ffn(scales, cls, o, grad, gp, etab, vecs, bup, wo, wu, wd, n_heads, hd, nsq=2, keep_tiles=3):
    n_seq, _, slen = cls.shape
    dim, ff = wu.shape
    tiles = ff // FTILE
    rest = tiles - keep_tiles
    halfs = slen // 2
    piece, slab = dim // N_PIECE, FTILE // N_PIECE
    n_blk = n_seq // nsq
    n_rows = n_seq * slen

    def blk(when, *t):
        return pl.BlockSpec((nsq,) + t, lambda j, r: (jnp.where(when(j), r, when(0) * (n_blk - 1)),) + (0,) * len(t))

    late = lambda j: j == tiles - 1
    both = lambda j: (j == 0) | (j == tiles - 1)
    anyspace = pl.BlockSpec(memory_space=pl.ANY)
    cube = (2,) * 3
    bwd_u, bwd_d = (rest, *cube, piece, FTILE), (rest, *cube, slab, dim)
    red_u, red_d = (keep_tiles, piece, FTILE), (keep_tiles, slab, dim)
    return pl.pallas_call(
        functools.partial(ffn_kernel, n_heads, hd, nsq, slen, keep_tiles),
        grid=(tiles, n_blk),
        in_specs=[whole(scales.shape), blk(both, 1, slen), blk(both, dim, slen), anyspace, anyspace,
                  whole(etab.shape), whole(vecs.shape), whole(bup.shape), whole(wo.shape),
                  pl.BlockSpec((dim, FTILE), lambda j, r: (0, j)), pl.BlockSpec((FTILE, dim), lambda j, r: (j, 0))],
        out_specs=[blk(late, halfs, dim), blk(late, halfs, dim), blk(late, dim, slen), blk(late, n_heads, slen),
                   blk(late, NCLS, dim), whole((4, dim)), whole((1, ff)), whole((dim, dim)), anyspace, anyspace,
                   whole(red_u), whole(red_d)],
        out_shape=[sdb(n_seq, halfs, dim), sdb(n_seq, halfs, dim), sdb(n_seq, dim, slen), sds(n_seq, n_heads, slen),
                   sds(n_seq, NCLS, dim), sds(4, dim), sds(1, ff), sds(dim, dim), sds(*bwd_u), sds(*bwd_d), sds(*red_u), sds(*red_d)],
        scratch_shapes=[vm(n_rows, dim), vm(n_rows, 1), pltpu.VMEM((n_rows, dim), BF), pltpu.VMEM((n_seq, 2, halfs, dim), BF),
                        vm(n_rows, dim), vm(n_rows, dim), vm(tiles, *cube, piece, FTILE), vm(tiles, *cube, slab, dim)]
        + stages((keep_tiles,), piece, FTILE) + stages((keep_tiles,), slab, dim)
        + [dma(2 * keep_tiles, 4), dma(2 * keep_tiles, 4), dma(2 * rest), dma(2)],
        compiler_params=params(collective_id=1, has_side_effects=True), name="ffn", cost_estimate=cost(60, 40),
    )(scales, cls, o, grad, gp, etab, vecs, bup, wo, wu, wd)


def attn_bwd(lens, scales, cls, cos, sin, qkv, do, lse, delta, hc, w, csums, ec, vecs, dvec_b, d_bup, d_wu, d_wd, d_wo,
             n_heads, hd, groups=5, nsq=2):
    n_seq, _, slen = cls.shape
    dim = n_heads * hd
    nh = n_heads // groups
    gdim = nh * hd
    cube = (2,) * 3
    blk = lambda *t: pl.BlockSpec((nsq,) + t, lambda g, i: (i,) + (0,) * len(t))
    wcol = lambda part: pl.BlockSpec((dim, gdim), lambda g, i: (0, part * groups + g))
    anyspace = pl.BlockSpec(memory_space=pl.ANY)
    ut, dt, ot = d_wu.shape[-2:], d_wd.shape[-2:], (dim // N_PIECE, dim)
    wt = (dim // N_PIECE, 3 * gdim)
    rest = d_wu.shape[0]
    fixed = (hc, csums, ec, vecs, dvec_b, d_bup.reshape(-1, dim))
    args = [lens, scales, cls, cos, sin, qkv.reshape(n_seq, 3, dim, slen), do, lse, delta, hc, w, w, w, *fixed[1:],
            d_wu, d_wd, d_wo.reshape(*cube, *ot)]
    specs = [SMEM, whole(scales.shape), blk(1, slen), whole(cos.shape), whole(sin.shape),
             pl.BlockSpec((nsq, 3, gdim, slen), lambda g, i: (i, 0, g, 0)), pl.BlockSpec((nsq, gdim, slen), lambda g, i: (i, g, 0)),
             blk(n_heads, slen), blk(n_heads, slen), whole(hc.shape), *[wcol(part) for part in range(3)],
             *[whole(t.shape) for t in fixed[1:]], *[anyspace] * 3]
    small = (16 + NCLS, dim)
    shapes = [sds(rest, *ut), sds(rest, *dt), sds(*ot), sds(groups, *wt), sds(*small)]
    n_str = 2 * rest + 1
    return pl.pallas_call(
        functools.partial(attn_bwd_kernel, hd, nh),
        grid=(groups, n_seq // nsq),
        in_specs=specs,
        out_specs=[whole(t.shape) for t in shapes],
        out_shape=shapes,
        scratch_shapes=[pltpu.VMEM((nsq, 3 * gdim, slen), BF), vm(3 * gdim, slen // 2), vm(n_seq * NCLS, 3 * gdim),
                        vm(n_seq * NCLS, dim), vm(groups, *cube, *wt), vm(*small), vm(4, *small),
                        vm(rest, 2, 2, *ut), vm(rest, 2, 2, *dt), vm(2, 2, *ot)]
        + stages((rest,), *ut) + stages((rest,), *dt) + stages((), *ot) + stages((groups,), *wt)
        + [dma(n_str + groups + 1, 4), dma(n_str + groups + 1, 4), dma(n_str), dma(4), dma(4)],
        compiler_params=params(collective_id=0, has_side_effects=True), name="attn_bwd", cost_estimate=cost(40, 20),
    )(*args)


def rope_tables(slen, hd):
    inv_freq = 1.0 / (ROPE_BASE ** (jnp.arange(0, hd, 2, dtype=F32) / hd))
    half = slen // 2
    turn = jnp.arange(slen).reshape(2, half)
    cp_index = lax.axis_index('cp')
    pos = jnp.where(cp_index == 0, turn, turn[::-1]).reshape(slen)
    angles = inv_freq[:, None] * pos.astype(F32)[None, :]
    return jnp.cos(angles), jnp.sin(angles)


def solution(mesh):
    swap = [(0, 1), (1, 0)]
    n_fsdp = mesh.shape['fsdp']

    def local_step(tokens, lengths, embed_table, layer_vecs, w_qkv, w_out, w_up, b_up, w_down, grad_out):
        cp_index = lax.axis_index('cp')
        me = lax.axis_index('fsdp')
        vocab, dim = embed_table.shape
        n_heads, hd = w_qkv.shape[2], w_qkv.shape[3]
        slabs = w_up.shape[1] // FTILE
        cos_t, sin_t = rope_tables(2 * tokens.shape[1], hd)
        small = jnp.concatenate([layer_vecs, b_up.reshape(-1, layer_vecs.shape[1])], 0)
        small = jnp.pad(small, ((0, 16 - small.shape[0]), (0, 0)))
        (qkv, o, lse, cls, scales, e_cls, hc, small_all, vecs, w_all, out_w, up_w, down_w, g_peer) = attn_fwd(
            lengths, tokens, embed_table, cos_t, sin_t, small, w_qkv.reshape(w_qkv.shape[0], -1), w_out, w_up,
            w_down.reshape(slabs, -1, dim), grad_out)
        up_b = jnp.swapaxes(small_all[:, 9:13].reshape(n_fsdp, slabs, -1), 0, 1).reshape(1, -1)
        (out_m, out_p, do, delta, csums, dvec_b, d_bup, d_wo, d_wu, d_wd, red_wu, red_wd) = ffn(
            scales, cls, o, grad_out, g_peer, embed_table, vecs, up_b, out_w.reshape(dim, dim), up_w.reshape(dim, -1),
            down_w.reshape(-1, dim), n_heads, hd)
        out_back = lax.ppermute(out_p, 'cp', swap)
        layer_out = jnp.where(cp_index == 0, jnp.concatenate([out_m, out_back], 0), jnp.concatenate([out_back, out_m], 0))
        rest_wu, rest_wd, red_wo, red_w, red_small = attn_bwd(
            lengths, scales, cls, cos_t, sin_t, qkv, do, lse, delta, hc, w_all.reshape(dim, -1), csums, e_cls, vecs, dvec_b, d_bup, d_wu, d_wd,
            d_wo, n_heads, hd)
        groups = red_w.shape[0]
        red_w = jnp.transpose(red_w.reshape(groups, -1, 3, n_heads // groups, hd), (1, 2, 0, 3, 4)).reshape(w_qkv.shape)
        d_vecs = lax.dynamic_slice_in_dim(red_small[:9], me * layer_vecs.shape[1], layer_vecs.shape[1], 1)
        d_bup = lax.dynamic_slice_in_dim(red_small[9:13].reshape(slabs, n_fsdp, -1), me, 1, 1).reshape(b_up.shape)
        red_wu = jnp.concatenate([red_wu, rest_wu], 0).reshape(slabs, -1, n_fsdp, FTILE // n_fsdp)
        d_wup = jnp.transpose(red_wu, (1, 2, 0, 3)).reshape(w_up.shape)
        d_wdown = jnp.concatenate([red_wd, rest_wd], 0).reshape(w_down.shape)
        d_table = jnp.concatenate([red_small[16:16 + NCLS], jnp.zeros((vocab - NCLS, dim), F32)], 0)
        return layer_out, d_table, d_vecs, red_w, red_wo, d_wup, d_bup, d_wdown

    in_specs = (P('fsdp', 'cp'), P('fsdp'), P(), P(None, 'fsdp'), P('fsdp', None, None, None), P('fsdp', None), P('fsdp', None), P('fsdp'), P('fsdp', None), P('fsdp', 'cp', None))
    out_specs = (P('fsdp', 'cp', None), P(), P(None, 'fsdp'), P('fsdp', None, None, None), P('fsdp', None), P('fsdp', None), P('fsdp'), P('fsdp', None))
    return jax.shard_map(local_step, mesh=mesh, in_specs=in_specs, out_specs=out_specs, check_vma=False)
```

```python
import functools

import jax
import jax.numpy as jnp
from jax import lax
from jax.experimental import pallas as pl
from jax.experimental.pallas import tpu as pltpu
from jax.sharding import PartitionSpec as P

MASK_ID = 32
PAD_ID = 1
NCLS = 32
LN_EPS = 1e-5
ROPE_BASE = 10000.0
TRAIN_RATIO = 0.15 * 0.8
NEG_BIG = -1e30
CORE, XDIR, YDIR = 1, 2, 4
ZDIR = 0
XY, YX = (XDIR, YDIR), (YDIR, XDIR)
BF = jnp.bfloat16
F32 = jnp.float32
VMEM_LIMIT = 67043328
NN = (((1,), (0,)), ((), ()))
NT = (((1,), (1,)), ((), ()))
TN = (((0,), (0,)), ((), ()))
FTILE = 512
N_PIECE = 8
FWD_HEADS = 10
MESH_ID = pl.DeviceIdType.MESH
FWD_PLAN = ("1:d0e0f0", "4:d1", "7:e1f1")
FFN_PLAN = ("4:asbs,5:a0b0,8:a1b1csds,9:c0d0,10:a2b2,12:c1d1esfs", "13:a3b3e0f0,14:c2d2,16:e1f1,17:c3d3,18:e2f2")
BWD_PLAN = ("1:a0b0,2:c0d0,4:vsa1b1,5:o0v0,7:c1d1,8:ws,9:a2b2w0,11:v1", "12:xso1,13:x0,14:c2d2,15:a3b3,16:ys,17:y0w1,18:o2v2x1")
BWD_TAIL = "zsqs,c3d3w2,z0q0,y1x2,k0,z1q1,y2,k1,v3w3x3o3,z2q2,k2,y3,z3q3,k3"


def mm(a, b, dims):
    return lax.dot_general(a, b, dims, preferred_element_type=F32)


def rmean(x):
    return jnp.mean(x, axis=-1, keepdims=True)


def csum(x):
    return jnp.sum(x, axis=0, keepdims=True)


def normalize(x):
    cen = x - rmean(x)
    rstd = lax.rsqrt(rmean(cen * cen) + LN_EPS)
    return cen * rstd, rstd


def norm_pull(dn, gain, xh, rstd):
    dy = dn * gain
    return rstd * (dy - rmean(dy) - xh * rmean(dy * xh))


def cat(parts):
    return jnp.concatenate(parts, axis=0)


def split3(x):
    hi = x.astype(BF)
    rest = x - hi.astype(F32)
    mid = rest.astype(BF)
    lo = (rest - mid.astype(F32)).astype(BF)
    return hi, mid, lo


def row_iota(rows, width):
    return lax.broadcasted_iota(jnp.int32, (rows, width), 0)


def one_hot_rows(cls):
    return (row_iota(NCLS, cls.shape[-1]) == cls).astype(BF)


def stack_rows(parts, width):
    row = row_iota(16, width)
    out = jnp.zeros(row.shape, F32)
    for i, part in enumerate(parts):
        out = jnp.where(row == i, part, out)
    return out.astype(BF)


def key_rows(pos, length):
    return stack_rows([jnp.where(pos < length, 0.0, NEG_BIG)] + [1.0] * 3, pos.shape[-1])


def rope_fwd(lo, hi, cos, sin):
    return cat([lo * cos - hi * sin, hi * cos + lo * sin])


def place():
    z, me = lax.axis_index('cp'), lax.axis_index('fsdp')
    bit = {CORE: lax.rem(me, XDIR), XDIR: lax.rem(me // XDIR, XDIR), YDIR: me // YDIR}
    partner = {way: (z, me + way - 2 * way * bit[way]) for way in bit}
    partner[ZDIR] = (1 - z, me)
    return bit, partner


def greet(partner):
    barrier = pltpu.get_barrier_semaphore()
    for way in partner:
        pl.semaphore_signal(barrier, inc=1, device_id=partner[way], device_id_type=MESH_ID)
    pl.semaphore_wait(barrier, len(partner))


def clean_table(ref):
    return jnp.where(row_iota(NCLS, ref.shape[1]) == PAD_ID, 0.0, ref[:NCLS, :].astype(F32))


class Stream:
    def __init__(self, num, order, src, bufs, out, sems, loc, own=None):
        self.num, self.order, self.src, self.bufs, self.out = num, order, src, bufs, out
        self.sems, self.loc, self.own = sems, loc, own

    def pick(self, stage, bit):
        way = self.order[stage - 1]
        buf = self.bufs[stage - 1]
        return buf.at[:, bit] if stage == 1 and way == XDIR else buf.at[bit]

    def copy(self, stage):
        bit, partner = self.loc
        way = (CORE, *self.order, ZDIR)[stage]
        if stage == 0:
            src = self.src(1 - bit[CORE])
        elif way == ZDIR:
            src = self.bufs[stage - 1]
        else:
            src = self.pick(stage, 1 - bit[way])
        return pltpu.make_async_remote_copy(
            src_ref=src, dst_ref=self.bufs[stage], send_sem=self.sems[0].at[self.num, stage],
            recv_sem=self.sems[1].at[self.num, stage], device_id=partner[way], device_id_type=MESH_ID)

    def local(self):
        return pltpu.make_async_copy(self.src(self.loc[0][CORE]), *self.own)

    def start(self):
        self.copy(0).start()
        if self.own:
            self.local().start()

    def advance(self, stage):
        bit = self.loc[0]
        buf = self.bufs[stage]
        self.copy(stage).wait()
        if stage == 0:
            if self.own:
                self.local().wait()
            buf[...] += self.own[0][...] if self.own else self.src(bit[CORE])[...]
        elif stage <= len(self.order):
            buf[...] += self.pick(stage, bit[self.order[stage - 1]])[...]
        else:
            self.out[...] = self.bufs[stage - 1][...] + buf[...]
            return
        self.copy(stage + 1).start()


class AllSum:
    def __init__(self, ref, bufs, sems, loc):
        self.ref, self.bufs, self.sems, self.loc = ref, bufs, sems, loc
        self.ways = (CORE, XDIR, YDIR, ZDIR)

    def copy(self, stage):
        return pltpu.make_async_remote_copy(
            src_ref=self.ref, dst_ref=self.bufs.at[stage], send_sem=self.sems[0].at[stage], recv_sem=self.sems[1].at[stage],
            device_id=self.loc[1][self.ways[stage]], device_id_type=MESH_ID)

    def start(self):
        self.copy(0).start()

    def advance(self, stage):
        self.copy(stage).wait()
        self.ref[...] += self.bufs[stage]
        if stage + 1 < len(self.ways):
            self.copy(stage + 1).start()


class Gather:
    def __init__(self, num, order, own, full, sems, loc, me):
        self.order, self.own, self.full, self.loc, self.me = order, own, full, loc, me
        self.send, self.recv, self.here = [sem.at[num] for sem in sems]

    def copies(self, stage, low=0, high=None):
        bit, partner = self.loc
        held, first = [self.me], 0
        for way in self.order[:stage]:
            first += len(held)
            held += [piece + way - 2 * way * bit[way] for piece in held]
        way = (*self.order, CORE)[stage]
        return [pltpu.make_async_remote_copy(
            src_ref=self.full(piece) if i else self.own, dst_ref=self.full(piece), send_sem=self.send.at[first + i],
            recv_sem=self.recv.at[first + i], device_id=partner[way], device_id_type=MESH_ID)
            for i, piece in enumerate(held) if i in range(len(held))[low:high]]

    def local(self):
        return pltpu.make_async_copy(self.own, self.full(self.me), self.here)

    def start(self, stage=0):
        todo = []
        if stage == 0:
            todo.append(self.local())
        if stage < len(self.order):
            todo += self.copies(stage)
        done = 1 << stage
        for copy in todo + self.copies(len(self.order), done >> 1, done):
            copy.start()

    def finish(self, stage):
        for copy in self.copies(stage):
            copy.wait()
        if stage == len(self.order):
            self.local().wait()

    def advance(self, stage):
        self.finish(stage)
        if stage < len(self.order):
            self.start(stage + 1)


def act(streams, text):
    for name, what in zip(text[::2], text[1::2]):
        if what == "s":
            streams[name].start()
        else:
            streams[name].advance(int(what))


def follow(plan, tick, streams):
    for item in ",".join(plan).split(","):
        when, text = item.split(":")

        @pl.when(tick == int(when))
        def _(text=text):
            act(streams, text)


def attn_fwd_kernel(n_heads, hd, lens, tok_ref, emb_ref, cos_ref, sin_ref, small_ref, wq_own, wo_own, wu_own, wd_own, grad_ref,
                    qkv_ref, o_ref, lse_ref, cls_ref, scale_ref, ec_ref, hc_ref, bup_ref, vecs_ref,
                    wq_out, wo_ref, wu_ref, wd_ref, gp_ref, class_scr, lin_scr, wu_scr, tok_scr, small_all, wq_ref,
                    send_sem, recv_sem, here_sem, swap_send, swap_recv, put_sem):
    step = pl.program_id(0)
    dim = n_heads * hd
    loc = place()
    z, me = lax.axis_index('cp'), lax.axis_index('fsdp')
    n_seq = tok_scr.shape[0]
    seq_half = tok_scr.shape[1]
    slen = 2 * seq_half
    mine, other = [pl.ds(pl.multiple_of(zz * n_seq, n_seq), n_seq) for zz in (z, 1 - z)]
    sems = (send_sem, recv_sem, here_sem)
    cut = 48
    streams = {}
    for name, order, own, full in (
            ("a", XY, small_ref, lambda f: small_all.at[f]),
            ("b", XY, wq_own.at[:cut], lambda f: wq_ref.at[f, :cut]),
            ("c", YX, wq_own.at[cut:], lambda f: wq_ref.at[f, cut:]),
            ("d", XY, wo_own, lambda f: wo_ref.at[f]),
            ("e", XY, wu_scr, lambda f: wu_ref.at[f]),
            ("f", YX, wd_own, lambda f: wd_ref.at[:, f])):
        streams[name] = Gather(len(streams), order, own, full, sems, loc, me)

    def swap(num, src, dst):
        return pltpu.make_async_remote_copy(src_ref=src, dst_ref=dst, send_sem=swap_send.at[num], recv_sem=swap_recv.at[num],
                                            device_id=loc[1][ZDIR], device_id_type=MESH_ID)

    swaps = [swap(0, tok_ref.at[other], tok_scr), swap(1, grad_ref.at[other], gp_ref)]
    keep = pltpu.make_async_copy(wq_ref, wq_out, put_sem)
    lane = lax.broadcasted_iota(jnp.int32, (1, slen), 1)
    pos = jnp.where(lane < seq_half, z * seq_half + lane, lane - z * seq_half)

    @pl.when(step == 0)
    def _():
        greet(loc[1])
        for copy in swaps:
            copy.start()
        act(streams, "asbscs")
        x = wu_own[...]
        n_slab = FTILE // N_PIECE
        slabs = x.shape[1] // FTILE
        wu_scr[...] = jnp.concatenate(
            [x[:, (f * slabs + j) * n_slab:(f * slabs + j + 1) * n_slab] for j in range(slabs) for f in range(N_PIECE)], axis=1)
        act(streams, "a0b0c0dsesfsa1")
        swaps[0].wait()
        tok = jnp.concatenate([tok_ref[mine, :], tok_scr[...]], axis=1)
        row = row_iota(n_seq, 1)
        length = jnp.zeros(row.shape, jnp.int32)
        for i in range(n_seq):
            length = jnp.where(row == i, lens[z * n_seq + i], length)
        masked = tok == MASK_ID
        count = jnp.sum(jnp.where(masked, 1.0, 0.0), axis=-1, keepdims=True)
        scale = (1.0 - TRAIN_RATIO) / (1.0 - count / length.astype(F32))
        scale_ref[...] = scale
        cls = jnp.where(masked | (pos >= length), PAD_ID, tok)
        emb = clean_table(emb_ref)
        for i in range(n_seq):
            cls_ref[i] = cls[i:i + 1]
            ec_ref[i * NCLS:(i + 1) * NCLS, :] = emb * scale[i:i + 1]
        act(streams, "a2")
        vecs_ref[...] = jnp.concatenate([small_all[f] for f in range(N_PIECE)], axis=1)
        hc_ref[...] = (normalize(ec_ref[...])[0] * vecs_ref[0:1, :] + vecs_ref[1:2, :]).astype(BF)
        flat = [jnp.concatenate([small_all[f, 9 + r:10 + r] for r in range(4)], axis=1) for f in range(N_PIECE)]
        bup_ref[...] = jnp.concatenate([t[:, j * n_slab:(j + 1) * n_slab] for j in range(slabs) for t in flat], axis=1)
        act(streams, "b1c1b2c2")
        keep.start()
        full = mm(hc_ref[...], wq_ref[...].reshape(dim, 3 * dim), NN)
        for part in range(3):
            cols = slice(part * dim, (part + 1) * dim)
            val = full[:, cols] + vecs_ref[2 + part:3 + part, :]
            class_scr[:, cols] = val if part else val * hd ** -0.5

    follow(FWD_PLAN, step, streams)
    rows = class_scr[pl.ds(step * NCLS, NCLS), :]
    hot = one_hot_rows(cls_ref[step])
    hot3 = cat([hot] * 3)
    for part in range(3):
        cols = slice(part * dim, (part + 1) * dim)
        lin_scr[cols, :] = mm(cat(split3(rows[:, cols])), hot3, TN)
    kx = key_rows(pos, lens[z * n_seq + step])
    qx = stack_rows([1.0], kx.shape[-1])
    cos, sin = cos_ref[...], sin_ref[...]
    half = hd // 2

    def heads(hs):
        bases = [pl.multiple_of(h * hd, hd) for h in hs]
        qs, ks, vs = [], [], []
        for base in bases:
            piece = lambda off, size: lin_scr[pl.ds(base + off, size), :]
            qs.append(rope_fwd(piece(0, half), piece(half, half), cos, sin).astype(BF))
            ks.append(rope_fwd(piece(dim, half), piece(dim + half, half), cos, sin).astype(BF))
            vs.append(piece(2 * dim, hd).astype(BF))
            for part, val in enumerate((qs[-1], ks[-1], vs[-1])):
                qkv_ref[0, pl.ds(part * dim + base, hd), :] = val
        ss = [mm(cat([k, kx]), cat([q, qx]), TN) for q, k in zip(qs, ks)]
        tops = [jnp.max(s, axis=0, keepdims=True) for s in ss]
        ps = [jnp.exp(s - t) for s, t in zip(ss, tops)]
        tots = [csum(p) for p in ps]
        os = [mm(v, p.astype(BF), NN) for v, p in zip(vs, ps)]
        for h, base, o, tot, top in zip(hs, bases, os, tots, tops):
            o_ref[0, pl.ds(base, hd), :] = o / tot
            lse_ref[0, pl.ds(h, 1), :] = top + jnp.log(tot)

    def body(i, carry):
        heads([i * FWD_HEADS + u for u in range(FWD_HEADS)])
        return carry

    lax.fori_loop(0, n_heads // FWD_HEADS, body, 0)

    @pl.when(step == n_seq - 1)
    def _():
        act(streams, "d2e2f2")
        swaps[1].wait()
        keep.wait()


def ffn_kernel(n_heads, hd, nsq, slen, keep_tiles,
               scale_ref, cls_ref, o_ref, grad_ref, gp_ref, et_ref, vecs_ref, bup_ref, wo_ref, wu_ref, wd_ref,
               outm_ref, outp_ref, do_ref, delta_ref, csum_ref, dvec_ref, dbup_ref, dwo_ref, gu_ref, gd_ref, ru_ref, rd_ref,
               xh_scr, rs_scr, n_scr, g_scr, y_scr, dn_scr, au_scr, ad_scr, u0, u1, u2, u3, d0, d1, d2, d3,
               send_sem, recv_sem, out_sem, grad_sem):
    tile, blk = pl.program_id(0), pl.program_id(1)
    n_tile, n_blk = pl.num_programs(0), pl.num_programs(1)
    tick = tile * n_blk + blk
    first, last = tile == 0, tile == n_tile - 1
    halfs = slen // 2
    n_rows = nsq * slen
    rows = pl.ds(pl.multiple_of(blk * n_rows, n_rows), n_rows)
    loc = place()
    sems = (send_sem, recv_sem)
    streams = {}
    for t in range(keep_tiles):
        for kind, (order, acc, bufs, out) in enumerate(((XY, au_scr, (u0, u1, u2, u3), ru_ref), (YX, ad_scr, (d0, d1, d2, d3), rd_ref))):
            streams["abcdef"[2 * t + kind]] = Stream(
                2 * t + kind, order, (lambda c, acc=acc, t=t: acc.at[t, :, :, c]), tuple(b.at[t] for b in bufs), out.at[t], sems, loc)

    def handed(t):
        return [pltpu.make_async_copy(acc.at[keep_tiles + t], out.at[t], out_sem.at[2 * t + kind])
                for kind, (acc, out) in enumerate(((au_scr, gu_ref), (ad_scr, gd_ref)))]

    n_seq = g_scr.shape[0]
    z = lax.axis_index('cp')
    loads = [pltpu.make_async_copy(src, g_scr.at[:, part], grad_sem.at[part])
             for part, src in enumerate((grad_ref.at[pl.ds(pl.multiple_of(z * n_seq, n_seq), n_seq)], gp_ref))]

    @pl.when(tick == 0)
    def _():
        for load in loads:
            load.start()
        greet(loc[1])
        dvec_ref[...] = jnp.zeros_like(dvec_ref)
        dbup_ref[...] = jnp.zeros_like(dbup_ref)
        dwo_ref[...] = jnp.zeros_like(dwo_ref)

    follow(FFN_PLAN, tick, streams)

    @pl.when(tick == (n_tile - 1) * n_blk)
    def _():
        for copy in handed(0):
            copy.start()

    @pl.when(first)
    def _():
        for i in range(nsq):
            r = pl.ds(pl.multiple_of(blk * n_rows + i * slen, slen), slen)
            e = mm(one_hot_rows(cls_ref[i]), clean_table(et_ref).astype(BF), TN) * scale_ref[pl.ds(blk * nsq + i, 1), :]
            x1 = e + mm(o_ref[i].astype(BF), wo_ref[...], TN) + vecs_ref[5:6, :]
            xh, rstd = normalize(x1)
            xh_scr[r, :] = xh
            rs_scr[r, :] = rstd
            y_scr[r, :] = x1 + vecs_ref[8:9, :]
            n_scr[r, :] = (xh * vecs_ref[6:7, :] + vecs_ref[7:8, :]).astype(BF)
        dn_scr[rows, :] = jnp.zeros_like(dn_scr[rows, :])

    @pl.when(tick == 0)
    def _():
        for load in loads:
            load.wait()

    @pl.when(blk == 0)
    def _():
        au_scr[tile] = jnp.zeros(au_scr.shape[1:], F32)
        ad_scr[tile] = jnp.zeros(ad_scr.shape[1:], F32)

    n = n_scr[rows, :]
    g = g_scr[pl.ds(blk * nsq, nsq)].reshape(n_rows, -1)
    wu = wu_ref[...]
    wd = wd_ref[...]
    cols = pl.ds(pl.multiple_of(tile * wu.shape[1], wu.shape[1]), wu.shape[1])
    u = mm(n, wu, NN) + bup_ref[:, cols]
    phi = 0.5 + 0.5 * lax.erf(u * 0.7071067811865476)
    a = (u * phi).astype(BF)
    slope = phi + u * (jnp.exp(-0.5 * u * u) * 0.3989422804014327)
    y_scr[rows, :] += mm(a, wd, NN)
    du = mm(g, wd, NT) * slope
    dub = du.astype(BF)
    dbup_ref[:, cols] += csum(du)
    ad_scr[tile] += mm(a, g, TN).reshape(ad_scr.shape[1:])
    au_scr[tile] += mm(n, dub, TN).reshape(au_scr.shape[1:])
    dn_scr[rows, :] += mm(dub, wu, NT)

    @pl.when(last)
    def _():
        for i in range(nsq):
            r = pl.ds(pl.multiple_of(blk * n_rows + i * slen, slen), slen)
            out = y_scr[r, :].astype(BF)
            outm_ref[i] = out[:halfs]
            outp_ref[i] = out[halfs:]
            dn = dn_scr[r, :]
            xh = xh_scr[r, :]
            g32 = g_scr[blk * nsq + i].reshape(slen, -1).astype(F32)
            dx = g32 + norm_pull(dn, vecs_ref[6:7, :], xh, rs_scr[r, :])
            dvec_ref[...] += cat([csum(dx), csum(dn * xh), csum(dn), csum(g32)])
            dxb = dx.astype(BF)
            o = o_ref[i]
            dwo_ref[...] += mm(o.astype(BF), dxb, NN)
            do = mm(wo_ref[...], dxb, NT)
            do_ref[i] = do.astype(BF)
            delta_ref[i] = jnp.sum((do * o).reshape(n_heads, hd, slen), axis=1)
            csum_ref[i] = mm(one_hot_rows(cls_ref[i]), dxb, NN)

    @pl.when(tick == n_tile * n_blk - 1)
    def _():
        for copy in handed(1):
            copy.start()
        for copy in handed(0) + handed(1):
            copy.wait()
        act(streams, "e3f3")


def attn_bwd_kernel(hd, nh, lens, scale_ref, cls_ref, cos_ref, sin_ref, qkv_ref, do_ref, lse_ref, delta_ref, hc_ref,
                    wq_ref, wk_ref, wv_ref, csum_ref, ec_ref, vecs_ref, dvb_ref, dbup_ref, ru_in, rd_in, gu_ref, gd_ref, go_ref,
                    wup_ref, rd_out, ro_ref, rw_ref, tab_ref, vec_ref, bup_ref,
                    dlin_scr, bsum_scr, dcls_scr, dn_scr, dw_scr, small_scr, small_in, ru_ref,
                    u_own, d_own, o_own, u0, u1, u2, u3, d0, d1, d2, d3, o0, o1, o2, o3, w0, w1, w2, w3,
                    send_sem, recv_sem, own_sem, ssend, srecv):
    group, step = pl.program_id(0), pl.program_id(1)
    n_group, n_step = pl.num_programs(0), pl.num_programs(1)
    tick = group * n_step + step
    nsq = cls_ref.shape[0]
    n_seq = nsq * n_step
    gdim = nh * hd
    half = hd // 2
    loc = place()
    sems = (send_sem, recv_sem)
    streams = {"k": AllSum(small_scr, small_in, (ssend, srecv), loc)}
    keep_tiles = rd_in.shape[0]
    rd_ref = rd_out.at[keep_tiles:]
    for t in range(gu_ref.shape[0]):
        for kind, (order, src, own, bufs, out) in enumerate(((XY, gu_ref, u_own, (u0, u1, u2, u3), ru_ref),
                                                             (YX, gd_ref, d_own, (d0, d1, d2, d3), rd_ref))):
            num = 2 * t + kind
            streams["abcd"[num]] = Stream(num, order, (lambda c, src=src, t=t: src.at[t, :, :, c]), tuple(b.at[t] for b in bufs),
                                          out.at[t], sems, loc, (own.at[t], own_sem.at[num]))
    num = own_sem.shape[0] - 1
    streams["o"] = Stream(num, YX, lambda c: go_ref.at[:, :, c], (o0, o1, o2, o3), ro_ref, sems, loc, (o_own, own_sem.at[num]))
    n_piece = rw_ref.shape[1]
    for i, name in enumerate("vwxyzq"):
        t = min(i, rw_ref.shape[0] - 1)
        lo, hi = {"z": (0, n_piece // 2), "q": (n_piece // 2, n_piece)}.get(name, (0, n_piece))
        part = slice(lo, hi)
        streams[name] = Stream(num + 1 + i, (XY, YX)[i % 2], (lambda c, t=t, part=part: dw_scr.at[t, :, :, c, part]),
                               (w0.at[t, :, :, part], w1.at[t, :, part], w2.at[t, part], w3.at[t, part]), rw_ref.at[t, part],
                               sems, loc)

    @pl.when(tick == 0)
    def _():
        greet(loc[1])
        act(streams, "asbscsdsos")
        rd_out[:keep_tiles] = rd_in[...]
        dn_scr[...] = jnp.zeros_like(dn_scr)
        small_scr[...] = jnp.zeros_like(small_scr)

    follow(BWD_PLAN, tick, streams)

    @pl.when(step == 0)
    def _():
        bsum_scr[...] = jnp.zeros_like(bsum_scr)

    width = cos_ref.shape[-1]
    z = lax.axis_index('cp')
    lane = lax.broadcasted_iota(jnp.int32, (1, width), 1)
    pos = jnp.where(lane < width // 2, z * (width // 2) + lane, lane - z * (width // 2))
    kxs = [key_rows(pos, lens[z * n_seq + step * nsq + b]) for b in range(nsq)]
    vx = stack_rows([1.0] * 3, width)
    cos, sin = cos_ref[...], sin_ref[...]

    def put(b, base, val):
        dlin_scr[b, base:base + hd, :] = val.astype(BF)
        bsum_scr[base:base + hd, :] += val[:, :width // 2] + val[:, width // 2:]

    def unrope(val):
        return rope_fwd(val[:half], val[half:], cos, -sin)

    def extra(ref, b, h):
        return [t.astype(F32) for t in split3(-ref[b, pl.ds(group * nh + h, 1), :])]

    items = [(b, h, slice(h * hd, (h + 1) * hd)) for b in range(nsq) for h in range(nh)]
    qs, ks, vs = [[qkv_ref[b, part, span, :] for b, _, span in items] for part in range(3)]
    dos = [do_ref[b, span, :] for b, _, span in items]
    ss = [mm(cat([k, kxs[b]]), cat([q, stack_rows([1.0] + extra(lse_ref, b, h), width)]), TN)
          for k, q, (b, h, _) in zip(ks, qs, items)]
    dps = [mm(cat([v, vx]), cat([do, stack_rows(extra(delta_ref, b, h), width)]), TN) for v, do, (b, h, _) in zip(vs, dos, items)]
    ps = [jnp.exp(t) for t in ss]
    pbs = [p.astype(BF) for p in ps]
    dss = [(p * dp).astype(BF) for p, dp in zip(ps, dps)]
    dvs = [mm(do, p, NT) for do, p in zip(dos, pbs)]
    dks = [mm(q, ds, NT) for q, ds in zip(qs, dss)]
    dqs = [mm(k, ds, NN) for k, ds in zip(ks, dss)]
    for dq, dk, dv, (b, h, _) in zip(dqs, dks, dvs, items):
        put(b, h * hd, unrope(dq) * hd ** -0.5)
        put(b, gdim + h * hd, unrope(dk))
        put(b, 2 * gdim + h * hd, dv)

    for b in range(nsq):
        at = pl.multiple_of((step * nsq + b) * NCLS, NCLS)
        dcls_scr[pl.ds(at, NCLS), :] = mm(one_hot_rows(cls_ref[b]), dlin_scr[b], NT)

    @pl.when(step == n_step - 1)
    def _():
        hc = hc_ref[...]
        acc = dcls_scr[...]
        hi, lo, _ = split3(acc)
        dw_scr[group] = mm(cat([hc, hc]), cat([hi, lo]), TN).reshape(dw_scr.shape[1:])
        dn = dn_scr[...]
        cols = pl.ds(pl.multiple_of(group * gdim, gdim), gdim)
        bias = csum(jnp.transpose(bsum_scr[...]))
        for part, w_ref in enumerate((wq_ref, wk_ref, wv_ref)):
            sel = slice(part * gdim, (part + 1) * gdim)
            dn = dn + mm(hi[:, sel], w_ref[...], NT) + mm(lo[:, sel], w_ref[...], NT)
            small_scr[2 + part:3 + part, cols] = bias[:, sel]
        dn_scr[...] = dn

    @pl.when(tick == n_group * n_step - 1)
    def _():
        tail = BWD_TAIL.split(",")
        act(streams, tail[0])
        dn = dn_scr[...]
        xh, rstd = normalize(ec_ref[...])
        de = norm_pull(dn, vecs_ref[0:1, :], xh, rstd)
        small_scr[0:2, :] = cat([csum(dn * xh), csum(dn)])
        width = dn.shape[1]
        small_scr[5:13, :] = cat([dvb_ref[...]] + [dbup_ref[:, i * width:(i + 1) * width] for i in range(4)])
        tab = jnp.zeros((NCLS, dn.shape[1]), F32)
        for b in range(dcls_scr.shape[0] // NCLS):
            tab = tab + (de[b * NCLS:(b + 1) * NCLS] + csum_ref[b]) * scale_ref[b:b + 1, :]
        small_scr[16:, :] = jnp.where(row_iota(*tab.shape) == PAD_ID, 0.0, tab)
        act(streams, "ks")
        slab = FTILE // N_PIECE
        for text in tail[1:]:
            act(streams, text)
            if text == "k0":
                tiles = [*[ru_in[t] for t in range(keep_tiles)], *[ru_ref[t] for t in range(ru_ref.shape[0])]]
                wup_ref[...] = jnp.concatenate(
                    [t[:, f * slab:(f + 1) * slab] for f in range(N_PIECE) for t in tiles], axis=1)
        me = lax.axis_index('fsdp')

        def own(pick):
            return sum(jnp.where(me == f, pick(f), 0.0) for f in range(N_PIECE))

        def bup_slab(j, f):
            row, col = divmod((j * N_PIECE + f) * slab, width)
            return small_scr[9 + row:10 + row, col:col + slab]

        n_col = vec_ref.shape[1]
        vec_ref[...] = own(lambda f: small_scr[:9, f * n_col:(f + 1) * n_col])
        bup_ref[...] = jnp.concatenate(
            [own(functools.partial(bup_slab, j)) for j in range(bup_ref.shape[1] // slab)], axis=1)
        tab_ref[:NCLS, :] = small_scr[16:, :]
        tab_ref[NCLS:, :] = jnp.zeros_like(tab_ref[NCLS:, :])


def whole(shape):
    return pl.BlockSpec(shape, lambda *_: (0,) * len(shape), pipeline_mode=pl.Buffered(1))


def params(**kw):
    return pltpu.CompilerParams(vmem_limit_bytes=VMEM_LIMIT, **kw)


def cost(flops, moved):
    return pl.CostEstimate(flops=flops * 10**9, bytes_accessed=moved * 10**6, transcendentals=0)


def sds(*t):
    return jax.ShapeDtypeStruct(t, F32)


def sdb(*t):
    return jax.ShapeDtypeStruct(t, BF)


def vm(*t):
    return pltpu.VMEM(t, F32)


def dma(*t):
    return pltpu.SemaphoreType.DMA(t)


def stages(lead, *t):
    return [vm(*lead, 2, 2, *t), vm(*lead, 2, *t), vm(*lead, *t), vm(*lead, *t)]


SMEM = pl.BlockSpec(memory_space=pltpu.SMEM)


def attn_fwd(lens, tokens, embed, cos, sin, small, wq, wo, wu, wd, grad):
    n_seq, seq_half = tokens.shape[0] // 2, tokens.shape[1]
    slen = 2 * seq_half
    dim = wo.shape[1]
    hd = 2 * cos.shape[0]
    n_heads = dim // hd
    row = lambda *t: pl.BlockSpec((1,) + t, lambda i: (i, 0, 0))
    anyspace = pl.BlockSpec(memory_space=pl.ANY)
    held = [(jnp.int32, (n_seq, 1, slen)), (F32, (n_seq, 1)), (F32, (n_seq * NCLS, dim)), (BF, (n_seq * NCLS, dim)),
            (F32, (1, wu.shape[1])), (F32, (small.shape[0], dim))]
    far = [(N_PIECE, *wq.shape), (N_PIECE, *wo.shape), (N_PIECE, *wu.shape), (wd.shape[0], N_PIECE, *wd.shape[1:]), (n_seq, *grad.shape[1:])]
    args = (tokens, embed, cos, sin, small, wq, wo, wu, wd)
    return pl.pallas_call(
        functools.partial(attn_fwd_kernel, n_heads, hd),
        grid=(n_seq,),
        in_specs=[SMEM, *[whole(t.shape) for t in args], anyspace],
        out_specs=[row(3 * dim, slen), row(dim, slen), row(n_heads, slen), *[whole(t) for _, t in held], *[anyspace] * len(far)],
        out_shape=[sdb(n_seq, 3 * dim, slen), sds(n_seq, dim, slen), sds(n_seq, n_heads, slen),
                   *[jax.ShapeDtypeStruct(t, kind) for kind, t in held], *[sdb(*t) for t in far]],
        scratch_shapes=[vm(n_seq * NCLS, 3 * dim), vm(3 * dim, slen), pltpu.VMEM(wu.shape, BF),
                        pltpu.VMEM((n_seq, seq_half), jnp.int32), vm(N_PIECE, *small.shape),
                        pltpu.VMEM((N_PIECE, *wq.shape), BF), dma(6, 7), dma(6, 7), dma(6), dma(2), dma(2), pltpu.SemaphoreType.DMA],
        compiler_params=params(collective_id=2, has_side_effects=True), name="attn_fwd", cost_estimate=cost(20, 18),
    )(lens, *args, grad)


def ffn(scales, cls, o, grad, gp, etab, vecs, bup, wo, wu, wd, n_heads, hd, nsq=2, keep_tiles=3):
    n_seq, _, slen = cls.shape
    dim, ff = wu.shape
    tiles = ff // FTILE
    rest = tiles - keep_tiles
    halfs = slen // 2
    piece, slab = dim // N_PIECE, FTILE // N_PIECE
    n_blk = n_seq // nsq
    n_rows = n_seq * slen

    def blk(when, *t):
        return pl.BlockSpec((nsq,) + t, lambda j, r: (jnp.where(when(j), r, when(0) * (n_blk - 1)),) + (0,) * len(t))

    late = lambda j: j == tiles - 1
    both = lambda j: (j == 0) | (j == tiles - 1)
    anyspace = pl.BlockSpec(memory_space=pl.ANY)
    cube = (2,) * 3
    bwd_u, bwd_d = (rest, *cube, piece, FTILE), (rest, *cube, slab, dim)
    red_u, red_d = (keep_tiles, piece, FTILE), (keep_tiles, slab, dim)
    return pl.pallas_call(
        functools.partial(ffn_kernel, n_heads, hd, nsq, slen, keep_tiles),
        grid=(tiles, n_blk),
        in_specs=[whole(scales.shape), blk(both, 1, slen), blk(both, dim, slen), anyspace, anyspace,
                  whole(etab.shape), whole(vecs.shape), whole(bup.shape), whole(wo.shape),
                  pl.BlockSpec((dim, FTILE), lambda j, r: (0, j)), pl.BlockSpec((FTILE, dim), lambda j, r: (j, 0))],
        out_specs=[blk(late, halfs, dim), blk(late, halfs, dim), blk(late, dim, slen), blk(late, n_heads, slen),
                   blk(late, NCLS, dim), whole((4, dim)), whole((1, ff)), whole((dim, dim)), anyspace, anyspace,
                   whole(red_u), whole(red_d)],
        out_shape=[sdb(n_seq, halfs, dim), sdb(n_seq, halfs, dim), sdb(n_seq, dim, slen), sds(n_seq, n_heads, slen),
                   sds(n_seq, NCLS, dim), sds(4, dim), sds(1, ff), sds(dim, dim), sds(*bwd_u), sds(*bwd_d), sds(*red_u), sds(*red_d)],
        scratch_shapes=[vm(n_rows, dim), vm(n_rows, 1), pltpu.VMEM((n_rows, dim), BF), pltpu.VMEM((n_seq, 2, halfs, dim), BF),
                        vm(n_rows, dim), vm(n_rows, dim), vm(tiles, *cube, piece, FTILE), vm(tiles, *cube, slab, dim)]
        + stages((keep_tiles,), piece, FTILE) + stages((keep_tiles,), slab, dim)
        + [dma(2 * keep_tiles, 4), dma(2 * keep_tiles, 4), dma(2 * rest), dma(2)],
        compiler_params=params(collective_id=1, has_side_effects=True), name="ffn", cost_estimate=cost(60, 40),
    )(scales, cls, o, grad, gp, etab, vecs, bup, wo, wu, wd)


def attn_bwd(lens, scales, cls, cos, sin, qkv, do, lse, delta, hc, w, csums, ec, vecs, dvec_b, d_bup, red_wu, red_wd, d_wu, d_wd, d_wo,
             n_heads, hd, groups=5, nsq=2):
    n_seq, _, slen = cls.shape
    dim = n_heads * hd
    nh = n_heads // groups
    gdim = nh * hd
    cube = (2,) * 3
    blk = lambda *t: pl.BlockSpec((nsq,) + t, lambda g, i: (i,) + (0,) * len(t))
    wcol = lambda part: pl.BlockSpec((dim, gdim), lambda g, i: (0, part * groups + g))
    anyspace = pl.BlockSpec(memory_space=pl.ANY)
    ut, dt, ot = d_wu.shape[-2:], d_wd.shape[-2:], (dim // N_PIECE, dim)
    wt = (dim // N_PIECE, 3 * gdim)
    rest = d_wu.shape[0]
    fixed = (hc, csums, ec, vecs, dvec_b, d_bup, red_wu, red_wd)
    args = [lens, scales, cls, cos, sin, qkv.reshape(n_seq, 3, dim, slen), do, lse, delta, hc, w, w, w, *fixed[1:],
            d_wu, d_wd, d_wo.reshape(*cube, *ot)]
    specs = [SMEM, whole(scales.shape), blk(1, slen), whole(cos.shape), whole(sin.shape),
             pl.BlockSpec((nsq, 3, gdim, slen), lambda g, i: (i, 0, g, 0)), pl.BlockSpec((nsq, gdim, slen), lambda g, i: (i, g, 0)),
             blk(n_heads, slen), blk(n_heads, slen), whole(hc.shape), *[wcol(part) for part in range(3)],
             *[whole(t.shape) for t in fixed[1:]], *[anyspace] * 3]
    small = (16 + NCLS, dim)
    ff = d_bup.shape[1]
    shapes = [sds(ut[0], ff), sds(rest + red_wd.shape[0], *dt), sds(*ot), sds(groups, *wt), sds(NCLS + 1, dim), sds(9, dim // N_PIECE),
              sds(1, ff // N_PIECE)]
    n_str = 2 * rest + 1
    return pl.pallas_call(
        functools.partial(attn_bwd_kernel, hd, nh),
        grid=(groups, n_seq // nsq),
        in_specs=specs,
        out_specs=[whole(t.shape) for t in shapes],
        out_shape=shapes,
        scratch_shapes=[pltpu.VMEM((nsq, 3 * gdim, slen), BF), vm(3 * gdim, slen // 2), vm(n_seq * NCLS, 3 * gdim),
                        vm(n_seq * NCLS, dim), vm(groups, *cube, *wt), vm(*small), vm(4, *small), vm(rest, *ut),
                        vm(rest, 2, 2, *ut), vm(rest, 2, 2, *dt), vm(2, 2, *ot)]
        + stages((rest,), *ut) + stages((rest,), *dt) + stages((), *ot) + stages((groups,), *wt)
        + [dma(n_str + groups + 1, 4), dma(n_str + groups + 1, 4), dma(n_str), dma(4), dma(4)],
        compiler_params=params(collective_id=0, has_side_effects=True), name="attn_bwd", cost_estimate=cost(40, 20),
    )(*args)


def rope_tables(slen, hd):
    inv_freq = 1.0 / (ROPE_BASE ** (jnp.arange(0, hd, 2, dtype=F32) / hd))
    half = slen // 2
    turn = jnp.arange(slen).reshape(2, half)
    cp_index = lax.axis_index('cp')
    pos = jnp.where(cp_index == 0, turn, turn[::-1]).reshape(slen)
    angles = inv_freq[:, None] * pos.astype(F32)[None, :]
    return jnp.cos(angles), jnp.sin(angles)


def solution(mesh):
    swap = [(0, 1), (1, 0)]

    def local_step(tokens, lengths, embed_table, layer_vecs, w_qkv, w_out, w_up, b_up, w_down, grad_out):
        cp_index = lax.axis_index('cp')
        dim = embed_table.shape[1]
        n_heads, hd = w_qkv.shape[2], w_qkv.shape[3]
        slabs = w_up.shape[1] // FTILE
        cos_t, sin_t = rope_tables(2 * tokens.shape[1], hd)
        small = jnp.concatenate([layer_vecs, b_up.reshape(-1, layer_vecs.shape[1])], 0)
        small = jnp.pad(small, ((0, 16 - small.shape[0]), (0, 0)))
        (qkv, o, lse, cls, scales, e_cls, hc, up_b, vecs, w_all, out_w, up_w, down_w, g_peer) = attn_fwd(
            lengths, tokens, embed_table, cos_t, sin_t, small, w_qkv.reshape(w_qkv.shape[0], -1), w_out, w_up,
            w_down.reshape(slabs, -1, dim), grad_out)
        (out_m, out_p, do, delta, csums, dvec_b, d_bup, d_wo, d_wu, d_wd, red_wu, red_wd) = ffn(
            scales, cls, o, grad_out, g_peer, embed_table, vecs, up_b, out_w.reshape(dim, dim), up_w.reshape(dim, -1),
            down_w.reshape(-1, dim), n_heads, hd)
        out_back = lax.ppermute(out_p, 'cp', swap)
        layer_out = jnp.where(cp_index == 0, jnp.concatenate([out_m, out_back], 0), jnp.concatenate([out_back, out_m], 0))
        d_wup, d_wdown, d_wout, d_w, d_table, d_vecs, d_bup = attn_bwd(
            lengths, scales, cls, cos_t, sin_t, qkv, do, lse, delta, hc, w_all.reshape(dim, -1), csums, e_cls, vecs, dvec_b, d_bup,
            red_wu, red_wd, d_wu, d_wd, d_wo, n_heads, hd)
        groups = d_w.shape[0]
        d_w = jnp.transpose(d_w.reshape(groups, -1, 3, n_heads // groups, hd), (1, 2, 0, 3, 4)).reshape(w_qkv.shape)
        return layer_out, d_table, d_vecs, d_w, d_wout, d_wup, d_bup.reshape(-1), d_wdown.reshape(w_down.shape)

    in_specs = (P('fsdp', 'cp'), P('fsdp'), P(), P(None, 'fsdp'), P('fsdp', None, None, None), P('fsdp', None), P('fsdp', None), P('fsdp'), P('fsdp', None), P('fsdp', 'cp', None))
    out_specs = (P('fsdp', 'cp', None), P(), P(None, 'fsdp'), P('fsdp', None, None, None), P('fsdp', None), P('fsdp', None), P('fsdp'), P('fsdp', None))
    return jax.shard_map(local_step, mesh=mesh, in_specs=in_specs, out_specs=out_specs, check_vma=False)
```

```python
import functools

import jax
import jax.numpy as jnp
from jax import lax
from jax.experimental import pallas as pl
from jax.experimental.pallas import tpu as pltpu
from jax.sharding import PartitionSpec as P

MASK_ID = 32
PAD_ID = 1
NCLS = 32
LN_EPS = 1e-5
ROPE_BASE = 10000.0
TRAIN_RATIO = 0.15 * 0.8
NEG_BIG = -1e30
CORE, XDIR, YDIR = 1, 2, 4
ZDIR = 0
XY, YX = (XDIR, YDIR), (YDIR, XDIR)
BF = jnp.bfloat16
F32 = jnp.float32
VMEM_LIMIT = 67043328
NN = (((1,), (0,)), ((), ()))
NT = (((1,), (1,)), ((), ()))
TN = (((0,), (0,)), ((), ()))
FTILE = 512
N_PIECE = 8
FWD_HEADS = 10
MESH_ID = pl.DeviceIdType.MESH
FWD_PLAN = ("1:d0e0f0", "4:d1", "7:e1f1")
FFN_PLAN = ("4:asbs,5:a0b0,8:a1b1csds,9:c0d0,10:a2b2,12:c1d1esfs", "13:a3b3e0f0,14:c2d2,16:e1f1,17:c3d3,18:e2f2")
BWD_PLAN = ("1:a0b0,2:c0d0,4:vsa1b1,5:o0v0,7:c1d1,8:ws,9:a2b2w0,11:v1", "12:xso1,13:x0,14:c2d2,15:a3b3,16:ys,17:y0w1,18:o2v2x1")
BWD_TAIL = "zsqs,c3d3w2,z0q0,y1x2,k0,z1q1,y2,k1,v3w3x3o3,z2q2,k2,y3,z3q3,k3"


def mm(a, b, dims):
    return lax.dot_general(a, b, dims, preferred_element_type=F32)


def rmean(x):
    return jnp.mean(x, axis=-1, keepdims=True)


def csum(x):
    return jnp.sum(x, axis=0, keepdims=True)


def normalize(x):
    cen = x - rmean(x)
    rstd = lax.rsqrt(rmean(cen * cen) + LN_EPS)
    return cen * rstd, rstd


def norm_pull(dn, gain, xh, rstd):
    dy = dn * gain
    return rstd * (dy - rmean(dy) - xh * rmean(dy * xh))


def cat(parts):
    return jnp.concatenate(parts, axis=0)


def split3(x):
    hi = x.astype(BF)
    rest = x - hi.astype(F32)
    mid = rest.astype(BF)
    lo = (rest - mid.astype(F32)).astype(BF)
    return hi, mid, lo


def row_iota(rows, width):
    return lax.broadcasted_iota(jnp.int32, (rows, width), 0)


def one_hot_rows(cls):
    return (row_iota(NCLS, cls.shape[-1]) == cls).astype(BF)


def stack_rows(parts, width):
    row = row_iota(16, width)
    out = jnp.zeros(row.shape, F32)
    for i, part in enumerate(parts):
        out = jnp.where(row == i, part, out)
    return out.astype(BF)


def key_rows(pos, length):
    return stack_rows([jnp.where(pos < length, 0.0, NEG_BIG)] + [1.0] * 3, pos.shape[-1])


def rope_fwd(lo, hi, cos, sin):
    return cat([lo * cos - hi * sin, hi * cos + lo * sin])


def place():
    z, me = lax.axis_index('cp'), lax.axis_index('fsdp')
    bit = {CORE: lax.rem(me, XDIR), XDIR: lax.rem(me // XDIR, XDIR), YDIR: me // YDIR}
    partner = {way: (z, me + way - 2 * way * bit[way]) for way in bit}
    partner[ZDIR] = (1 - z, me)
    return bit, partner


def greet(partner):
    barrier = pltpu.get_barrier_semaphore()
    for way in partner:
        pl.semaphore_signal(barrier, inc=1, device_id=partner[way], device_id_type=MESH_ID)
    pl.semaphore_wait(barrier, len(partner))


def clean_table(ref):
    return jnp.where(row_iota(NCLS, ref.shape[1]) == PAD_ID, 0.0, ref[:NCLS, :].astype(F32))


class Stream:
    def __init__(self, num, order, src, bufs, out, sems, loc, own=None):
        self.num, self.order, self.src, self.bufs, self.out = num, order, src, bufs, out
        self.sems, self.loc, self.own = sems, loc, own

    def pick(self, stage, bit):
        way = self.order[stage - 1]
        buf = self.bufs[stage - 1]
        return buf.at[:, bit] if stage == 1 and way == XDIR else buf.at[bit]

    def copy(self, stage):
        bit, partner = self.loc
        way = (CORE, *self.order, ZDIR)[stage]
        if stage == 0:
            src = self.src(1 - bit[CORE])
        elif way == ZDIR:
            src = self.bufs[stage - 1]
        else:
            src = self.pick(stage, 1 - bit[way])
        return pltpu.make_async_remote_copy(
            src_ref=src, dst_ref=self.bufs[stage], send_sem=self.sems[0].at[self.num, stage],
            recv_sem=self.sems[1].at[self.num, stage], device_id=partner[way], device_id_type=MESH_ID)

    def local(self):
        return pltpu.make_async_copy(self.src(self.loc[0][CORE]), *self.own)

    def start(self):
        self.copy(0).start()
        if self.own:
            self.local().start()

    def advance(self, stage):
        bit = self.loc[0]
        buf = self.bufs[stage]
        self.copy(stage).wait()
        if stage == 0:
            if self.own:
                self.local().wait()
            buf[...] += self.own[0][...] if self.own else self.src(bit[CORE])[...]
        elif stage <= len(self.order):
            buf[...] += self.pick(stage, bit[self.order[stage - 1]])[...]
        else:
            self.out[...] = self.bufs[stage - 1][...] + buf[...]
            return
        self.copy(stage + 1).start()


class AllSum:
    def __init__(self, ref, bufs, sems, loc):
        self.ref, self.bufs, self.sems, self.loc = ref, bufs, sems, loc
        self.ways = (CORE, XDIR, YDIR, ZDIR)

    def copy(self, stage):
        return pltpu.make_async_remote_copy(
            src_ref=self.ref, dst_ref=self.bufs.at[stage], send_sem=self.sems[0].at[stage], recv_sem=self.sems[1].at[stage],
            device_id=self.loc[1][self.ways[stage]], device_id_type=MESH_ID)

    def start(self):
        self.copy(0).start()

    def advance(self, stage):
        self.copy(stage).wait()
        self.ref[...] += self.bufs[stage]
        if stage + 1 < len(self.ways):
            self.copy(stage + 1).start()


class Gather:
    def __init__(self, num, order, own, full, sems, loc, me):
        self.order, self.own, self.full, self.loc, self.me = order, own, full, loc, me
        self.send, self.recv, self.here = [sem.at[num] for sem in sems]

    def copies(self, stage, low=0, high=None):
        bit, partner = self.loc
        held, first = [self.me], 0
        for way in self.order[:stage]:
            first += len(held)
            held += [piece + way - 2 * way * bit[way] for piece in held]
        way = (*self.order, CORE)[stage]
        return [pltpu.make_async_remote_copy(
            src_ref=self.full(piece) if i else self.own, dst_ref=self.full(piece), send_sem=self.send.at[first + i],
            recv_sem=self.recv.at[first + i], device_id=partner[way], device_id_type=MESH_ID)
            for i, piece in enumerate(held) if i in range(len(held))[low:high]]

    def local(self):
        return pltpu.make_async_copy(self.own, self.full(self.me), self.here)

    def start(self, stage=0):
        todo = []
        if stage == 0:
            todo.append(self.local())
        if stage < len(self.order):
            todo += self.copies(stage)
        done = 1 << stage
        for copy in todo + self.copies(len(self.order), done >> 1, done):
            copy.start()

    def finish(self, stage):
        for copy in self.copies(stage):
            copy.wait()
        if stage == len(self.order):
            self.local().wait()

    def advance(self, stage):
        self.finish(stage)
        if stage < len(self.order):
            self.start(stage + 1)


def act(streams, text):
    for name, what in zip(text[::2], text[1::2]):
        if what == "s":
            streams[name].start()
        else:
            streams[name].advance(int(what))


def follow(plan, tick, streams):
    for item in ",".join(plan).split(","):
        when, text = item.split(":")

        @pl.when(tick == int(when))
        def _(text=text):
            act(streams, text)


def attn_fwd_kernel(n_heads, hd, lens, tok_ref, emb_ref, cos_ref, sin_ref, small_ref, wq_own, wo_own, wu_own, wd_own, grad_ref,
                    qkv_ref, o_ref, lse_ref, cls_ref, scale_ref, ec_ref, hc_ref, bup_ref, vecs_ref,
                    wq_out, wo_ref, wu_ref, wd_ref, gp_ref, class_scr, lin_scr, wu_scr, tok_scr, small_all, wq_ref,
                    send_sem, recv_sem, here_sem, swap_send, swap_recv, put_sem):
    step = pl.program_id(0)
    dim = n_heads * hd
    loc = place()
    z, me = lax.axis_index('cp'), lax.axis_index('fsdp')
    n_seq = tok_scr.shape[0]
    seq_half = tok_scr.shape[1]
    slen = 2 * seq_half
    mine, other = [pl.ds(pl.multiple_of(zz * n_seq, n_seq), n_seq) for zz in (z, 1 - z)]
    sems = (send_sem, recv_sem, here_sem)
    cut = 48
    streams = {}
    for name, order, own, full in (
            ("a", XY, small_ref, lambda f: small_all.at[f]),
            ("b", XY, wq_own.at[:cut], lambda f: wq_ref.at[f, :cut]),
            ("c", YX, wq_own.at[cut:], lambda f: wq_ref.at[f, cut:]),
            ("d", XY, wo_own, lambda f: wo_ref.at[f]),
            ("e", XY, wu_scr, lambda f: wu_ref.at[f]),
            ("f", YX, wd_own, lambda f: wd_ref.at[:, f])):
        streams[name] = Gather(len(streams), order, own, full, sems, loc, me)

    def swap(num, src, dst):
        return pltpu.make_async_remote_copy(src_ref=src, dst_ref=dst, send_sem=swap_send.at[num], recv_sem=swap_recv.at[num],
                                            device_id=loc[1][ZDIR], device_id_type=MESH_ID)

    swaps = [swap(0, tok_ref.at[other], tok_scr), swap(1, grad_ref.at[other], gp_ref)]
    keep = pltpu.make_async_copy(wq_ref, wq_out, put_sem)
    lane = lax.broadcasted_iota(jnp.int32, (1, slen), 1)
    pos = jnp.where(lane < seq_half, z * seq_half + lane, lane - z * seq_half)

    @pl.when(step == 0)
    def _():
        greet(loc[1])
        for copy in swaps:
            copy.start()
        act(streams, "asbscs")
        x = wu_own[...]
        n_slab = FTILE // N_PIECE
        slabs = x.shape[1] // FTILE
        wu_scr[...] = jnp.concatenate(
            [x[:, (f * slabs + j) * n_slab:(f * slabs + j + 1) * n_slab] for j in range(slabs) for f in range(N_PIECE)], axis=1)
        act(streams, "a0b0c0dsesfsa1")
        swaps[0].wait()
        tok = jnp.concatenate([tok_ref[mine, :], tok_scr[...]], axis=1)
        row = row_iota(n_seq, 1)
        length = jnp.zeros(row.shape, jnp.int32)
        for i in range(n_seq):
            length = jnp.where(row == i, lens[z * n_seq + i], length)
        masked = tok == MASK_ID
        count = jnp.sum(jnp.where(masked, 1.0, 0.0), axis=-1, keepdims=True)
        scale = (1.0 - TRAIN_RATIO) / (1.0 - count / length.astype(F32))
        scale_ref[...] = scale
        cls = jnp.where(masked | (pos >= length), PAD_ID, tok)
        emb = clean_table(emb_ref)
        for i in range(n_seq):
            cls_ref[i] = cls[i:i + 1]
            ec_ref[i * NCLS:(i + 1) * NCLS, :] = emb * scale[i:i + 1]
        act(streams, "a2")
        vecs_ref[...] = jnp.concatenate([small_all[f] for f in range(N_PIECE)], axis=1)
        hc_ref[...] = (normalize(ec_ref[...])[0] * vecs_ref[0:1, :] + vecs_ref[1:2, :]).astype(BF)
        flat = [jnp.concatenate([small_all[f, 9 + r:10 + r] for r in range(4)], axis=1) for f in range(N_PIECE)]
        bup_ref[...] = jnp.concatenate([t[:, j * n_slab:(j + 1) * n_slab] for j in range(slabs) for t in flat], axis=1)
        act(streams, "b1c1b2c2")
        keep.start()
        full = mm(hc_ref[...], wq_ref[...].reshape(dim, 3 * dim), NN)
        for part in range(3):
            cols = slice(part * dim, (part + 1) * dim)
            val = full[:, cols] + vecs_ref[2 + part:3 + part, :]
            class_scr[:, cols] = val if part else val * hd ** -0.5

    follow(FWD_PLAN, step, streams)
    rows = class_scr[pl.ds(step * NCLS, NCLS), :]
    hot = one_hot_rows(cls_ref[step])
    hot3 = cat([hot] * 3)
    for part in range(3):
        cols = slice(part * dim, (part + 1) * dim)
        lin_scr[cols, :] = mm(cat(split3(rows[:, cols])), hot3, TN)
    kx = key_rows(pos, lens[z * n_seq + step])
    qx = stack_rows([1.0], kx.shape[-1])
    cos, sin = cos_ref[...], sin_ref[...]
    half = hd // 2

    def heads(hs):
        bases = [pl.multiple_of(h * hd, hd) for h in hs]
        qs, ks, vs = [], [], []
        for base in bases:
            piece = lambda off, size: lin_scr[pl.ds(base + off, size), :]
            qs.append(rope_fwd(piece(0, half), piece(half, half), cos, sin).astype(BF))
            ks.append(rope_fwd(piece(dim, half), piece(dim + half, half), cos, sin).astype(BF))
            vs.append(piece(2 * dim, hd).astype(BF))
            for part, val in enumerate((qs[-1], ks[-1], vs[-1])):
                qkv_ref[0, pl.ds(part * dim + base, hd), :] = val
        ss = [mm(cat([k, kx]), cat([q, qx]), TN) for q, k in zip(qs, ks)]
        tops = [jnp.max(s, axis=0, keepdims=True) for s in ss]
        ps = [jnp.exp(s - t) for s, t in zip(ss, tops)]
        tots = [csum(p) for p in ps]
        os = [mm(v, p.astype(BF), NN) for v, p in zip(vs, ps)]
        for h, base, o, tot, top in zip(hs, bases, os, tots, tops):
            o_ref[0, pl.ds(base, hd), :] = o / tot
            lse_ref[0, pl.ds(h, 1), :] = top + jnp.log(tot)

    def body(i, carry):
        heads([i * FWD_HEADS + u for u in range(FWD_HEADS)])
        return carry

    lax.fori_loop(0, n_heads // FWD_HEADS, body, 0)

    @pl.when(step == n_seq - 1)
    def _():
        act(streams, "d2e2f2")
        swaps[1].wait()
        keep.wait()


def ffn_kernel(n_heads, hd, nsq, slen, keep_tiles,
               scale_ref, cls_ref, o_ref, grad_ref, gp_ref, et_ref, vecs_ref, bup_ref, wo_ref, wu_ref, wd_ref,
               outm_ref, outp_ref, do_ref, delta_ref, csum_ref, dvec_ref, dbup_ref, dwo_ref, gu_ref, gd_ref, ru_ref, rd_ref,
               xh_scr, rs_scr, n_scr, g_scr, y_scr, dn_scr, au_scr, ad_scr, u0, u1, u2, u3, d0, d1, d2, d3,
               send_sem, recv_sem, out_sem, grad_sem):
    tile, blk = pl.program_id(0), pl.program_id(1)
    n_tile, n_blk = pl.num_programs(0), pl.num_programs(1)
    tick = tile * n_blk + blk
    first, last = tile == 0, tile == n_tile - 1
    halfs = slen // 2
    n_rows = nsq * slen
    rows = pl.ds(pl.multiple_of(blk * n_rows, n_rows), n_rows)
    loc = place()
    sems = (send_sem, recv_sem)
    streams = {}
    for t in range(keep_tiles):
        for kind, (order, acc, bufs, out) in enumerate(((XY, au_scr, (u0, u1, u2, u3), ru_ref), (YX, ad_scr, (d0, d1, d2, d3), rd_ref))):
            streams["abcdef"[2 * t + kind]] = Stream(
                2 * t + kind, order, (lambda c, acc=acc, t=t: acc.at[t, :, :, c]), tuple(b.at[t] for b in bufs), out.at[t], sems, loc)

    def handed(t):
        return [pltpu.make_async_copy(acc.at[keep_tiles + t], out.at[t], out_sem.at[2 * t + kind])
                for kind, (acc, out) in enumerate(((au_scr, gu_ref), (ad_scr, gd_ref)))]

    n_seq = g_scr.shape[0]
    z = lax.axis_index('cp')
    loads = [pltpu.make_async_copy(src, g_scr.at[:, part], grad_sem.at[part])
             for part, src in enumerate((grad_ref.at[pl.ds(pl.multiple_of(z * n_seq, n_seq), n_seq)], gp_ref))]

    @pl.when(tick == 0)
    def _():
        for load in loads:
            load.start()
        greet(loc[1])
        dvec_ref[...] = jnp.zeros_like(dvec_ref)
        dbup_ref[...] = jnp.zeros_like(dbup_ref)
        dwo_ref[...] = jnp.zeros_like(dwo_ref)

    follow(FFN_PLAN, tick, streams)

    @pl.when(tick == (n_tile - 1) * n_blk)
    def _():
        for copy in handed(0):
            copy.start()

    @pl.when(first)
    def _():
        for i in range(nsq):
            r = pl.ds(pl.multiple_of(blk * n_rows + i * slen, slen), slen)
            e = mm(one_hot_rows(cls_ref[i]), clean_table(et_ref).astype(BF), TN) * scale_ref[pl.ds(blk * nsq + i, 1), :]
            x1 = e + mm(o_ref[i].astype(BF), wo_ref[...], TN) + vecs_ref[5:6, :]
            xh, rstd = normalize(x1)
            xh_scr[r, :] = xh
            rs_scr[r, :] = rstd
            y_scr[r, :] = x1 + vecs_ref[8:9, :]
            n_scr[r, :] = (xh * vecs_ref[6:7, :] + vecs_ref[7:8, :]).astype(BF)
        dn_scr[rows, :] = jnp.zeros_like(dn_scr[rows, :])

    @pl.when(tick == 0)
    def _():
        for load in loads:
            load.wait()

    @pl.when(blk == 0)
    def _():
        au_scr[tile] = jnp.zeros(au_scr.shape[1:], F32)
        ad_scr[tile] = jnp.zeros(ad_scr.shape[1:], F32)

    n = n_scr[rows, :]
    g = g_scr[pl.ds(blk * nsq, nsq)].reshape(n_rows, -1)
    wu = wu_ref[...]
    wd = wd_ref[...]
    cols = pl.ds(pl.multiple_of(tile * wu.shape[1], wu.shape[1]), wu.shape[1])
    u = mm(n, wu, NN) + bup_ref[:, cols]
    dg = mm(g, wd, NT)
    phi = 0.5 + 0.5 * lax.erf(u * 0.7071067811865476)
    a = (u * phi).astype(BF)
    slope = phi + u * (jnp.exp(-0.5 * u * u) * 0.3989422804014327)
    du = dg * slope
    dub = du.astype(BF)
    y_scr[rows, :] += mm(a, wd, NN)
    dbup_ref[:, cols] += csum(du)
    ad_scr[tile] += mm(a, g, TN).reshape(ad_scr.shape[1:])
    au_scr[tile] += mm(n, dub, TN).reshape(au_scr.shape[1:])
    dn_scr[rows, :] += mm(dub, wu, NT)

    @pl.when(last)
    def _():
        for i in range(nsq):
            r = pl.ds(pl.multiple_of(blk * n_rows + i * slen, slen), slen)
            out = y_scr[r, :].astype(BF)
            outm_ref[i] = out[:halfs]
            outp_ref[i] = out[halfs:]
            dn = dn_scr[r, :]
            xh = xh_scr[r, :]
            g32 = g_scr[blk * nsq + i].reshape(slen, -1).astype(F32)
            dx = g32 + norm_pull(dn, vecs_ref[6:7, :], xh, rs_scr[r, :])
            dvec_ref[...] += cat([csum(dx), csum(dn * xh), csum(dn), csum(g32)])
            dxb = dx.astype(BF)
            o = o_ref[i]
            dwo_ref[...] += mm(o.astype(BF), dxb, NN)
            do = mm(wo_ref[...], dxb, NT)
            do_ref[i] = do.astype(BF)
            delta_ref[i] = jnp.sum((do * o).reshape(n_heads, hd, slen), axis=1)
            csum_ref[i] = mm(one_hot_rows(cls_ref[i]), dxb, NN)

    @pl.when(tick == n_tile * n_blk - 1)
    def _():
        for copy in handed(1):
            copy.start()
        for copy in handed(0) + handed(1):
            copy.wait()
        act(streams, "e3f3")


def attn_bwd_kernel(hd, nh, lens, scale_ref, cls_ref, cos_ref, sin_ref, qkv_ref, do_ref, lse_ref, delta_ref, hc_ref,
                    wq_ref, wk_ref, wv_ref, csum_ref, ec_ref, vecs_ref, dvb_ref, dbup_ref, ru_in, rd_in, gu_ref, gd_ref, go_ref,
                    wup_ref, rd_out, ro_ref, rw_ref, tab_ref, vec_ref, bup_ref,
                    dlin_scr, bsum_scr, dcls_scr, dn_scr, dw_scr, small_scr, small_in, ru_ref,
                    u_own, d_own, o_own, u0, u1, u2, u3, d0, d1, d2, d3, o0, o1, o2, o3, w0, w1, w2, w3,
                    send_sem, recv_sem, own_sem, ssend, srecv):
    group, step = pl.program_id(0), pl.program_id(1)
    n_group, n_step = pl.num_programs(0), pl.num_programs(1)
    tick = group * n_step + step
    nsq = cls_ref.shape[0]
    n_seq = nsq * n_step
    gdim = nh * hd
    half = hd // 2
    loc = place()
    sems = (send_sem, recv_sem)
    streams = {"k": AllSum(small_scr, small_in, (ssend, srecv), loc)}
    keep_tiles = rd_in.shape[0]
    rd_ref = rd_out.at[keep_tiles:]
    for t in range(gu_ref.shape[0]):
        for kind, (order, src, own, bufs, out) in enumerate(((XY, gu_ref, u_own, (u0, u1, u2, u3), ru_ref),
                                                             (YX, gd_ref, d_own, (d0, d1, d2, d3), rd_ref))):
            num = 2 * t + kind
            streams["abcd"[num]] = Stream(num, order, (lambda c, src=src, t=t: src.at[t, :, :, c]), tuple(b.at[t] for b in bufs),
                                          out.at[t], sems, loc, (own.at[t], own_sem.at[num]))
    num = own_sem.shape[0] - 1
    streams["o"] = Stream(num, YX, lambda c: go_ref.at[:, :, c], (o0, o1, o2, o3), ro_ref, sems, loc, (o_own, own_sem.at[num]))
    n_piece = rw_ref.shape[1]
    for i, name in enumerate("vwxyzq"):
        t = min(i, rw_ref.shape[0] - 1)
        lo, hi = {"z": (0, n_piece // 2), "q": (n_piece // 2, n_piece)}.get(name, (0, n_piece))
        part = slice(lo, hi)
        streams[name] = Stream(num + 1 + i, (XY, YX)[i % 2], (lambda c, t=t, part=part: dw_scr.at[t, :, :, c, part]),
                               (w0.at[t, :, :, part], w1.at[t, :, part], w2.at[t, part], w3.at[t, part]), rw_ref.at[t, part],
                               sems, loc)

    @pl.when(tick == 0)
    def _():
        greet(loc[1])
        act(streams, "asbscsdsos")
        rd_out[:keep_tiles] = rd_in[...]
        dn_scr[...] = jnp.zeros_like(dn_scr)
        small_scr[...] = jnp.zeros_like(small_scr)

    follow(BWD_PLAN, tick, streams)

    @pl.when(step == 0)
    def _():
        bsum_scr[...] = jnp.zeros_like(bsum_scr)

    width = cos_ref.shape[-1]
    z = lax.axis_index('cp')
    lane = lax.broadcasted_iota(jnp.int32, (1, width), 1)
    pos = jnp.where(lane < width // 2, z * (width // 2) + lane, lane - z * (width // 2))
    kxs = [key_rows(pos, lens[z * n_seq + step * nsq + b]) for b in range(nsq)]
    vx = stack_rows([1.0] * 3, width)
    cos, sin = cos_ref[...], sin_ref[...]

    def put(b, base, val):
        dlin_scr[b, base:base + hd, :] = val.astype(BF)
        bsum_scr[base:base + hd, :] += val[:, :width // 2] + val[:, width // 2:]

    def unrope(val):
        return rope_fwd(val[:half], val[half:], cos, -sin)

    def extra(ref, b, h):
        return [t.astype(F32) for t in split3(-ref[b, pl.ds(group * nh + h, 1), :])]

    items = [(b, h, slice(h * hd, (h + 1) * hd)) for b in range(nsq) for h in range(nh)]
    qs, ks, vs = [[qkv_ref[b, part, span, :] for b, _, span in items] for part in range(3)]
    dos = [do_ref[b, span, :] for b, _, span in items]
    ss = [mm(cat([k, kxs[b]]), cat([q, stack_rows([1.0] + extra(lse_ref, b, h), width)]), TN)
          for k, q, (b, h, _) in zip(ks, qs, items)]
    dps = [mm(cat([v, vx]), cat([do, stack_rows(extra(delta_ref, b, h), width)]), TN) for v, do, (b, h, _) in zip(vs, dos, items)]
    ps = [jnp.exp(t) for t in ss]
    pbs = [p.astype(BF) for p in ps]
    dss = [(p * dp).astype(BF) for p, dp in zip(ps, dps)]
    dvs = [mm(do, p, NT) for do, p in zip(dos, pbs)]
    dks = [mm(q, ds, NT) for q, ds in zip(qs, dss)]
    dqs = [mm(k, ds, NN) for k, ds in zip(ks, dss)]
    for dq, dk, dv, (b, h, _) in zip(dqs, dks, dvs, items):
        put(b, h * hd, unrope(dq) * hd ** -0.5)
        put(b, gdim + h * hd, unrope(dk))
        put(b, 2 * gdim + h * hd, dv)

    for b in range(nsq):
        at = pl.multiple_of((step * nsq + b) * NCLS, NCLS)
        dcls_scr[pl.ds(at, NCLS), :] = mm(one_hot_rows(cls_ref[b]), dlin_scr[b], NT)

    @pl.when(step == n_step - 1)
    def _():
        hc = hc_ref[...]
        acc = dcls_scr[...]
        hi, lo, _ = split3(acc)
        dw_scr[group] = mm(cat([hc, hc]), cat([hi, lo]), TN).reshape(dw_scr.shape[1:])
        dn = dn_scr[...]
        cols = pl.ds(pl.multiple_of(group * gdim, gdim), gdim)
        bias = csum(jnp.transpose(bsum_scr[...]))
        for part, w_ref in enumerate((wq_ref, wk_ref, wv_ref)):
            sel = slice(part * gdim, (part + 1) * gdim)
            dn = dn + mm(hi[:, sel], w_ref[...], NT) + mm(lo[:, sel], w_ref[...], NT)
            small_scr[2 + part:3 + part, cols] = bias[:, sel]
        dn_scr[...] = dn

    @pl.when(tick == n_group * n_step - 1)
    def _():
        tail = BWD_TAIL.split(",")
        act(streams, tail[0])
        dn = dn_scr[...]
        xh, rstd = normalize(ec_ref[...])
        de = norm_pull(dn, vecs_ref[0:1, :], xh, rstd)
        small_scr[0:2, :] = cat([csum(dn * xh), csum(dn)])
        width = dn.shape[1]
        small_scr[5:13, :] = cat([dvb_ref[...]] + [dbup_ref[:, i * width:(i + 1) * width] for i in range(4)])
        tab = jnp.zeros((NCLS, dn.shape[1]), F32)
        for b in range(dcls_scr.shape[0] // NCLS):
            tab = tab + (de[b * NCLS:(b + 1) * NCLS] + csum_ref[b]) * scale_ref[b:b + 1, :]
        small_scr[16:, :] = jnp.where(row_iota(*tab.shape) == PAD_ID, 0.0, tab)
        act(streams, "ks")
        slab = FTILE // N_PIECE
        for text in tail[1:]:
            act(streams, text)
            if text == "k0":
                tiles = [*[ru_in[t] for t in range(keep_tiles)], *[ru_ref[t] for t in range(ru_ref.shape[0])]]
                wup_ref[...] = jnp.concatenate(
                    [t[:, f * slab:(f + 1) * slab] for f in range(N_PIECE) for t in tiles], axis=1)
        me = lax.axis_index('fsdp')

        def own(pick):
            return sum(jnp.where(me == f, pick(f), 0.0) for f in range(N_PIECE))

        def bup_slab(j, f):
            row, col = divmod((j * N_PIECE + f) * slab, width)
            return small_scr[9 + row:10 + row, col:col + slab]

        n_col = vec_ref.shape[1]
        vec_ref[...] = own(lambda f: small_scr[:9, f * n_col:(f + 1) * n_col])
        bup_ref[...] = jnp.concatenate(
            [own(functools.partial(bup_slab, j)) for j in range(bup_ref.shape[1] // slab)], axis=1)
        tab_ref[:NCLS, :] = small_scr[16:, :]
        tab_ref[NCLS:, :] = jnp.zeros_like(tab_ref[NCLS:, :])


def whole(shape):
    return pl.BlockSpec(shape, lambda *_: (0,) * len(shape), pipeline_mode=pl.Buffered(1))


def params(**kw):
    return pltpu.CompilerParams(vmem_limit_bytes=VMEM_LIMIT, **kw)


def cost(flops, moved):
    return pl.CostEstimate(flops=flops * 10**9, bytes_accessed=moved * 10**6, transcendentals=0)


def sds(*t):
    return jax.ShapeDtypeStruct(t, F32)


def sdb(*t):
    return jax.ShapeDtypeStruct(t, BF)


def vm(*t):
    return pltpu.VMEM(t, F32)


def dma(*t):
    return pltpu.SemaphoreType.DMA(t)


def stages(lead, *t):
    return [vm(*lead, 2, 2, *t), vm(*lead, 2, *t), vm(*lead, *t), vm(*lead, *t)]


SMEM = pl.BlockSpec(memory_space=pltpu.SMEM)


def attn_fwd(lens, tokens, embed, cos, sin, small, wq, wo, wu, wd, grad):
    n_seq, seq_half = tokens.shape[0] // 2, tokens.shape[1]
    slen = 2 * seq_half
    dim = wo.shape[1]
    hd = 2 * cos.shape[0]
    n_heads = dim // hd
    row = lambda *t: pl.BlockSpec((1,) + t, lambda i: (i, 0, 0))
    anyspace = pl.BlockSpec(memory_space=pl.ANY)
    held = [(jnp.int32, (n_seq, 1, slen)), (F32, (n_seq, 1)), (F32, (n_seq * NCLS, dim)), (BF, (n_seq * NCLS, dim)),
            (F32, (1, wu.shape[1])), (F32, (small.shape[0], dim))]
    far = [(N_PIECE, *wq.shape), (N_PIECE, *wo.shape), (N_PIECE, *wu.shape), (wd.shape[0], N_PIECE, *wd.shape[1:]), (n_seq, *grad.shape[1:])]
    args = (tokens, embed, cos, sin, small, wq, wo, wu, wd)
    return pl.pallas_call(
        functools.partial(attn_fwd_kernel, n_heads, hd),
        grid=(n_seq,),
        in_specs=[SMEM, *[whole(t.shape) for t in args], anyspace],
        out_specs=[row(3 * dim, slen), row(dim, slen), row(n_heads, slen), *[whole(t) for _, t in held], *[anyspace] * len(far)],
        out_shape=[sdb(n_seq, 3 * dim, slen), sds(n_seq, dim, slen), sds(n_seq, n_heads, slen),
                   *[jax.ShapeDtypeStruct(t, kind) for kind, t in held], *[sdb(*t) for t in far]],
        scratch_shapes=[vm(n_seq * NCLS, 3 * dim), vm(3 * dim, slen), pltpu.VMEM(wu.shape, BF),
                        pltpu.VMEM((n_seq, seq_half), jnp.int32), vm(N_PIECE, *small.shape),
                        pltpu.VMEM((N_PIECE, *wq.shape), BF), dma(6, 7), dma(6, 7), dma(6), dma(2), dma(2), pltpu.SemaphoreType.DMA],
        compiler_params=params(collective_id=2, has_side_effects=True), name="attn_fwd", cost_estimate=cost(20, 18),
    )(lens, *args, grad)


def ffn(scales, cls, o, grad, gp, etab, vecs, bup, wo, wu, wd, n_heads, hd, nsq=2, keep_tiles=3):
    n_seq, _, slen = cls.shape
    dim, ff = wu.shape
    tiles = ff // FTILE
    rest = tiles - keep_tiles
    halfs = slen // 2
    piece, slab = dim // N_PIECE, FTILE // N_PIECE
    n_blk = n_seq // nsq
    n_rows = n_seq * slen

    def blk(when, *t):
        return pl.BlockSpec((nsq,) + t, lambda j, r: (jnp.where(when(j), r, when(0) * (n_blk - 1)),) + (0,) * len(t))

    late = lambda j: j == tiles - 1
    both = lambda j: (j == 0) | (j == tiles - 1)
    anyspace = pl.BlockSpec(memory_space=pl.ANY)
    cube = (2,) * 3
    bwd_u, bwd_d = (rest, *cube, piece, FTILE), (rest, *cube, slab, dim)
    red_u, red_d = (keep_tiles, piece, FTILE), (keep_tiles, slab, dim)
    return pl.pallas_call(
        functools.partial(ffn_kernel, n_heads, hd, nsq, slen, keep_tiles),
        grid=(tiles, n_blk),
        in_specs=[whole(scales.shape), blk(both, 1, slen), blk(both, dim, slen), anyspace, anyspace,
                  whole(etab.shape), whole(vecs.shape), whole(bup.shape), whole(wo.shape),
                  pl.BlockSpec((dim, FTILE), lambda j, r: (0, j)), pl.BlockSpec((FTILE, dim), lambda j, r: (j, 0))],
        out_specs=[blk(late, halfs, dim), blk(late, halfs, dim), blk(late, dim, slen), blk(late, n_heads, slen),
                   blk(late, NCLS, dim), whole((4, dim)), whole((1, ff)), whole((dim, dim)), anyspace, anyspace,
                   whole(red_u), whole(red_d)],
        out_shape=[sdb(n_seq, halfs, dim), sdb(n_seq, halfs, dim), sdb(n_seq, dim, slen), sds(n_seq, n_heads, slen),
                   sds(n_seq, NCLS, dim), sds(4, dim), sds(1, ff), sds(dim, dim), sds(*bwd_u), sds(*bwd_d), sds(*red_u), sds(*red_d)],
        scratch_shapes=[vm(n_rows, dim), vm(n_rows, 1), pltpu.VMEM((n_rows, dim), BF), pltpu.VMEM((n_seq, 2, halfs, dim), BF),
                        vm(n_rows, dim), vm(n_rows, dim), vm(tiles, *cube, piece, FTILE), vm(tiles, *cube, slab, dim)]
        + stages((keep_tiles,), piece, FTILE) + stages((keep_tiles,), slab, dim)
        + [dma(2 * keep_tiles, 4), dma(2 * keep_tiles, 4), dma(2 * rest), dma(2)],
        compiler_params=params(collective_id=1, has_side_effects=True), name="ffn", cost_estimate=cost(60, 40),
    )(scales, cls, o, grad, gp, etab, vecs, bup, wo, wu, wd)


def attn_bwd(lens, scales, cls, cos, sin, qkv, do, lse, delta, hc, w, csums, ec, vecs, dvec_b, d_bup, red_wu, red_wd, d_wu, d_wd, d_wo,
             n_heads, hd, groups=5, nsq=2):
    n_seq, _, slen = cls.shape
    dim = n_heads * hd
    nh = n_heads // groups
    gdim = nh * hd
    cube = (2,) * 3
    blk = lambda *t: pl.BlockSpec((nsq,) + t, lambda g, i: (i,) + (0,) * len(t))
    wcol = lambda part: pl.BlockSpec((dim, gdim), lambda g, i: (0, part * groups + g))
    anyspace = pl.BlockSpec(memory_space=pl.ANY)
    ut, dt, ot = d_wu.shape[-2:], d_wd.shape[-2:], (dim // N_PIECE, dim)
    wt = (dim // N_PIECE, 3 * gdim)
    rest = d_wu.shape[0]
    fixed = (hc, csums, ec, vecs, dvec_b, d_bup, red_wu, red_wd)
    args = [lens, scales, cls, cos, sin, qkv.reshape(n_seq, 3, dim, slen), do, lse, delta, hc, w, w, w, *fixed[1:],
            d_wu, d_wd, d_wo.reshape(*cube, *ot)]
    specs = [SMEM, whole(scales.shape), blk(1, slen), whole(cos.shape), whole(sin.shape),
             pl.BlockSpec((nsq, 3, gdim, slen), lambda g, i: (i, 0, g, 0)), pl.BlockSpec((nsq, gdim, slen), lambda g, i: (i, g, 0)),
             blk(n_heads, slen), blk(n_heads, slen), whole(hc.shape), *[wcol(part) for part in range(3)],
             *[whole(t.shape) for t in fixed[1:]], *[anyspace] * 3]
    small = (16 + NCLS, dim)
    ff = d_bup.shape[1]
    shapes = [sds(ut[0], ff), sds(rest + red_wd.shape[0], *dt), sds(*ot), sds(groups, *wt), sds(NCLS + 1, dim), sds(9, dim // N_PIECE),
              sds(1, ff // N_PIECE)]
    n_str = 2 * rest + 1
    return pl.pallas_call(
        functools.partial(attn_bwd_kernel, hd, nh),
        grid=(groups, n_seq // nsq),
        in_specs=specs,
        out_specs=[whole(t.shape) for t in shapes],
        out_shape=shapes,
        scratch_shapes=[pltpu.VMEM((nsq, 3 * gdim, slen), BF), vm(3 * gdim, slen // 2), vm(n_seq * NCLS, 3 * gdim),
                        vm(n_seq * NCLS, dim), vm(groups, *cube, *wt), vm(*small), vm(4, *small), vm(rest, *ut),
                        vm(rest, 2, 2, *ut), vm(rest, 2, 2, *dt), vm(2, 2, *ot)]
        + stages((rest,), *ut) + stages((rest,), *dt) + stages((), *ot) + stages((groups,), *wt)
        + [dma(n_str + groups + 1, 4), dma(n_str + groups + 1, 4), dma(n_str), dma(4), dma(4)],
        compiler_params=params(collective_id=0, has_side_effects=True), name="attn_bwd", cost_estimate=cost(40, 20),
    )(*args)


def rope_tables(slen, hd):
    inv_freq = 1.0 / (ROPE_BASE ** (jnp.arange(0, hd, 2, dtype=F32) / hd))
    half = slen // 2
    turn = jnp.arange(slen).reshape(2, half)
    cp_index = lax.axis_index('cp')
    pos = jnp.where(cp_index == 0, turn, turn[::-1]).reshape(slen)
    angles = inv_freq[:, None] * pos.astype(F32)[None, :]
    return jnp.cos(angles), jnp.sin(angles)


def solution(mesh):
    swap = [(0, 1), (1, 0)]

    def local_step(tokens, lengths, embed_table, layer_vecs, w_qkv, w_out, w_up, b_up, w_down, grad_out):
        cp_index = lax.axis_index('cp')
        dim = embed_table.shape[1]
        n_heads, hd = w_qkv.shape[2], w_qkv.shape[3]
        slabs = w_up.shape[1] // FTILE
        cos_t, sin_t = rope_tables(2 * tokens.shape[1], hd)
        small = jnp.concatenate([layer_vecs, b_up.reshape(-1, layer_vecs.shape[1])], 0)
        small = jnp.pad(small, ((0, 16 - small.shape[0]), (0, 0)))
        (qkv, o, lse, cls, scales, e_cls, hc, up_b, vecs, w_all, out_w, up_w, down_w, g_peer) = attn_fwd(
            lengths, tokens, embed_table, cos_t, sin_t, small, w_qkv.reshape(w_qkv.shape[0], -1), w_out, w_up,
            w_down.reshape(slabs, -1, dim), grad_out)
        (out_m, out_p, do, delta, csums, dvec_b, d_bup, d_wo, d_wu, d_wd, red_wu, red_wd) = ffn(
            scales, cls, o, grad_out, g_peer, embed_table, vecs, up_b, out_w.reshape(dim, dim), up_w.reshape(dim, -1),
            down_w.reshape(-1, dim), n_heads, hd)
        out_back = lax.ppermute(out_p, 'cp', swap)
        layer_out = jnp.where(cp_index == 0, jnp.concatenate([out_m, out_back], 0), jnp.concatenate([out_back, out_m], 0))
        d_wup, d_wdown, d_wout, d_w, d_table, d_vecs, d_bup = attn_bwd(
            lengths, scales, cls, cos_t, sin_t, qkv, do, lse, delta, hc, w_all.reshape(dim, -1), csums, e_cls, vecs, dvec_b, d_bup,
            red_wu, red_wd, d_wu, d_wd, d_wo, n_heads, hd)
        groups = d_w.shape[0]
        d_w = jnp.transpose(d_w.reshape(groups, -1, 3, n_heads // groups, hd), (1, 2, 0, 3, 4)).reshape(w_qkv.shape)
        return layer_out, d_table, d_vecs, d_w, d_wout, d_wup, d_bup.reshape(-1), d_wdown.reshape(w_down.shape)

    in_specs = (P('fsdp', 'cp'), P('fsdp'), P(), P(None, 'fsdp'), P('fsdp', None, None, None), P('fsdp', None), P('fsdp', None), P('fsdp'), P('fsdp', None), P('fsdp', 'cp', None))
    out_specs = (P('fsdp', 'cp', None), P(), P(None, 'fsdp'), P('fsdp', None, None, None), P('fsdp', None), P('fsdp', None), P('fsdp'), P('fsdp', None))
    return jax.shard_map(local_step, mesh=mesh, in_specs=in_specs, out_specs=out_specs, check_vma=False)
```
